32 devices in a mesh: dp: 4 (over y, z), ep: 8 (over x, core).
Axes of the slice: x: 4, y: 2, z: 2, core: 2. Of those that a mesh axis runs over, the one named last changes fastest.
The devices are a block of a 4x4x8 slice.
Arguments:
- grad_y: bfloat16 [4096, 1024], P(('dp', 'ep')), parts along dimension 0
- gate_vals: float32 [4096, 8], P(('dp', 'ep')), parts along dimension 0
- topk_idx: int32 [4096, 8], P(('dp', 'ep')), parts along dimension 0
- slot_ids: int32 [4096, 8], P(('dp', 'ep')), parts along dimension 0
- pair_counts: int32 [32, 32], P(('dp', 'ep')), parts along dimension 0
- y_routed: bfloat16 [4096, 8, 1024], P(('dp', 'ep')), parts along dimension 0
- x_disp: bfloat16 [128, 512, 1024], P(('dp', 'ep')), parts along dimension 0
- h_gate: bfloat16 [128, 512, 512], P(('dp', 'ep')), parts along dimension 0
- h_up: bfloat16 [128, 512, 512], P(('dp', 'ep')), parts along dimension 0
- w_gate: bfloat16 [32, 1024, 512], P('ep')
- w_up: bfloat16 [32, 1024, 512], P('ep')
- w_down: bfloat16 [32, 512, 1024], P('ep')
Outputs:
- output 1: bfloat16 [4096, 1024], P(('dp', 'ep')), parts along dimension 0
- output 2: float32 [4096, 8], P(('dp', 'ep')), parts along dimension 0
- output 3: float32 [128, 1024, 512], P(('dp', 'ep')), parts along dimension 0
- output 4: float32 [128, 1024, 512], P(('dp', 'ep')), parts along dimension 0
- output 5: float32 [128, 512, 1024], P(('dp', 'ep')), parts along dimension 0
There are 4 independent parts. The reference program is written for one: setup_inputs(seed, part) draws one part's arguments, and reference() takes and returns one part's arrays. A program takes and returns all parts, laid end to end along the dimension named above; an argument that names none is the same for every part.
All inputs are finite; a program needn't handle non-finite values.
Results may differ from the reference program's by a relative error of at most 0.014959.
Values are sent between devices in bfloat16 or wider.
A program may use at most 768 MiB of HBM per device.

```python
import jax
import jax.numpy as jnp
from jax import lax

GROUP_DEV = 8
TOKENS_DEV = 128
EXPERTS = 32
TOP_K = 8
MODEL_DIM = 1024
FFN_DIM = 512
CAPACITY = 64
N_TOKENS = GROUP_DEV * TOKENS_DEV
EXPERT_ROWS = GROUP_DEV * CAPACITY


def setup_inputs(seed: int = 0, part: int = 0) -> dict:
    base_key = jax.random.fold_in(jax.random.key(seed), part)
    key_list = jax.random.split(base_key, 8)
    weight_keys = jax.random.split(jax.random.key(seed + 1), 3)
    key_noise, key_bias, key_hot = jax.random.split(key_list[0], 3)
    expert_iota = jnp.arange(EXPERTS, dtype=jnp.int32)
    token_iota = jnp.arange(TOKENS_DEV, dtype=jnp.int32)
    noise_int = jax.random.randint(key_noise, (GROUP_DEV, TOKENS_DEV, EXPERTS), 0, 4 * EXPERTS)
    bias_base = jax.random.randint(key_bias, (EXPERTS,), 0, 2 * EXPERTS)
    bias_int = (bias_base * bias_base) // (4 * EXPERTS)
    hot_expert = jax.random.randint(key_hot, (GROUP_DEV,), 0, EXPERTS)
    hot_bonus = jnp.where((token_iota[None, :, None] < CAPACITY) & (expert_iota[None, None, :] == hot_expert[:, None, None]), 8 * EXPERTS, 0)
    scores = (noise_int + bias_int[None, None, :] + hot_bonus) * EXPERTS + expert_iota[None, None, :]
    expert_ids = lax.top_k(scores, TOP_K)[1].astype(jnp.int32)

    def rank_one(ids_dev):
        flat_ids = ids_dev.reshape(-1)
        onehot = (flat_ids[:, None] == expert_iota[None, :]).astype(jnp.int32)
        before = jnp.cumsum(onehot, axis=0) - onehot
        rank_pos = jnp.sum(before * onehot, axis=1)
        return rank_pos.reshape(TOKENS_DEV, TOP_K), jnp.sum(onehot, axis=0)

    rank_pos, n_total = lax.map(rank_one, expert_ids)
    slot_dev = jnp.where(rank_pos < CAPACITY, rank_pos, -1).astype(jnp.int32)
    pair_counts = jnp.minimum(n_total, CAPACITY).astype(jnp.int32)
    is_kept = slot_dev >= 0
    slot_safe = jnp.where(is_kept, slot_dev, CAPACITY)
    slot_clip = jnp.where(is_kept, slot_dev, 0)
    src_dev = jnp.broadcast_to(jnp.arange(GROUP_DEV, dtype=jnp.int32)[:, None, None], expert_ids.shape)

    w_gate = (jax.random.normal(weight_keys[0], (EXPERTS, MODEL_DIM, FFN_DIM), jnp.float32) * MODEL_DIM ** -0.5).astype(jnp.bfloat16)
    w_up = (jax.random.normal(weight_keys[1], (EXPERTS, MODEL_DIM, FFN_DIM), jnp.float32) * MODEL_DIM ** -0.5).astype(jnp.bfloat16)
    w_down = (jax.random.normal(weight_keys[2], (EXPERTS, FFN_DIM, MODEL_DIM), jnp.float32) * FFN_DIM ** -0.5).astype(jnp.bfloat16)
    x_tok = jax.random.normal(key_list[1], (GROUP_DEV, TOKENS_DEV, MODEL_DIM), jnp.float32).astype(jnp.bfloat16)
    stale_rows = jax.random.normal(key_list[2], (EXPERTS, GROUP_DEV, CAPACITY, MODEL_DIM), jnp.float32).astype(jnp.bfloat16)
    x_vals = jnp.broadcast_to(x_tok[:, :, None, :], (GROUP_DEV, TOKENS_DEV, TOP_K, MODEL_DIM))
    x_disp = stale_rows.at[expert_ids, src_dev, slot_safe].set(x_vals, mode="drop").reshape(EXPERTS, EXPERT_ROWS, MODEL_DIM)

    def forward_one(operands):
        x_rows, w_gate_e, w_up_e, w_down_e = operands
        h_g = jnp.dot(x_rows, w_gate_e, preferred_element_type=jnp.float32).astype(jnp.bfloat16)
        h_u = jnp.dot(x_rows, w_up_e, preferred_element_type=jnp.float32).astype(jnp.bfloat16)
        gate_f = h_g.astype(jnp.float32)
        hidden_act = (gate_f * jax.nn.sigmoid(gate_f) * h_u.astype(jnp.float32)).astype(jnp.bfloat16)
        y_rows = jnp.dot(hidden_act, w_down_e, preferred_element_type=jnp.float32).astype(jnp.bfloat16)
        return h_g, h_u, y_rows

    h_gate, h_up, y_exp = lax.map(forward_one, (x_disp, w_gate, w_up, w_down))
    y_pick = y_exp.reshape(EXPERTS, GROUP_DEV, CAPACITY, MODEL_DIM)[expert_ids, src_dev, slot_clip]
    y_routed = jnp.where(is_kept[..., None], y_pick, jnp.zeros((), jnp.bfloat16)).reshape(N_TOKENS, TOP_K, MODEL_DIM)
    grad_y = jax.random.normal(key_list[3], (N_TOKENS, MODEL_DIM), jnp.float32).astype(jnp.bfloat16)
    gate_vals = jax.random.uniform(key_list[4], (N_TOKENS, TOP_K), jnp.float32, 0.25, 1.0)
    return {"grad_y": grad_y, "gate_vals": gate_vals, "topk_idx": expert_ids.reshape(N_TOKENS, TOP_K), "slot_ids": slot_dev.reshape(N_TOKENS, TOP_K), "pair_counts": pair_counts, "y_routed": y_routed, "x_disp": x_disp, "h_gate": h_gate, "h_up": h_up, "w_gate": w_gate, "w_up": w_up, "w_down": w_down}


def reference(grad_y, gate_vals, topk_idx, slot_ids, pair_counts, y_routed, x_disp, h_gate, h_up, w_gate, w_up, w_down):
    grad_gate = jnp.einsum("td,tkd->tk", grad_y.astype(jnp.float32), y_routed.astype(jnp.float32))
    is_kept = slot_ids >= 0
    src_dev = jnp.broadcast_to((jnp.arange(N_TOKENS, dtype=jnp.int32) // TOKENS_DEV)[:, None], topk_idx.shape)
    slot_safe = jnp.where(is_kept, slot_ids, CAPACITY)
    slot_clip = jnp.where(is_kept, slot_ids, 0)
    gated_rows = (gate_vals[:, :, None] * grad_y.astype(jnp.float32)[:, None, :]).astype(jnp.bfloat16)
    disp_rows = jnp.zeros((EXPERTS, GROUP_DEV, CAPACITY, MODEL_DIM), jnp.bfloat16).at[topk_idx, src_dev, slot_safe].set(gated_rows, mode="drop")
    keep_row = jnp.arange(CAPACITY)[None, None, :] < jnp.transpose(pair_counts)[:, :, None]
    disp_rows = jnp.where(keep_row[..., None], disp_rows, jnp.zeros((), jnp.bfloat16)).reshape(EXPERTS, EXPERT_ROWS, MODEL_DIM)

    def expert_one(operands):
        grad_rows, x_rows, hg_rows, hu_rows, w_gate_e, w_up_e, w_down_e = operands
        grad_hidden = jnp.dot(grad_rows, w_down_e.T, preferred_element_type=jnp.float32).astype(jnp.bfloat16)
        gate_f = hg_rows.astype(jnp.float32)
        up_f = hu_rows.astype(jnp.float32)
        gate_sig = jax.nn.sigmoid(gate_f)
        gate_act = gate_f * gate_sig
        hidden_act = (gate_act * up_f).astype(jnp.bfloat16)
        grad_h = grad_hidden.astype(jnp.float32)
        grad_hgate = (grad_h * up_f * gate_sig * (1.0 + gate_f * (1.0 - gate_sig))).astype(jnp.bfloat16)
        grad_hup = (grad_h * gate_act).astype(jnp.bfloat16)
        grad_wdown = jnp.dot(hidden_act.T, grad_rows, preferred_element_type=jnp.float32)
        grad_wgate = jnp.dot(x_rows.T, grad_hgate, preferred_element_type=jnp.float32)
        grad_wup = jnp.dot(x_rows.T, grad_hup, preferred_element_type=jnp.float32)
        grad_disp = (jnp.dot(grad_hgate, w_gate_e.T, preferred_element_type=jnp.float32) + jnp.dot(grad_hup, w_up_e.T, preferred_element_type=jnp.float32)).astype(jnp.bfloat16)
        return grad_disp, grad_wgate, grad_wup, grad_wdown

    grad_disp, grad_w_gate, grad_w_up, grad_w_down = lax.map(expert_one, (disp_rows, x_disp, h_gate, h_up, w_gate, w_up, w_down))
    back_rows = grad_disp.reshape(EXPERTS, GROUP_DEV, CAPACITY, MODEL_DIM)[topk_idx, src_dev, slot_clip]
    grad_x = jnp.sum(jnp.where(is_kept[..., None], back_rows.astype(jnp.float32), 0.0), axis=1).astype(jnp.bfloat16)
    return grad_x, grad_gate, grad_w_gate, grad_w_up, grad_w_down
```

```python
import functools

import jax
import jax.numpy as jnp
from jax import lax
from jax.experimental import pallas as pl
from jax.experimental.pallas import tpu as pltpu
from jax.sharding import PartitionSpec as P

F32, BF16 = jnp.float32, jnp.bfloat16
COLS = 256
OPP, LEFT, RIGHT, OWN = range(4)


def dot_last(a, b):
    return lax.dot_general(a, b, (((1,), (1,)), ((), ())), preferred_element_type=F32)


def dot_first(a, b):
    return lax.dot_general(a, b, (((0,), (0,)), ((), ())), preferred_element_type=F32)


def exchange_kernel(axis, n_dev, topk_ref, slot_ref, gate_ref, count_ref, gy_hbm, y_hbm, hg_hbm, hu_hbm, wg_hbm, wu_hbm, wd_hbm,
                    d_out, dh_out, a_out, gg_out, right_out, left_out, own_out,
                    gy_all, route_send, route_all, y_buf, hg_buf, hu_buf, wgu_buf, wd_buf, f1_buf, s_buf, a_buf,
                    oh_buf, d_buf, dh_buf, r_buf, keep_buf, pair_send, pair_recv, hop_recv,
                    load_sem, store_sem, route_ssem, route_rsem, gy_ssem, gy_rsem, pair_ssem, pair_rsem, hop_ssem, hop_rsem):
    n_loc, n_rows, ffn = hg_hbm.shape
    tok, model = gy_hbm.shape
    top_k = topk_ref.shape[1]
    cap = n_rows // n_dev
    n_exp = n_loc * n_dev
    half = tok // 2
    pair_rows = 2 * cap
    n_chip = n_dev // 2

    me = lax.axis_index(axis)
    chip = lax.div(me, 2)
    core = me - 2 * chip
    chips = [lax.rem(chip + step, n_chip) for step in (2, n_chip - 1, 1, 0)]
    homes = [2 * c + core for c in chips]
    others = [2 * c + 1 - core for c in chips]
    opp, left, right = homes[OPP], homes[LEFT], homes[RIGHT]
    sib = others[OWN]
    top, bottom = pl.ds(0, half), pl.ds(half, half)

    barrier = pltpu.get_barrier_semaphore()
    for step in range(1, n_dev):
        pl.semaphore_signal(barrier, inc=1, device_id={axis: lax.rem(me + step, n_dev)}, device_id_type=pl.DeviceIdType.MESH)

    loads = {}

    def load(name, src, dst):
        loads[name] = pltpu.make_async_copy(src, dst, load_sem.at[len(loads)])
        loads[name].start()

    load("gy", gy_hbm, gy_all.at[me])
    for e in range(n_loc):
        load(("hg", e), hg_hbm.at[e], hg_buf.at[e])
        load(("hu", e), hu_hbm.at[e], hu_buf.at[e])
    load("y", y_hbm, y_buf)
    load("wd", wd_hbm, wd_buf)
    load("wg", wg_hbm, wgu_buf.at[:, :, pl.ds(0, ffn)])
    load("wu", wu_hbm, wgu_buf.at[:, :, pl.ds(ffn, ffn)])

    topk_t = topk_ref[...].astype(F32).T
    slot_t = slot_ref[...].astype(F32).T
    gate_t = gate_ref[...].T
    exp_iota = lax.broadcasted_iota(jnp.int32, (n_exp, tok), 0).astype(F32)
    diag = lax.broadcasted_iota(jnp.int32, (n_exp, n_exp), 0) == lax.broadcasted_iota(jnp.int32, (n_exp, n_exp), 1)
    count = jnp.sum(jnp.where(diag, count_ref[...].astype(F32), 0.0), axis=1, keepdims=True)
    slot_d = jnp.zeros((n_exp, tok), F32)
    gate_d = jnp.zeros((n_exp, tok), F32)
    for j in range(top_k):
        hit = topk_t[j : j + 1] == exp_iota
        slot_d += jnp.where(hit, slot_t[j : j + 1] + 1.0, 0.0)
        gate_d += jnp.where(hit, gate_t[j : j + 1], 0.0)
    slot_d -= 1.0
    slot_d = jnp.where(slot_d < count, slot_d, -1.0)
    for i in range(n_dev):
        route_send[i, 0:n_loc] = slot_d[i * n_loc : (i + 1) * n_loc]
        route_send[i, n_loc : 2 * n_loc] = gate_d[i * n_loc : (i + 1) * n_loc]
    route_all[me] = route_send[me]

    loads["gy"].wait()
    pl.semaphore_wait(barrier, n_dev - 1)

    def remote(src, dst, ssem, rsem, dev):
        return pltpu.make_async_remote_copy(src_ref=src, dst_ref=dst, send_sem=ssem, recv_sem=rsem, device_id={axis: dev}, device_id_type=pl.DeviceIdType.MESH)

    sends = []

    def gy_copy(block, part, send_slot, recv_slot, dev):
        ref = gy_all.at[block, part]
        return remote(ref, ref, gy_ssem.at[send_slot], gy_rsem.at[recv_slot], dev)

    def gy_send(block, part, recv_slot, dev):
        copy = gy_copy(block, part, recv_slot, recv_slot, dev)
        copy.start()
        sends.append(copy)

    def gy_wait(block, part, recv_slot):
        gy_copy(block, part, recv_slot, recv_slot, sib).wait_recv()

    gy_send(me, top, 0, right)
    gy_send(me, bottom, 2, left)
    gy_send(me, bottom, 1, right)
    gy_send(me, top, 3, left)
    gy_send(me, pl.ds(0, tok), 6, sib)
    for step in range(1, n_dev):
        dst = lax.rem(me + step, n_dev)
        copy = remote(route_send.at[dst], route_all.at[me], route_ssem.at[step - 1], route_rsem.at[step - 1], dst)
        copy.start()
        sends.append(copy)

    chunk = 32
    n_chunk = n_rows // chunk

    def factors(e):
        def body(i, carry):
            rows = pl.ds(pl.multiple_of(i * chunk, chunk), chunk)
            h1 = hg_buf[e, rows].astype(F32)
            h3 = hu_buf[e, rows].astype(F32)
            sig = jax.nn.sigmoid(h1)
            act = h1 * sig
            s_buf[e, rows] = act
            a_buf[e, rows] = (act * h3).astype(BF16)
            f1_buf[e, rows] = h3 * sig * (1.0 + h1 * (1.0 - sig))
            return carry

        loads[("hg", e)].wait()
        loads[("hu", e)].wait()
        lax.fori_loop(0, n_chunk, body, 0)

    factors(0)
    factors(1)

    gy_wait(left, top, 0)
    gy_send(left, top, 4, right)
    gy_send(left, top, 7, sib)
    gy_wait(right, bottom, 2)
    gy_send(right, bottom, 5, left)
    gy_send(right, bottom, 9, sib)

    factors(2)
    factors(3)
    store_a = pltpu.make_async_copy(a_buf, a_out, store_sem.at[4])
    store_a.start()

    gy_wait(left, bottom, 1)
    gy_send(left, bottom, 8, sib)
    gy_wait(right, top, 3)
    gy_send(right, top, 10, sib)

    loads["y"].wait()
    group = 32
    gg = jnp.zeros((top_k, tok), F32)
    tok_major = lax.broadcasted_iota(jnp.int32, (group, top_k, tok), 0)
    tok_lane = lax.broadcasted_iota(jnp.int32, (group, top_k, tok), 2)
    for i in range(tok // group):
        prod = dot_last(y_buf[pl.ds(i * group * top_k, group * top_k)], gy_all[me])
        gg += jnp.sum(jnp.where(tok_major + i * group == tok_lane, prod.reshape(group, top_k, tok), 0.0), axis=0)
    gg_out[...] = gg.T

    for step in range(1, n_dev):
        src = lax.rem(me + n_dev - step, n_dev)
        remote(route_send.at[src], route_all.at[src], route_ssem.at[step - 1], route_rsem.at[step - 1], src).wait_recv()

    gy_wait(opp, top, 4)
    gy_send(opp, top, 11, sib)
    gy_wait(opp, bottom, 5)
    gy_send(opp, bottom, 12, sib)

    slot_iota = lax.broadcasted_iota(jnp.int32, (cap, tok), 0).astype(F32)

    def build_rows(s):
        route = route_all[s]
        gates = []
        for e in range(n_loc):
            hit = route[e : e + 1] == slot_iota
            oh_buf[s, pl.ds(e * cap, cap)] = jnp.where(hit, 1.0, 0.0).astype(BF16)
            gates.append(jnp.sum(jnp.where(hit, route[n_loc + e : n_loc + e + 1], 0.0), axis=1, keepdims=True))
        gate = jnp.concatenate(gates, axis=0)
        pick = oh_buf[s]
        for n in range(0, model, COLS):
            rows = (jnp.dot(pick, gy_all[s, :, pl.ds(n, COLS)], preferred_element_type=F32) * gate).astype(BF16)
            for e in range(n_loc):
                d_buf[e, pl.ds(pl.multiple_of(s * cap, cap), cap), pl.ds(n, COLS)] = rows[e * cap : (e + 1) * cap]

    def rows_of(c):
        return pl.ds(pl.multiple_of(c * pair_rows, pair_rows), pair_rows)

    def experts(which, lo, hi):
        def body(e, carry):
            d_rows = jnp.concatenate([d_buf[e, rows_of(c)] for c in which], axis=0)
            for n in range(0, ffn, COLS):
                grad = dot_last(d_rows, wd_buf[e, pl.ds(n, COLS)]).astype(BF16).astype(F32)
                for i, c in enumerate(which):
                    part = grad[i * pair_rows : (i + 1) * pair_rows]
                    dh_buf[e, rows_of(c), pl.ds(n, COLS)] = (part * f1_buf[e, rows_of(c), pl.ds(n, COLS)]).astype(BF16)
                    dh_buf[e, rows_of(c), pl.ds(ffn + n, COLS)] = (part * s_buf[e, rows_of(c), pl.ds(n, COLS)]).astype(BF16)
            dh_rows = jnp.concatenate([dh_buf[e, rows_of(c)] for c in which], axis=0)
            out_rows = pl.ds(pl.multiple_of(e * cap, cap), cap)
            for n in range(0, model, COLS):
                ret = dot_last(dh_rows, wgu_buf[e, pl.ds(n, COLS)]).astype(BF16)
                for i, c in enumerate(which):
                    for k in range(2):
                        lo_row = i * pair_rows + k * cap
                        r_buf[2 * c + k, out_rows, pl.ds(n, COLS)] = ret[lo_row : lo_row + cap]
            return carry

        lax.fori_loop(lo, hi, body, 0)

    def sum_rows(s, dst):
        pick = oh_buf[s]
        for n in range(0, model, COLS):
            dst[:, pl.ds(n, COLS)] = dot_first(pick, r_buf[s, :, pl.ds(n, COLS)])

    stores = []

    def store_rows(role):
        rows = rows_of(chips[role])
        for k, (src, dst) in enumerate(((d_buf, d_out), (dh_buf, dh_out))):
            copy = pltpu.make_async_copy(src.at[:, rows], dst.at[:, rows], store_sem.at[5 + 2 * role + k])
            copy.start()
            stores.append(copy)

    pairs = {}

    def finish(role):
        store_rows(role)
        sum_rows(others[role], pair_send.at[role])
        pairs[role] = remote(pair_send.at[role], pair_recv.at[role], pair_ssem.at[role], pair_rsem.at[role], sib)
        pairs[role].start()
        sends.append(pairs[role])
        sum_rows(homes[role], keep_buf.at[role])

    loads["wd"].wait()
    gy_wait(others[OPP], top, 11)
    gy_wait(others[OPP], bottom, 12)
    build_rows(homes[OPP])
    build_rows(others[OPP])
    loads["wg"].wait()
    loads["wu"].wait()
    experts([chips[OPP]], 0, n_loc)
    finish(OPP)

    gy_wait(others[LEFT], top, 7)
    gy_wait(others[LEFT], bottom, 8)
    gy_wait(others[RIGHT], bottom, 9)
    gy_wait(others[RIGHT], top, 10)
    for role in (LEFT, RIGHT):
        build_rows(homes[role])
        build_rows(others[role])
    experts([chips[LEFT], chips[RIGHT]], 0, n_loc // 2)

    pairs[OPP].wait_recv()
    keep_buf[OPP] = keep_buf[OPP] + pair_recv[OPP]
    hop_right = remote(keep_buf.at[OPP, top], hop_recv.at[0], hop_ssem.at[0], hop_rsem.at[0], right)
    hop_right.start()
    hop_left = remote(keep_buf.at[OPP, bottom], hop_recv.at[1], hop_ssem.at[1], hop_rsem.at[1], left)
    hop_left.start()
    sends.extend([hop_right, hop_left])

    experts([chips[LEFT], chips[RIGHT]], n_loc // 2, n_loc)
    finish(LEFT)
    finish(RIGHT)

    gy_wait(others[OWN], pl.ds(0, tok), 6)
    build_rows(homes[OWN])
    build_rows(others[OWN])
    experts([chips[OWN]], 0, n_loc)
    finish(OWN)

    pairs[LEFT].wait_recv()
    pairs[RIGHT].wait_recv()
    right_out[bottom] = keep_buf[RIGHT, bottom] + pair_recv[RIGHT, bottom]
    left_out[top] = keep_buf[LEFT, top] + pair_recv[LEFT, top]
    pairs[OWN].wait_recv()
    own_out[...] = keep_buf[OWN] + pair_recv[OWN]
    hop_right.wait_recv()
    right_out[top] = keep_buf[RIGHT, top] + pair_recv[RIGHT, top] + hop_recv[0]
    hop_left.wait_recv()
    left_out[bottom] = keep_buf[LEFT, bottom] + pair_recv[LEFT, bottom] + hop_recv[1]

    for copy in sends:
        copy.wait_send()
    for copy in stores:
        copy.wait()
    store_a.wait()


def exchange(axis, n_dev, topk_idx, slot_ids, gate_vals, pair_counts, grad_y, y_rows, h_gate, h_up, w_gate, w_up, w_down):
    n_loc, n_rows, ffn = h_gate.shape
    tok, model = grad_y.shape
    top_k = topk_idx.shape[1]
    cap = n_rows // n_dev
    vmem = pl.BlockSpec(memory_space=pltpu.VMEM)
    hbm = pl.BlockSpec(memory_space=pl.ANY)
    dma = pltpu.SemaphoreType.DMA
    part = jax.ShapeDtypeStruct((tok, model), F32)
    return pl.pallas_call(
        functools.partial(exchange_kernel, axis, n_dev),
        name="exchange",
        out_shape=(
            jax.ShapeDtypeStruct((n_loc, n_rows, model), BF16),
            jax.ShapeDtypeStruct((n_loc, n_rows, 2 * ffn), BF16),
            jax.ShapeDtypeStruct((n_loc, n_rows, ffn), BF16),
            jax.ShapeDtypeStruct((tok, top_k), F32),
            part, part, part,
        ),
        in_specs=[vmem] * 4 + [hbm] * 7,
        out_specs=(hbm, hbm, hbm, vmem, vmem, vmem, vmem),
        scratch_shapes=[
            pltpu.VMEM((n_dev, tok, model), BF16),
            pltpu.VMEM((n_dev, 2 * n_loc, tok), F32),
            pltpu.VMEM((n_dev, 2 * n_loc, tok), F32),
            pltpu.VMEM(y_rows.shape, BF16),
            pltpu.VMEM(h_gate.shape, BF16),
            pltpu.VMEM(h_up.shape, BF16),
            pltpu.VMEM((n_loc, model, 2 * ffn), BF16),
            pltpu.VMEM(w_down.shape, BF16),
            pltpu.VMEM(h_gate.shape, F32),
            pltpu.VMEM(h_gate.shape, F32),
            pltpu.VMEM(h_gate.shape, BF16),
            pltpu.VMEM((n_dev, n_loc * cap, tok), BF16),
            pltpu.VMEM((n_loc, n_rows, model), BF16),
            pltpu.VMEM((n_loc, n_rows, 2 * ffn), BF16),
            pltpu.VMEM((n_dev, n_loc * cap, model), BF16),
            pltpu.VMEM((4, tok, model), F32),
            pltpu.VMEM((4, tok, model), F32),
            pltpu.VMEM((4, tok, model), F32),
            pltpu.VMEM((2, tok // 2, model), F32),
            dma((5 + 2 * n_loc,)), dma((13,)), dma((n_dev - 1,)), dma((n_dev - 1,)), dma((13,)), dma((13,)),
            dma((4,)), dma((4,)), dma((2,)), dma((2,)),
        ],
        compiler_params=pltpu.CompilerParams(collective_id=0, has_side_effects=True, vmem_limit_bytes=60 * 1024 * 1024),
    )(topk_idx, slot_ids, gate_vals, pair_counts, grad_y, y_rows, h_gate, h_up, w_gate, w_up, w_down)


def weight_kernel(ffn, x_ref, dh_ref, a_ref, d_ref, gg_ref, wg_out, wu_out, wd_out, gg_out):
    @pl.when((pl.program_id(0) == 0) & (pl.program_id(1) == 0))
    def _():
        gg_out[...] = gg_ref[...]

    x = x_ref[0]
    for n in range(0, ffn, COLS):
        wg_out[0, :, pl.ds(n, COLS)] = dot_first(x, dh_ref[0, :, pl.ds(n, COLS)])
        wu_out[0, :, pl.ds(n, COLS)] = dot_first(x, dh_ref[0, :, pl.ds(ffn + n, COLS)])
    a = a_ref[0]
    for n in range(0, d_ref.shape[2], COLS):
        wd_out[0, :, pl.ds(n, COLS)] = dot_first(a, d_ref[0, :, pl.ds(n, COLS)])


def weight_grads(x_disp, dh_rows, a_rows, d_rows, gg):
    n_loc, n_rows, model = x_disp.shape
    ffn = a_rows.shape[2]
    split = 2
    m_blk, f_blk = model // split, ffn // split
    flops = 2 * n_loc * n_rows * model * 3 * ffn
    moved = 2 * (x_disp.size + dh_rows.size + a_rows.size + d_rows.size) + 12 * n_loc * model * ffn
    return pl.pallas_call(
        functools.partial(weight_kernel, ffn),
        name="weight_grads",
        grid=(n_loc, split),
        in_specs=[
            pl.BlockSpec((1, n_rows, m_blk), lambda e, h: (e, 0, h)),
            pl.BlockSpec((1, n_rows, 2 * ffn), lambda e, h: (e, 0, 0)),
            pl.BlockSpec((1, n_rows, f_blk), lambda e, h: (e, 0, h)),
            pl.BlockSpec((1, n_rows, model), lambda e, h: (e, 0, 0)),
            pl.BlockSpec(gg.shape, lambda e, h: (0, 0)),
        ],
        out_specs=(
            pl.BlockSpec((1, m_blk, ffn), lambda e, h: (e, h, 0)),
            pl.BlockSpec((1, m_blk, ffn), lambda e, h: (e, h, 0)),
            pl.BlockSpec((1, f_blk, model), lambda e, h: (e, h, 0)),
            pl.BlockSpec(gg.shape, lambda e, h: (0, 0)),
        ),
        out_shape=(
            jax.ShapeDtypeStruct((n_loc, model, ffn), F32),
            jax.ShapeDtypeStruct((n_loc, model, ffn), F32),
            jax.ShapeDtypeStruct((n_loc, ffn, model), F32),
            jax.ShapeDtypeStruct(gg.shape, F32),
        ),
        cost_estimate=pl.CostEstimate(flops=flops, bytes_accessed=moved, transcendentals=0),
        compiler_params=pltpu.CompilerParams(vmem_limit_bytes=40 * 1024 * 1024),
    )(x_disp, dh_rows, a_rows, d_rows, gg)


def final_kernel(own_ref, left_ref, right_ref, gx_out):
    gx_out[...] = (own_ref[...] + left_ref[...] + right_ref[...]).astype(BF16)


def final_sum(own, from_left, from_right):
    vmem = pl.BlockSpec(memory_space=pltpu.VMEM)
    return pl.pallas_call(
        final_kernel,
        name="final_sum",
        out_shape=jax.ShapeDtypeStruct(own.shape, BF16),
        in_specs=[vmem] * 3,
        out_specs=vmem,
    )(own, from_left, from_right)


def solution(mesh):
    axis = "ep"
    n_dev = mesh.shape[axis]
    rows_spec = P(("dp", "ep"), None)
    cube_spec = P(("dp", "ep"), None, None)
    weight_spec = P("ep", None, None)
    to_right = [(i, (i + 2) % n_dev) for i in range(n_dev)]
    to_left = [(i, (i - 2) % n_dev) for i in range(n_dev)]

    def local_step(grad_y, gate_vals, topk_idx, slot_ids, pair_counts, y_routed, x_disp, h_gate, h_up, w_gate, w_up, w_down):
        y_rows = y_routed.reshape(-1, y_routed.shape[2])
        d_rows, dh_rows, a_rows, gg, for_right, for_left, own = exchange(
            axis, n_dev, topk_idx, slot_ids, gate_vals, pair_counts, grad_y, y_rows, h_gate, h_up, w_gate, w_up, w_down)
        from_left = lax.ppermute(for_right, axis, to_right)
        from_right = lax.ppermute(for_left, axis, to_left)
        grad_wgate, grad_wup, grad_wdown, grad_gate = weight_grads(x_disp, dh_rows, a_rows, d_rows, gg)
        grad_x = final_sum(own, from_left, from_right)
        return grad_x, grad_gate, grad_wgate, grad_wup, grad_wdown

    return jax.shard_map(local_step, mesh=mesh, in_specs=(rows_spec, rows_spec, rows_spec, rows_spec, rows_spec, cube_spec, cube_spec, cube_spec, cube_spec, weight_spec, weight_spec, weight_spec), out_specs=(rows_spec, rows_spec, cube_spec, cube_spec, cube_spec), check_vma=False)
```

```python
import functools

import jax
import jax.numpy as jnp
from jax import lax
from jax.experimental import pallas as pl
from jax.experimental.pallas import tpu as pltpu
from jax.sharding import PartitionSpec as P

F32, BF16 = jnp.float32, jnp.bfloat16
COLS = 256
OPP, LEFT, RIGHT, OWN = range(4)


def dot_last(a, b):
    return lax.dot_general(a, b, (((1,), (1,)), ((), ())), preferred_element_type=F32)


def dot_first(a, b):
    return lax.dot_general(a, b, (((0,), (0,)), ((), ())), preferred_element_type=F32)


def exchange_kernel(axis, n_dev, topk_ref, slot_ref, gate_ref, count_ref, gy_hbm, y_hbm, hg_hbm, hu_hbm, wg_hbm, wu_hbm, wd_hbm,
                    d_out, dh_out, a_out, gg_out, right_out, left_out, own_out,
                    gy_all, route_send, route_all, y_buf, hg_buf, hu_buf, wgu_buf, wd_buf, f1_buf, s_buf, a_buf,
                    oh_buf, d_buf, dh_buf, r_buf, keep_buf, pair_send, pair_recv, hop_recv,
                    load_sem, store_sem, route_ssem, route_rsem, gy_ssem, gy_rsem, pair_ssem, pair_rsem, hop_ssem, hop_rsem):
    n_loc, n_rows, ffn = hg_hbm.shape
    tok, model = gy_hbm.shape
    top_k = topk_ref.shape[0]
    cap = n_rows // n_dev
    n_exp = n_loc * n_dev
    half = tok // 2
    pair_rows = 2 * cap
    n_chip = n_dev // 2

    me = lax.axis_index(axis)
    chip = lax.div(me, 2)
    core = me - 2 * chip
    chips = [lax.rem(chip + step, n_chip) for step in (2, n_chip - 1, 1, 0)]
    homes = [2 * c + core for c in chips]
    others = [2 * c + 1 - core for c in chips]
    opp, left, right = homes[OPP], homes[LEFT], homes[RIGHT]
    sib = others[OWN]
    top, bottom = pl.ds(0, half), pl.ds(half, half)

    barrier = pltpu.get_barrier_semaphore()
    for step in range(1, n_dev):
        pl.semaphore_signal(barrier, inc=1, device_id={axis: lax.rem(me + step, n_dev)}, device_id_type=pl.DeviceIdType.MESH)

    loads = {}

    def load(name, src, dst):
        loads[name] = pltpu.make_async_copy(src, dst, load_sem.at[len(loads)])
        loads[name].start()

    load("gy", gy_hbm, gy_all.at[me])
    for e in range(n_loc):
        load(("hg", e), hg_hbm.at[e], hg_buf.at[e])
        load(("hu", e), hu_hbm.at[e], hu_buf.at[e])
    load("y", y_hbm, y_buf)
    load("wd", wd_hbm, wd_buf)
    load("wg", wg_hbm, wgu_buf.at[:, :, pl.ds(0, ffn)])
    load("wu", wu_hbm, wgu_buf.at[:, :, pl.ds(ffn, ffn)])

    topk_t = topk_ref[...].astype(F32)
    slot_t = slot_ref[...].astype(F32)
    gate_t = gate_ref[...]
    exp_iota = lax.broadcasted_iota(jnp.int32, (n_exp, tok), 0).astype(F32)
    diag = lax.broadcasted_iota(jnp.int32, (n_exp, n_exp), 0) == lax.broadcasted_iota(jnp.int32, (n_exp, n_exp), 1)
    count = jnp.sum(jnp.where(diag, count_ref[...].astype(F32), 0.0), axis=1, keepdims=True)
    slot_d = jnp.zeros((n_exp, tok), F32)
    gate_d = jnp.zeros((n_exp, tok), F32)
    for j in range(top_k):
        hit = topk_t[j : j + 1] == exp_iota
        slot_d += jnp.where(hit, slot_t[j : j + 1] + 1.0, 0.0)
        gate_d += jnp.where(hit, gate_t[j : j + 1], 0.0)
    slot_d -= 1.0
    slot_d = jnp.where(slot_d < count, slot_d, -1.0)
    for i in range(n_dev):
        route_send[i, 0:n_loc] = slot_d[i * n_loc : (i + 1) * n_loc]
        route_send[i, n_loc : 2 * n_loc] = gate_d[i * n_loc : (i + 1) * n_loc]
    route_all[me] = route_send[me]

    loads["gy"].wait()
    pl.semaphore_wait(barrier, n_dev - 1)

    def remote(src, dst, ssem, rsem, dev):
        return pltpu.make_async_remote_copy(src_ref=src, dst_ref=dst, send_sem=ssem, recv_sem=rsem, device_id={axis: dev}, device_id_type=pl.DeviceIdType.MESH)

    sends = []

    def gy_copy(block, part, send_slot, recv_slot, dev):
        ref = gy_all.at[block, part]
        return remote(ref, ref, gy_ssem.at[send_slot], gy_rsem.at[recv_slot], dev)

    def gy_send(block, part, recv_slot, dev):
        copy = gy_copy(block, part, recv_slot, recv_slot, dev)
        copy.start()
        sends.append(copy)

    def gy_wait(block, part, recv_slot):
        gy_copy(block, part, recv_slot, recv_slot, sib).wait_recv()

    gy_send(me, top, 0, right)
    gy_send(me, bottom, 2, left)
    gy_send(me, bottom, 1, right)
    gy_send(me, top, 3, left)
    gy_send(me, pl.ds(0, tok), 6, sib)
    for step in range(1, n_dev):
        dst = lax.rem(me + step, n_dev)
        copy = remote(route_send.at[dst], route_all.at[me], route_ssem.at[step - 1], route_rsem.at[step - 1], dst)
        copy.start()
        sends.append(copy)

    chunk = 32
    n_chunk = n_rows // chunk

    def factors(e):
        def body(i, carry):
            rows = pl.ds(pl.multiple_of(i * chunk, chunk), chunk)
            h1 = hg_buf[e, rows].astype(F32)
            h3 = hu_buf[e, rows].astype(F32)
            sig = jax.nn.sigmoid(h1)
            act = h1 * sig
            s_buf[e, rows] = act
            a_buf[e, rows] = (act * h3).astype(BF16)
            f1_buf[e, rows] = h3 * sig * (1.0 + h1 * (1.0 - sig))
            return carry

        loads[("hg", e)].wait()
        loads[("hu", e)].wait()
        lax.fori_loop(0, n_chunk, body, 0)

    factors(0)
    factors(1)

    gy_wait(left, top, 0)
    gy_send(left, top, 4, right)
    gy_send(left, top, 7, sib)
    gy_wait(right, bottom, 2)
    gy_send(right, bottom, 5, left)
    gy_send(right, bottom, 9, sib)

    factors(2)
    factors(3)
    store_a = pltpu.make_async_copy(a_buf, a_out, store_sem.at[4])
    store_a.start()

    gy_wait(left, bottom, 1)
    gy_send(left, bottom, 8, sib)
    gy_wait(right, top, 3)
    gy_send(right, top, 10, sib)

    loads["y"].wait()
    group = 32
    gg = jnp.zeros((top_k, tok), F32)
    tok_major = lax.broadcasted_iota(jnp.int32, (group, top_k, tok), 0)
    tok_lane = lax.broadcasted_iota(jnp.int32, (group, top_k, tok), 2)
    for i in range(tok // group):
        prod = dot_last(y_buf[pl.ds(i * group * top_k, group * top_k)], gy_all[me])
        gg += jnp.sum(jnp.where(tok_major + i * group == tok_lane, prod.reshape(group, top_k, tok), 0.0), axis=0)
    gg_out[...] = gg

    for step in range(1, n_dev):
        src = lax.rem(me + n_dev - step, n_dev)
        remote(route_send.at[src], route_all.at[src], route_ssem.at[step - 1], route_rsem.at[step - 1], src).wait_recv()

    gy_wait(opp, top, 4)
    gy_send(opp, top, 11, sib)
    gy_wait(opp, bottom, 5)
    gy_send(opp, bottom, 12, sib)

    slot_iota = lax.broadcasted_iota(jnp.int32, (cap, tok), 0).astype(F32)

    def build_rows(s):
        route = route_all[s]
        gates = []
        for e in range(n_loc):
            hit = route[e : e + 1] == slot_iota
            oh_buf[s, pl.ds(e * cap, cap)] = jnp.where(hit, 1.0, 0.0).astype(BF16)
            gates.append(jnp.sum(jnp.where(hit, route[n_loc + e : n_loc + e + 1], 0.0), axis=1, keepdims=True))
        gate = jnp.concatenate(gates, axis=0)
        pick = oh_buf[s]
        for n in range(0, model, COLS):
            rows = (jnp.dot(pick, gy_all[s, :, pl.ds(n, COLS)], preferred_element_type=F32) * gate).astype(BF16)
            for e in range(n_loc):
                d_buf[e, pl.ds(pl.multiple_of(s * cap, cap), cap), pl.ds(n, COLS)] = rows[e * cap : (e + 1) * cap]

    def rows_of(c):
        return pl.ds(pl.multiple_of(c * pair_rows, pair_rows), pair_rows)

    def experts(which, lo, hi):
        def body(e, carry):
            d_rows = jnp.concatenate([d_buf[e, rows_of(c)] for c in which], axis=0)
            for n in range(0, ffn, COLS):
                grad = dot_last(d_rows, wd_buf[e, pl.ds(n, COLS)]).astype(BF16).astype(F32)
                for i, c in enumerate(which):
                    part = grad[i * pair_rows : (i + 1) * pair_rows]
                    dh_buf[e, rows_of(c), pl.ds(n, COLS)] = (part * f1_buf[e, rows_of(c), pl.ds(n, COLS)]).astype(BF16)
                    dh_buf[e, rows_of(c), pl.ds(ffn + n, COLS)] = (part * s_buf[e, rows_of(c), pl.ds(n, COLS)]).astype(BF16)
            dh_rows = jnp.concatenate([dh_buf[e, rows_of(c)] for c in which], axis=0)
            out_rows = pl.ds(pl.multiple_of(e * cap, cap), cap)
            for n in range(0, model, COLS):
                ret = dot_last(dh_rows, wgu_buf[e, pl.ds(n, COLS)]).astype(BF16)
                for i, c in enumerate(which):
                    for k in range(2):
                        lo_row = i * pair_rows + k * cap
                        r_buf[2 * c + k, out_rows, pl.ds(n, COLS)] = ret[lo_row : lo_row + cap]
            return carry

        lax.fori_loop(lo, hi, body, 0)

    def sum_rows(s, dst):
        pick = oh_buf[s]
        for n in range(0, model, COLS):
            dst[:, pl.ds(n, COLS)] = dot_first(pick, r_buf[s, :, pl.ds(n, COLS)])

    stores = []

    def store_rows(role):
        rows = rows_of(chips[role])
        for k, (src, dst) in enumerate(((d_buf, d_out), (dh_buf, dh_out))):
            copy = pltpu.make_async_copy(src.at[:, rows], dst.at[:, rows], store_sem.at[5 + 2 * role + k])
            copy.start()
            stores.append(copy)

    pairs = {}

    def finish(role):
        store_rows(role)
        sum_rows(others[role], pair_send.at[role])
        pairs[role] = remote(pair_send.at[role], pair_recv.at[role], pair_ssem.at[role], pair_rsem.at[role], sib)
        pairs[role].start()
        sends.append(pairs[role])
        sum_rows(homes[role], keep_buf.at[role])

    loads["wd"].wait()
    gy_wait(others[OPP], top, 11)
    gy_wait(others[OPP], bottom, 12)
    build_rows(homes[OPP])
    build_rows(others[OPP])
    loads["wg"].wait()
    loads["wu"].wait()
    experts([chips[OPP]], 0, n_loc)
    finish(OPP)

    gy_wait(others[LEFT], top, 7)
    gy_wait(others[LEFT], bottom, 8)
    gy_wait(others[RIGHT], bottom, 9)
    gy_wait(others[RIGHT], top, 10)
    for role in (LEFT, RIGHT):
        build_rows(homes[role])
        build_rows(others[role])
    experts([chips[LEFT], chips[RIGHT]], 0, n_loc // 2)

    pairs[OPP].wait_recv()
    keep_buf[OPP] = keep_buf[OPP] + pair_recv[OPP]
    hop_right = remote(keep_buf.at[OPP, top], hop_recv.at[0], hop_ssem.at[0], hop_rsem.at[0], right)
    hop_right.start()
    hop_left = remote(keep_buf.at[OPP, bottom], hop_recv.at[1], hop_ssem.at[1], hop_rsem.at[1], left)
    hop_left.start()
    sends.extend([hop_right, hop_left])

    experts([chips[LEFT], chips[RIGHT]], n_loc // 2, n_loc)
    finish(LEFT)
    finish(RIGHT)

    gy_wait(others[OWN], pl.ds(0, tok), 6)
    build_rows(homes[OWN])
    build_rows(others[OWN])
    experts([chips[OWN]], 0, n_loc)
    finish(OWN)

    pairs[LEFT].wait_recv()
    pairs[RIGHT].wait_recv()
    right_out[bottom] = keep_buf[RIGHT, bottom] + pair_recv[RIGHT, bottom]
    left_out[top] = keep_buf[LEFT, top] + pair_recv[LEFT, top]
    pairs[OWN].wait_recv()
    own_out[...] = keep_buf[OWN] + pair_recv[OWN]
    hop_right.wait_recv()
    right_out[top] = keep_buf[RIGHT, top] + pair_recv[RIGHT, top] + hop_recv[0]
    hop_left.wait_recv()
    left_out[bottom] = keep_buf[LEFT, bottom] + pair_recv[LEFT, bottom] + hop_recv[1]

    for copy in sends:
        copy.wait_send()
    for copy in stores:
        copy.wait()
    store_a.wait()


def exchange(axis, n_dev, topk_idx, slot_ids, gate_vals, pair_counts, grad_y, y_rows, h_gate, h_up, w_gate, w_up, w_down):
    n_loc, n_rows, ffn = h_gate.shape
    tok, model = grad_y.shape
    top_k = topk_idx.shape[0]
    cap = n_rows // n_dev
    vmem = pl.BlockSpec(memory_space=pltpu.VMEM)
    hbm = pl.BlockSpec(memory_space=pl.ANY)
    dma = pltpu.SemaphoreType.DMA
    part = jax.ShapeDtypeStruct((tok, model), F32)
    return pl.pallas_call(
        functools.partial(exchange_kernel, axis, n_dev),
        name="exchange",
        out_shape=(
            jax.ShapeDtypeStruct((n_loc, n_rows, model), BF16),
            jax.ShapeDtypeStruct((n_loc, n_rows, 2 * ffn), BF16),
            jax.ShapeDtypeStruct((n_loc, n_rows, ffn), BF16),
            jax.ShapeDtypeStruct((top_k, tok), F32),
            part, part, part,
        ),
        in_specs=[vmem] * 4 + [hbm] * 7,
        out_specs=(hbm, hbm, hbm, vmem, vmem, vmem, vmem),
        scratch_shapes=[
            pltpu.VMEM((n_dev, tok, model), BF16),
            pltpu.VMEM((n_dev, 2 * n_loc, tok), F32),
            pltpu.VMEM((n_dev, 2 * n_loc, tok), F32),
            pltpu.VMEM(y_rows.shape, BF16),
            pltpu.VMEM(h_gate.shape, BF16),
            pltpu.VMEM(h_up.shape, BF16),
            pltpu.VMEM((n_loc, model, 2 * ffn), BF16),
            pltpu.VMEM(w_down.shape, BF16),
            pltpu.VMEM(h_gate.shape, F32),
            pltpu.VMEM(h_gate.shape, F32),
            pltpu.VMEM(h_gate.shape, BF16),
            pltpu.VMEM((n_dev, n_loc * cap, tok), BF16),
            pltpu.VMEM((n_loc, n_rows, model), BF16),
            pltpu.VMEM((n_loc, n_rows, 2 * ffn), BF16),
            pltpu.VMEM((n_dev, n_loc * cap, model), BF16),
            pltpu.VMEM((4, tok, model), F32),
            pltpu.VMEM((4, tok, model), F32),
            pltpu.VMEM((4, tok, model), F32),
            pltpu.VMEM((2, tok // 2, model), F32),
            dma((5 + 2 * n_loc,)), dma((13,)), dma((n_dev - 1,)), dma((n_dev - 1,)), dma((13,)), dma((13,)),
            dma((4,)), dma((4,)), dma((2,)), dma((2,)),
        ],
        compiler_params=pltpu.CompilerParams(collective_id=0, has_side_effects=True, vmem_limit_bytes=60 * 1024 * 1024),
    )(topk_idx, slot_ids, gate_vals, pair_counts, grad_y, y_rows, h_gate, h_up, w_gate, w_up, w_down)


def weight_kernel(ffn, x_ref, dh_ref, a_ref, d_ref, gg_ref, wg_out, wu_out, wd_out, gg_out):
    @pl.when((pl.program_id(0) == 0) & (pl.program_id(1) == 0))
    def _():
        gg_out[...] = gg_ref[...]

    x = x_ref[0]
    for n in range(0, ffn, COLS):
        wg_out[0, :, pl.ds(n, COLS)] = dot_first(x, dh_ref[0, :, pl.ds(n, COLS)])
        wu_out[0, :, pl.ds(n, COLS)] = dot_first(x, dh_ref[0, :, pl.ds(ffn + n, COLS)])
    a = a_ref[0]
    for n in range(0, d_ref.shape[2], COLS):
        wd_out[0, :, pl.ds(n, COLS)] = dot_first(a, d_ref[0, :, pl.ds(n, COLS)])


def weight_grads(x_disp, dh_rows, a_rows, d_rows, gg):
    n_loc, n_rows, model = x_disp.shape
    ffn = a_rows.shape[2]
    split = 2
    m_blk, f_blk = model // split, ffn // split
    flops = 2 * n_loc * n_rows * model * 3 * ffn
    moved = 2 * (x_disp.size + dh_rows.size + a_rows.size + d_rows.size) + 12 * n_loc * model * ffn
    return pl.pallas_call(
        functools.partial(weight_kernel, ffn),
        name="weight_grads",
        grid=(n_loc, split),
        in_specs=[
            pl.BlockSpec((1, n_rows, m_blk), lambda e, h: (e, 0, h)),
            pl.BlockSpec((1, n_rows, 2 * ffn), lambda e, h: (e, 0, 0)),
            pl.BlockSpec((1, n_rows, f_blk), lambda e, h: (e, 0, h)),
            pl.BlockSpec((1, n_rows, model), lambda e, h: (e, 0, 0)),
            pl.BlockSpec(gg.shape, lambda e, h: (0, 0)),
        ],
        out_specs=(
            pl.BlockSpec((1, m_blk, ffn), lambda e, h: (e, h, 0)),
            pl.BlockSpec((1, m_blk, ffn), lambda e, h: (e, h, 0)),
            pl.BlockSpec((1, f_blk, model), lambda e, h: (e, h, 0)),
            pl.BlockSpec(gg.shape, lambda e, h: (0, 0)),
        ),
        out_shape=(
            jax.ShapeDtypeStruct((n_loc, model, ffn), F32),
            jax.ShapeDtypeStruct((n_loc, model, ffn), F32),
            jax.ShapeDtypeStruct((n_loc, ffn, model), F32),
            jax.ShapeDtypeStruct(gg.shape, F32),
        ),
        cost_estimate=pl.CostEstimate(flops=flops, bytes_accessed=moved, transcendentals=0),
        compiler_params=pltpu.CompilerParams(vmem_limit_bytes=60 * 1024 * 1024),
    )(x_disp, dh_rows, a_rows, d_rows, gg)


def final_kernel(own_ref, left_ref, right_ref, gx_out):
    gx_out[...] = (own_ref[...] + left_ref[...] + right_ref[...]).astype(BF16)


def final_sum(own, from_left, from_right):
    vmem = pl.BlockSpec(memory_space=pltpu.VMEM)
    return pl.pallas_call(
        final_kernel,
        name="final_sum",
        out_shape=jax.ShapeDtypeStruct(own.shape, BF16),
        in_specs=[vmem] * 3,
        out_specs=vmem,
        compiler_params=pltpu.CompilerParams(vmem_limit_bytes=8 * 1024 * 1024),
    )(own, from_left, from_right)


def solution(mesh):
    axis = "ep"
    n_dev = mesh.shape[axis]
    rows_spec = P(("dp", "ep"), None)
    cube_spec = P(("dp", "ep"), None, None)
    weight_spec = P("ep", None, None)
    to_right = [(i, (i + 2) % n_dev) for i in range(n_dev)]
    to_left = [(i, (i - 2) % n_dev) for i in range(n_dev)]

    def local_step(grad_y, gate_vals, topk_idx, slot_ids, pair_counts, y_routed, x_disp, h_gate, h_up, w_gate, w_up, w_down):
        y_rows = y_routed.reshape(-1, y_routed.shape[2])
        d_rows, dh_rows, a_rows, gg, for_right, for_left, own = exchange(
            axis, n_dev, topk_idx.T, slot_ids.T, gate_vals.T, pair_counts, grad_y, y_rows, h_gate, h_up, w_gate, w_up, w_down)
        from_left = lax.ppermute(for_right, axis, to_right)
        from_right = lax.ppermute(for_left, axis, to_left)
        grad_wgate, grad_wup, grad_wdown, grad_gate = weight_grads(x_disp, dh_rows, a_rows, d_rows, gg)
        grad_x = final_sum(own, from_left, from_right)
        return grad_x, grad_gate.T, grad_wgate, grad_wup, grad_wdown

    return jax.shard_map(local_step, mesh=mesh, in_specs=(rows_spec, rows_spec, rows_spec, rows_spec, rows_spec, cube_spec, cube_spec, cube_spec, cube_spec, weight_spec, weight_spec, weight_spec), out_specs=(rows_spec, rows_spec, cube_spec, cube_spec, cube_spec), check_vma=False)
```

```python
import functools

import jax
import jax.numpy as jnp
from jax import lax
from jax.experimental import pallas as pl
from jax.experimental.pallas import tpu as pltpu
from jax.sharding import PartitionSpec as P

F32, BF16 = jnp.float32, jnp.bfloat16
COLS = 256
EXCHANGE_VMEM = 50 * 1024 * 1024
WEIGHT_VMEM = 24 * 1024 * 1024
OPP, LEFT, RIGHT, OWN = range(4)


def dot_last(a, b):
    return lax.dot_general(a, b, (((1,), (1,)), ((), ())), preferred_element_type=F32)


def dot_first(a, b):
    return lax.dot_general(a, b, (((0,), (0,)), ((), ())), preferred_element_type=F32)


def exchange_kernel(axis, n_dev, topk_ref, slot_ref, gate_ref, count_ref, gy_hbm, y_hbm, hg_hbm, hu_hbm, wg_hbm, wu_hbm, wd_hbm,
                    d_buf, dh_buf, a_buf, gg_out, right_out, left_out, own_out,
                    gy_all, route_send, route_all, y_buf, hg_buf, hu_buf, wgu_buf, wd_buf, f1_buf, s_buf,
                    oh_buf, r_buf, keep_buf, pair_send, pair_recv, hop_recv,
                    load_sem, route_ssem, route_rsem, gy_ssem, gy_rsem, pair_ssem, pair_rsem, hop_ssem, hop_rsem):
    n_loc, n_rows, ffn = hg_hbm.shape
    tok, model = gy_hbm.shape
    top_k = topk_ref.shape[0]
    cap = n_rows // n_dev
    n_exp = n_loc * n_dev
    half = tok // 2
    pair_rows = 2 * cap
    n_chip = n_dev // 2

    me = lax.axis_index(axis)
    chip = lax.div(me, 2)
    core = me - 2 * chip
    chips = [lax.rem(chip + step, n_chip) for step in (2, n_chip - 1, 1, 0)]
    homes = [2 * c + core for c in chips]
    others = [2 * c + 1 - core for c in chips]
    opp, left, right = homes[OPP], homes[LEFT], homes[RIGHT]
    sib = others[OWN]
    top, bottom = pl.ds(0, half), pl.ds(half, half)

    barrier = pltpu.get_barrier_semaphore()
    for step in range(1, n_dev):
        pl.semaphore_signal(barrier, inc=1, device_id={axis: lax.rem(me + step, n_dev)}, device_id_type=pl.DeviceIdType.MESH)

    loads = {}

    def load(name, src, dst):
        loads[name] = pltpu.make_async_copy(src, dst, load_sem.at[len(loads)])
        loads[name].start()

    load("gy", gy_hbm, gy_all.at[me])
    for e in range(n_loc):
        load(("hg", e), hg_hbm.at[e], hg_buf.at[e])
        load(("hu", e), hu_hbm.at[e], hu_buf.at[e])
    load("y", y_hbm, y_buf)
    load("wd", wd_hbm, wd_buf)
    load("wg", wg_hbm, wgu_buf.at[:, :, pl.ds(0, ffn)])
    load("wu", wu_hbm, wgu_buf.at[:, :, pl.ds(ffn, ffn)])

    topk_t = topk_ref[...].astype(F32)
    slot_t = slot_ref[...].astype(F32)
    gate_t = gate_ref[...]
    exp_iota = lax.broadcasted_iota(jnp.int32, (n_exp, tok), 0).astype(F32)
    diag = lax.broadcasted_iota(jnp.int32, (n_exp, n_exp), 0) == lax.broadcasted_iota(jnp.int32, (n_exp, n_exp), 1)
    count = jnp.sum(jnp.where(diag, count_ref[...].astype(F32), 0.0), axis=1, keepdims=True)
    slot_d = jnp.zeros((n_exp, tok), F32)
    gate_d = jnp.zeros((n_exp, tok), F32)
    for j in range(top_k):
        hit = topk_t[j : j + 1] == exp_iota
        slot_d += jnp.where(hit, slot_t[j : j + 1] + 1.0, 0.0)
        gate_d += jnp.where(hit, gate_t[j : j + 1], 0.0)
    slot_d -= 1.0
    slot_d = jnp.where(slot_d < count, slot_d, -1.0)
    for i in range(n_dev):
        route_send[i, 0:n_loc] = slot_d[i * n_loc : (i + 1) * n_loc]
        route_send[i, n_loc : 2 * n_loc] = gate_d[i * n_loc : (i + 1) * n_loc]
    route_all[me] = route_send[me]

    loads["gy"].wait()
    pl.semaphore_wait(barrier, n_dev - 1)

    def remote(src, dst, ssem, rsem, dev):
        return pltpu.make_async_remote_copy(src_ref=src, dst_ref=dst, send_sem=ssem, recv_sem=rsem, device_id={axis: dev}, device_id_type=pl.DeviceIdType.MESH)

    sends = []

    def gy_copy(block, part, send_slot, recv_slot, dev):
        ref = gy_all.at[block, part]
        return remote(ref, ref, gy_ssem.at[send_slot], gy_rsem.at[recv_slot], dev)

    def gy_send(block, part, recv_slot, dev):
        copy = gy_copy(block, part, recv_slot, recv_slot, dev)
        copy.start()
        sends.append(copy)

    def gy_wait(block, part, recv_slot):
        gy_copy(block, part, recv_slot, recv_slot, sib).wait_recv()

    gy_send(me, top, 0, right)
    gy_send(me, bottom, 2, left)
    gy_send(me, bottom, 1, right)
    gy_send(me, top, 3, left)
    gy_send(me, pl.ds(0, tok), 6, sib)
    for step in range(1, n_dev):
        dst = lax.rem(me + step, n_dev)
        copy = remote(route_send.at[dst], route_all.at[me], route_ssem.at[step - 1], route_rsem.at[step - 1], dst)
        copy.start()
        sends.append(copy)

    chunk = 32
    n_chunk = n_rows // chunk

    def factors(e):
        def body(i, carry):
            rows = pl.ds(pl.multiple_of(i * chunk, chunk), chunk)
            h1 = hg_buf[e, rows].astype(F32)
            h3 = hu_buf[e, rows].astype(F32)
            sig = jax.nn.sigmoid(h1)
            act = h1 * sig
            s_buf[e, rows] = act
            a_buf[e, rows] = (act * h3).astype(BF16)
            f1_buf[e, rows] = h3 * sig * (1.0 + h1 * (1.0 - sig))
            return carry

        loads[("hg", e)].wait()
        loads[("hu", e)].wait()
        lax.fori_loop(0, n_chunk, body, 0)

    factors(0)
    factors(1)

    gy_wait(left, top, 0)
    gy_send(left, top, 4, right)
    gy_send(left, top, 7, sib)
    gy_wait(right, bottom, 2)
    gy_send(right, bottom, 5, left)
    gy_send(right, bottom, 9, sib)

    factors(2)
    factors(3)

    gy_wait(left, bottom, 1)
    gy_send(left, bottom, 8, sib)
    gy_wait(right, top, 3)
    gy_send(right, top, 10, sib)

    loads["y"].wait()
    group = 32
    gg = jnp.zeros((top_k, tok), F32)
    tok_major = lax.broadcasted_iota(jnp.int32, (group, top_k, tok), 0)
    tok_lane = lax.broadcasted_iota(jnp.int32, (group, top_k, tok), 2)
    for i in range(tok // group):
        prod = dot_last(y_buf[pl.ds(i * group * top_k, group * top_k)], gy_all[me])
        gg += jnp.sum(jnp.where(tok_major + i * group == tok_lane, prod.reshape(group, top_k, tok), 0.0), axis=0)
    gg_out[...] = gg

    for step in range(1, n_dev):
        src = lax.rem(me + n_dev - step, n_dev)
        remote(route_send.at[src], route_all.at[src], route_ssem.at[step - 1], route_rsem.at[step - 1], src).wait_recv()

    gy_wait(opp, top, 4)
    gy_send(opp, top, 11, sib)
    gy_wait(opp, bottom, 5)
    gy_send(opp, bottom, 12, sib)

    slot_iota = lax.broadcasted_iota(jnp.int32, (cap, tok), 0).astype(F32)

    def build_rows(s):
        route = route_all[s]
        gates = []
        for e in range(n_loc):
            hit = route[e : e + 1] == slot_iota
            oh_buf[s, pl.ds(e * cap, cap)] = jnp.where(hit, 1.0, 0.0).astype(BF16)
            gates.append(jnp.sum(jnp.where(hit, route[n_loc + e : n_loc + e + 1], 0.0), axis=1, keepdims=True))
        gate = jnp.concatenate(gates, axis=0)
        pick = oh_buf[s]
        for n in range(0, model, COLS):
            rows = (jnp.dot(pick, gy_all[s, :, pl.ds(n, COLS)], preferred_element_type=F32) * gate).astype(BF16)
            for e in range(n_loc):
                d_buf[e, pl.ds(pl.multiple_of(s * cap, cap), cap), pl.ds(n, COLS)] = rows[e * cap : (e + 1) * cap]

    def rows_of(c):
        return pl.ds(pl.multiple_of(c * pair_rows, pair_rows), pair_rows)

    def experts(which, lo, hi):
        def body(e, carry):
            d_rows = jnp.concatenate([d_buf[e, rows_of(c)] for c in which], axis=0)
            for n in range(0, ffn, COLS):
                grad = dot_last(d_rows, wd_buf[e, pl.ds(n, COLS)]).astype(BF16).astype(F32)
                for i, c in enumerate(which):
                    part = grad[i * pair_rows : (i + 1) * pair_rows]
                    dh_buf[e, rows_of(c), pl.ds(n, COLS)] = (part * f1_buf[e, rows_of(c), pl.ds(n, COLS)]).astype(BF16)
                    dh_buf[e, rows_of(c), pl.ds(ffn + n, COLS)] = (part * s_buf[e, rows_of(c), pl.ds(n, COLS)]).astype(BF16)
            dh_rows = jnp.concatenate([dh_buf[e, rows_of(c)] for c in which], axis=0)
            out_rows = pl.ds(pl.multiple_of(e * cap, cap), cap)
            for n in range(0, model, COLS):
                ret = dot_last(dh_rows, wgu_buf[e, pl.ds(n, COLS)]).astype(BF16)
                for i, c in enumerate(which):
                    for k in range(2):
                        lo_row = i * pair_rows + k * cap
                        r_buf[2 * c + k, out_rows, pl.ds(n, COLS)] = ret[lo_row : lo_row + cap]
            return carry

        lax.fori_loop(lo, hi, body, 0)

    def sum_rows(s, dst):
        pick = oh_buf[s]
        for n in range(0, model, COLS):
            dst[:, pl.ds(n, COLS)] = dot_first(pick, r_buf[s, :, pl.ds(n, COLS)])

    pairs = {}

    def finish(role):
        sum_rows(others[role], pair_send.at[role])
        pairs[role] = remote(pair_send.at[role], pair_recv.at[role], pair_ssem.at[role], pair_rsem.at[role], sib)
        pairs[role].start()
        sends.append(pairs[role])
        sum_rows(homes[role], keep_buf.at[role])

    loads["wd"].wait()
    gy_wait(others[OPP], top, 11)
    gy_wait(others[OPP], bottom, 12)
    build_rows(homes[OPP])
    build_rows(others[OPP])
    loads["wg"].wait()
    loads["wu"].wait()
    experts([chips[OPP]], 0, n_loc)
    finish(OPP)

    gy_wait(others[LEFT], top, 7)
    gy_wait(others[LEFT], bottom, 8)
    gy_wait(others[RIGHT], bottom, 9)
    gy_wait(others[RIGHT], top, 10)
    for role in (LEFT, RIGHT):
        build_rows(homes[role])
        build_rows(others[role])
    experts([chips[LEFT], chips[RIGHT]], 0, n_loc // 2)

    pairs[OPP].wait_recv()
    keep_buf[OPP] = keep_buf[OPP] + pair_recv[OPP]
    hop_right = remote(keep_buf.at[OPP, top], hop_recv.at[0], hop_ssem.at[0], hop_rsem.at[0], right)
    hop_right.start()
    hop_left = remote(keep_buf.at[OPP, bottom], hop_recv.at[1], hop_ssem.at[1], hop_rsem.at[1], left)
    hop_left.start()
    sends.extend([hop_right, hop_left])

    experts([chips[LEFT], chips[RIGHT]], n_loc // 2, n_loc)
    finish(LEFT)
    finish(RIGHT)

    gy_wait(others[OWN], pl.ds(0, tok), 6)
    build_rows(homes[OWN])
    build_rows(others[OWN])
    experts([chips[OWN]], 0, n_loc)
    finish(OWN)

    pairs[LEFT].wait_recv()
    pairs[RIGHT].wait_recv()
    right_out[bottom] = keep_buf[RIGHT, bottom] + pair_recv[RIGHT, bottom]
    left_out[top] = keep_buf[LEFT, top] + pair_recv[LEFT, top]
    pairs[OWN].wait_recv()
    own_out[...] = keep_buf[OWN] + pair_recv[OWN]
    hop_right.wait_recv()
    right_out[top] = keep_buf[RIGHT, top] + pair_recv[RIGHT, top] + hop_recv[0]
    hop_left.wait_recv()
    left_out[bottom] = keep_buf[LEFT, bottom] + pair_recv[LEFT, bottom] + hop_recv[1]

    for copy in sends:
        copy.wait_send()


def exchange(axis, n_dev, topk_idx, slot_ids, gate_vals, pair_counts, grad_y, y_rows, h_gate, h_up, w_gate, w_up, w_down):
    n_loc, n_rows, ffn = h_gate.shape
    tok, model = grad_y.shape
    top_k = topk_idx.shape[0]
    cap = n_rows // n_dev
    vmem = pl.BlockSpec(memory_space=pltpu.VMEM)
    hbm = pl.BlockSpec(memory_space=pl.ANY)
    dma = pltpu.SemaphoreType.DMA
    part = pltpu.VMEM((tok, model), F32)
    return pl.pallas_call(
        functools.partial(exchange_kernel, axis, n_dev),
        name="exchange",
        out_shape=(
            pltpu.VMEM((n_loc, n_rows, model), BF16),
            pltpu.VMEM((n_loc, n_rows, 2 * ffn), BF16),
            pltpu.VMEM((n_loc, n_rows, ffn), BF16),
            pltpu.VMEM((top_k, tok), F32),
            part, part, part,
        ),
        in_specs=[vmem] * 4 + [hbm] * 7,
        out_specs=(vmem,) * 7,
        scratch_shapes=[
            pltpu.VMEM((n_dev, tok, model), BF16),
            pltpu.VMEM((n_dev, 2 * n_loc, tok), F32),
            pltpu.VMEM((n_dev, 2 * n_loc, tok), F32),
            pltpu.VMEM(y_rows.shape, BF16),
            pltpu.VMEM(h_gate.shape, BF16),
            pltpu.VMEM(h_up.shape, BF16),
            pltpu.VMEM((n_loc, model, 2 * ffn), BF16),
            pltpu.VMEM(w_down.shape, BF16),
            pltpu.VMEM(h_gate.shape, F32),
            pltpu.VMEM(h_gate.shape, F32),
            pltpu.VMEM((n_dev, n_loc * cap, tok), BF16),
            pltpu.VMEM((n_dev, n_loc * cap, model), BF16),
            pltpu.VMEM((4, tok, model), F32),
            pltpu.VMEM((4, tok, model), F32),
            pltpu.VMEM((4, tok, model), F32),
            pltpu.VMEM((2, tok // 2, model), F32),
            dma((5 + 2 * n_loc,)), dma((n_dev - 1,)), dma((n_dev - 1,)), dma((13,)), dma((13,)),
            dma((4,)), dma((4,)), dma((2,)), dma((2,)),
        ],
        compiler_params=pltpu.CompilerParams(collective_id=0, has_side_effects=True, vmem_limit_bytes=EXCHANGE_VMEM),
    )(topk_idx, slot_ids, gate_vals, pair_counts, grad_y, y_rows, h_gate, h_up, w_gate, w_up, w_down)


def weight_kernel(x_hbm, dh_buf, a_buf, d_buf, gg_ref, wg_hbm, wu_hbm, wd_hbm, gg_out, x_buf, wg_buf, wu_buf, wd_buf, in_sem, out_sem):
    n_loc, ffn, model = a_buf.shape[0], a_buf.shape[2], d_buf.shape[2]
    gg_out[...] = gg_ref[...]
    ins = []
    for e in range(n_loc):
        ins.append(pltpu.make_async_copy(x_hbm.at[e], x_buf.at[e], in_sem.at[e]))
        ins[e].start()
    outs = {}

    def store(key, src, dst, sem):
        outs[key] = pltpu.make_async_copy(src, dst, sem)
        outs[key].start()

    for e in range(n_loc):
        slot = e % 2
        for k in range(3):
            if (slot, k) in outs:
                outs.pop((slot, k)).wait()
        for n in range(0, model, COLS):
            wd_buf[slot, :, pl.ds(n, COLS)] = dot_first(a_buf[e], d_buf[e, :, pl.ds(n, COLS)])
        store((slot, 0), wd_buf.at[slot], wd_hbm.at[e], out_sem.at[slot, 0])
        ins[e].wait()
        for n in range(0, ffn, COLS):
            wg_buf[slot, :, pl.ds(n, COLS)] = dot_first(x_buf[e], dh_buf[e, :, pl.ds(n, COLS)])
        store((slot, 1), wg_buf.at[slot], wg_hbm.at[e], out_sem.at[slot, 1])
        for n in range(0, ffn, COLS):
            wu_buf[slot, :, pl.ds(n, COLS)] = dot_first(x_buf[e], dh_buf[e, :, pl.ds(ffn + n, COLS)])
        store((slot, 2), wu_buf.at[slot], wu_hbm.at[e], out_sem.at[slot, 2])
    for copy in outs.values():
        copy.wait()


def weight_grads(x_disp, dh_rows, a_rows, d_rows, gg):
    n_loc, n_rows, model = x_disp.shape
    ffn = a_rows.shape[2]
    flops = 2 * n_loc * n_rows * model * 3 * ffn
    moved = 2 * x_disp.size + 12 * n_loc * model * ffn
    vmem = pl.BlockSpec(memory_space=pltpu.VMEM)
    hbm = pl.BlockSpec(memory_space=pl.ANY)
    return pl.pallas_call(
        weight_kernel,
        name="weight_grads",
        in_specs=[hbm] + [vmem] * 4,
        out_specs=(hbm, hbm, hbm, vmem),
        out_shape=(
            jax.ShapeDtypeStruct((n_loc, model, ffn), F32),
            jax.ShapeDtypeStruct((n_loc, model, ffn), F32),
            jax.ShapeDtypeStruct((n_loc, ffn, model), F32),
            jax.ShapeDtypeStruct(gg.shape, F32),
        ),
        scratch_shapes=[
            pltpu.VMEM(x_disp.shape, BF16),
            pltpu.VMEM((2, model, ffn), F32),
            pltpu.VMEM((2, model, ffn), F32),
            pltpu.VMEM((2, ffn, model), F32),
            pltpu.SemaphoreType.DMA((n_loc,)),
            pltpu.SemaphoreType.DMA((2, 3)),
        ],
        cost_estimate=pl.CostEstimate(flops=flops, bytes_accessed=moved, transcendentals=0),
        compiler_params=pltpu.CompilerParams(vmem_limit_bytes=WEIGHT_VMEM),
    )(pltpu.with_memory_space_constraint(x_disp, pltpu.HBM), *(pltpu.with_memory_space_constraint(rows, pltpu.VMEM) for rows in (dh_rows, a_rows, d_rows, gg)))


def final_kernel(own_ref, left_ref, right_ref, gx_out):
    gx_out[...] = (own_ref[...] + left_ref[...] + right_ref[...]).astype(BF16)


def final_sum(own, from_left, from_right):
    vmem = pl.BlockSpec(memory_space=pltpu.VMEM)
    return pl.pallas_call(
        final_kernel,
        name="final_sum",
        out_shape=jax.ShapeDtypeStruct(own.shape, BF16),
        in_specs=[vmem] * 3,
        out_specs=vmem,
        compiler_params=pltpu.CompilerParams(vmem_limit_bytes=8 * 1024 * 1024),
    )(*(pltpu.with_memory_space_constraint(part, pltpu.VMEM) for part in (own, from_left, from_right)))


def solution(mesh):
    axis = "ep"
    n_dev = mesh.shape[axis]
    rows_spec = P(("dp", "ep"), None)
    cube_spec = P(("dp", "ep"), None, None)
    weight_spec = P("ep", None, None)
    to_right = [(i, (i + 2) % n_dev) for i in range(n_dev)]
    to_left = [(i, (i - 2) % n_dev) for i in range(n_dev)]

    def local_step(grad_y, gate_vals, topk_idx, slot_ids, pair_counts, y_routed, x_disp, h_gate, h_up, w_gate, w_up, w_down):
        y_rows = y_routed.reshape(-1, y_routed.shape[2])
        d_rows, dh_rows, a_rows, gg, for_right, for_left, own = exchange(
            axis, n_dev, topk_idx.T, slot_ids.T, gate_vals.T, pair_counts, grad_y, y_rows, h_gate, h_up, w_gate, w_up, w_down)
        from_left = lax.ppermute(for_right, axis, to_right)
        from_right = lax.ppermute(for_left, axis, to_left)
        grad_wgate, grad_wup, grad_wdown, grad_gate = weight_grads(x_disp, dh_rows, a_rows, d_rows, gg)
        grad_x = final_sum(own, from_left, from_right)
        return grad_x, grad_gate.T, grad_wgate, grad_wup, grad_wdown

    return jax.shard_map(local_step, mesh=mesh, in_specs=(rows_spec, rows_spec, rows_spec, rows_spec, rows_spec, cube_spec, cube_spec, cube_spec, cube_spec, weight_spec, weight_spec, weight_spec), out_specs=(rows_spec, rows_spec, cube_spec, cube_spec, cube_spec), check_vma=False)
```

```python
import functools

import jax
import jax.numpy as jnp
from jax import lax
from jax.experimental import pallas as pl
from jax.experimental.pallas import tpu as pltpu
from jax.sharding import PartitionSpec as P

F32, BF16 = jnp.float32, jnp.bfloat16
COLS = 256
EXCHANGE_VMEM = 50 * 1024 * 1024
WEIGHT_VMEM = 24 * 1024 * 1024
OPP, LEFT, RIGHT, OWN = range(4)


def dot_last(a, b):
    return lax.dot_general(a, b, (((1,), (1,)), ((), ())), preferred_element_type=F32)


def dot_first(a, b):
    return lax.dot_general(a, b, (((0,), (0,)), ((), ())), preferred_element_type=F32)


def exchange_kernel(axis, n_dev, topk_ref, slot_ref, gate_ref, count_ref, gy_hbm, y_hbm, hg_hbm, hu_hbm, wg_hbm, wu_hbm, wd_hbm,
                    d_buf, dh_buf, a_buf, gg_out, right_out, left_out, own_out,
                    gy_all, route_send, route_all, y_buf, hg_buf, hu_buf, wgu_buf, wd_buf, f1_buf, s_buf,
                    oh_buf, r_buf, pair_send, pair_recv, opp_send, opp_keep, opp_recv, hop_recv,
                    load_sem, route_ssem, route_rsem, gy_ssem, gy_rsem, pair_ssem, pair_rsem, hop_ssem, hop_rsem):
    n_loc, n_rows, ffn = hg_hbm.shape
    tok, model = gy_hbm.shape
    top_k = topk_ref.shape[0]
    cap = n_rows // n_dev
    n_exp = n_loc * n_dev
    half = tok // 2
    pair_rows = 2 * cap
    n_chip = n_dev // 2

    me = lax.axis_index(axis)
    chip = lax.div(me, 2)
    core = me - 2 * chip
    chips = [lax.rem(chip + step, n_chip) for step in (2, n_chip - 1, 1, 0)]
    homes = [2 * c + core for c in chips]
    others = [2 * c + 1 - core for c in chips]
    opp, left, right = homes[OPP], homes[LEFT], homes[RIGHT]
    sib = others[OWN]
    top, bottom = pl.ds(0, half), pl.ds(half, half)

    barrier = pltpu.get_barrier_semaphore()
    for step in range(1, n_dev):
        pl.semaphore_signal(barrier, inc=1, device_id={axis: lax.rem(me + step, n_dev)}, device_id_type=pl.DeviceIdType.MESH)

    loads = {}

    def load(name, src, dst):
        loads[name] = pltpu.make_async_copy(src, dst, load_sem.at[len(loads)])
        loads[name].start()

    load("gy", gy_hbm, gy_all.at[me])
    for e in range(n_loc):
        load(("hg", e), hg_hbm.at[e], hg_buf.at[e])
        load(("hu", e), hu_hbm.at[e], hu_buf.at[e])
    load("y", y_hbm, y_buf)
    load("wd", wd_hbm, wd_buf)
    load("wg", wg_hbm, wgu_buf.at[:, :, pl.ds(0, ffn)])
    load("wu", wu_hbm, wgu_buf.at[:, :, pl.ds(ffn, ffn)])

    topk_t = topk_ref[...].astype(F32)
    slot_t = slot_ref[...].astype(F32)
    gate_t = gate_ref[...]
    exp_iota = lax.broadcasted_iota(jnp.int32, (n_exp, tok), 0).astype(F32)
    diag = lax.broadcasted_iota(jnp.int32, (n_exp, n_exp), 0) == lax.broadcasted_iota(jnp.int32, (n_exp, n_exp), 1)
    count = jnp.sum(jnp.where(diag, count_ref[...].astype(F32), 0.0), axis=1, keepdims=True)
    slot_d = jnp.zeros((n_exp, tok), F32)
    gate_d = jnp.zeros((n_exp, tok), F32)
    for j in range(top_k):
        hit = topk_t[j : j + 1] == exp_iota
        slot_d += jnp.where(hit, slot_t[j : j + 1] + 1.0, 0.0)
        gate_d += jnp.where(hit, gate_t[j : j + 1], 0.0)
    slot_d -= 1.0
    slot_d = jnp.where(slot_d < count, slot_d, -1.0)
    for i in range(n_dev):
        route_send[i, 0:n_loc] = slot_d[i * n_loc : (i + 1) * n_loc]
        route_send[i, n_loc : 2 * n_loc] = gate_d[i * n_loc : (i + 1) * n_loc]
    route_all[me] = route_send[me]

    loads["gy"].wait()
    pl.semaphore_wait(barrier, n_dev - 1)

    def remote(src, dst, ssem, rsem, dev):
        return pltpu.make_async_remote_copy(src_ref=src, dst_ref=dst, send_sem=ssem, recv_sem=rsem, device_id={axis: dev}, device_id_type=pl.DeviceIdType.MESH)

    sends = []

    def gy_copy(block, part, send_slot, recv_slot, dev):
        ref = gy_all.at[block, part]
        return remote(ref, ref, gy_ssem.at[send_slot], gy_rsem.at[recv_slot], dev)

    def gy_send(block, part, recv_slot, dev):
        copy = gy_copy(block, part, recv_slot, recv_slot, dev)
        copy.start()
        sends.append(copy)

    def gy_wait(block, part, recv_slot):
        gy_copy(block, part, recv_slot, recv_slot, sib).wait_recv()

    gy_send(me, top, 0, right)
    gy_send(me, bottom, 2, left)
    gy_send(me, bottom, 1, right)
    gy_send(me, top, 3, left)
    gy_send(me, pl.ds(0, tok), 6, sib)
    for step in range(1, n_dev):
        dst = lax.rem(me + step, n_dev)
        copy = remote(route_send.at[dst], route_all.at[me], route_ssem.at[step - 1], route_rsem.at[step - 1], dst)
        copy.start()
        sends.append(copy)

    chunk = 32
    n_chunk = n_rows // chunk

    def factors(e):
        def body(i, carry):
            rows = pl.ds(pl.multiple_of(i * chunk, chunk), chunk)
            h1 = hg_buf[e, rows].astype(F32)
            h3 = hu_buf[e, rows].astype(F32)
            sig = jax.nn.sigmoid(h1)
            act = h1 * sig
            s_buf[e, rows] = act
            a_buf[e, rows] = (act * h3).astype(BF16)
            f1_buf[e, rows] = h3 * sig * (1.0 + h1 * (1.0 - sig))
            return carry

        loads[("hg", e)].wait()
        loads[("hu", e)].wait()
        lax.fori_loop(0, n_chunk, body, 0)

    for e in range(n_loc):
        factors(e)

    loads["y"].wait()
    group = 32
    gg = jnp.zeros((top_k, tok), F32)
    tok_major = lax.broadcasted_iota(jnp.int32, (group, top_k, tok), 0)
    tok_lane = lax.broadcasted_iota(jnp.int32, (group, top_k, tok), 2)
    for i in range(tok // group):
        prod = dot_last(y_buf[pl.ds(i * group * top_k, group * top_k)], gy_all[me])
        gg += jnp.sum(jnp.where(tok_major + i * group == tok_lane, prod.reshape(group, top_k, tok), 0.0), axis=0)
    gg_out[...] = gg

    for step in range(1, n_dev):
        src = lax.rem(me + n_dev - step, n_dev)
        remote(route_send.at[src], route_all.at[src], route_ssem.at[step - 1], route_rsem.at[step - 1], src).wait_recv()

    slot_iota = lax.broadcasted_iota(jnp.int32, (cap, tok), 0).astype(F32)

    def build_rows(s):
        route = route_all[s]
        gates = []
        for e in range(n_loc):
            hit = route[e : e + 1] == slot_iota
            oh_buf[s, pl.ds(e * cap, cap)] = jnp.where(hit, 1.0, 0.0).astype(BF16)
            gates.append(jnp.sum(jnp.where(hit, route[n_loc + e : n_loc + e + 1], 0.0), axis=1, keepdims=True))
        gate = jnp.concatenate(gates, axis=0)
        pick = oh_buf[s]
        for n in range(0, model, COLS):
            rows = (jnp.dot(pick, gy_all[s, :, pl.ds(n, COLS)], preferred_element_type=F32) * gate).astype(BF16)
            for e in range(n_loc):
                d_buf[e, pl.ds(pl.multiple_of(s * cap, cap), cap), pl.ds(n, COLS)] = rows[e * cap : (e + 1) * cap]

    def rows_of(c):
        return pl.ds(pl.multiple_of(c * pair_rows, pair_rows), pair_rows)

    def hidden_grads(roles):
        which = [chips[role] for role in roles]

        def body(e, carry):
            d_rows = jnp.concatenate([d_buf[e, rows_of(c)] for c in which], axis=0)
            for n in range(0, ffn, COLS):
                grad = dot_last(d_rows, wd_buf[e, pl.ds(n, COLS)]).astype(BF16).astype(F32)
                for i, c in enumerate(which):
                    part = grad[i * pair_rows : (i + 1) * pair_rows]
                    dh_buf[e, rows_of(c), pl.ds(n, COLS)] = (part * f1_buf[e, rows_of(c), pl.ds(n, COLS)]).astype(BF16)
                    dh_buf[e, rows_of(c), pl.ds(ffn + n, COLS)] = (part * s_buf[e, rows_of(c), pl.ds(n, COLS)]).astype(BF16)
            return carry

        lax.fori_loop(0, n_loc, body, 0)

    def returned(roles, lo, hi, cols):
        which = [chips[role] for role in roles]

        def body(e, carry):
            dh_rows = jnp.concatenate([dh_buf[e, rows_of(c)] for c in which], axis=0)
            out_rows = pl.ds(pl.multiple_of(e * cap, cap), cap)
            for n in cols:
                ret = dot_last(dh_rows, wgu_buf[e, pl.ds(n, COLS)]).astype(BF16)
                for i, c in enumerate(which):
                    for k in range(2):
                        lo_row = i * pair_rows + k * cap
                        r_buf[2 * c + k, out_rows, pl.ds(n, COLS)] = ret[lo_row : lo_row + cap]
            return carry

        lax.fori_loop(lo, hi, body, 0)

    all_cols = range(0, model, COLS)

    def token_sum(s, n):
        return dot_first(oh_buf[s], r_buf[s, :, pl.ds(n, COLS)])

    pairs = {}

    def send_pair(key, slot, ref_send, ref_recv):
        pairs[key] = remote(ref_send, ref_recv, pair_ssem.at[slot], pair_rsem.at[slot], sib)
        pairs[key].start()
        sends.append(pairs[key])

    def finish(role, out):
        for n in all_cols:
            pair_send[role, :, pl.ds(n, COLS)] = token_sum(others[role], n)
        send_pair(role, role, pair_send.at[role], pair_recv.at[role])
        for n in all_cols:
            out[:, pl.ds(n, COLS)] = token_sum(homes[role], n)

    loads["wd"].wait()
    gy_wait(others[OWN], pl.ds(0, tok), 6)
    build_rows(homes[OWN])
    build_rows(others[OWN])
    hidden_grads([OWN])

    gy_wait(left, top, 0)
    gy_send(left, top, 4, right)
    gy_send(left, top, 7, sib)
    gy_wait(right, bottom, 2)
    gy_send(right, bottom, 5, left)
    gy_send(right, bottom, 9, sib)

    loads["wg"].wait()
    loads["wu"].wait()
    returned([OWN], 0, n_loc - 1, all_cols)

    gy_wait(left, bottom, 1)
    gy_send(left, bottom, 8, sib)
    gy_wait(right, top, 3)
    gy_send(right, top, 10, sib)

    returned([OWN], n_loc - 1, n_loc, all_cols)
    finish(OWN, own_out)

    build_rows(homes[LEFT])
    build_rows(homes[RIGHT])
    gy_wait(others[LEFT], top, 7)
    gy_wait(others[LEFT], bottom, 8)
    build_rows(others[LEFT])
    gy_wait(others[RIGHT], bottom, 9)
    gy_wait(others[RIGHT], top, 10)
    build_rows(others[RIGHT])

    gy_wait(opp, top, 4)
    gy_send(opp, top, 11, sib)
    gy_wait(opp, bottom, 5)
    gy_send(opp, bottom, 12, sib)

    hidden_grads([LEFT, RIGHT])

    build_rows(homes[OPP])
    gy_wait(others[OPP], top, 11)
    gy_wait(others[OPP], bottom, 12)
    build_rows(others[OPP])
    hidden_grads([OPP])

    hops = []

    def hop(i):
        pairs[OPP, i].wait_recv()
        opp_keep[i] = opp_keep[i] + opp_recv[i]
        for k, (part, dev) in enumerate(((top, right), (bottom, left))):
            copy = remote(opp_keep.at[i, part], hop_recv.at[k, i], hop_ssem.at[k, i], hop_rsem.at[k, i], dev)
            copy.start()
            sends.append(copy)
            hops.append((k, i, copy))

    for i, n in enumerate(all_cols):
        returned([OPP], 0, n_loc, [n])
        opp_send[i] = token_sum(others[OPP], n)
        send_pair((OPP, i), 4 + i, opp_send.at[i], opp_recv.at[i])
        opp_keep[i] = token_sum(homes[OPP], n)
        if i:
            hop(i - 1)

    half_loc = n_loc // 2
    returned([LEFT, RIGHT], 0, half_loc, all_cols)
    hop(model // COLS - 1)
    returned([LEFT, RIGHT], half_loc, n_loc, all_cols)
    finish(LEFT, left_out)
    finish(RIGHT, right_out)

    pairs[OWN].wait_recv()
    own_out[...] = own_out[...] + pair_recv[OWN]
    pairs[LEFT].wait_recv()
    left_out[...] = left_out[...] + pair_recv[LEFT]
    pairs[RIGHT].wait_recv()
    right_out[...] = right_out[...] + pair_recv[RIGHT]
    for k, i, copy in hops:
        copy.wait_recv()
        out, part = ((right_out, top), (left_out, bottom))[k]
        cols = pl.ds(i * COLS, COLS)
        out[part, cols] = out[part, cols] + hop_recv[k, i]

    for copy in sends:
        copy.wait_send()


def exchange(axis, n_dev, topk_idx, slot_ids, gate_vals, pair_counts, grad_y, y_rows, h_gate, h_up, w_gate, w_up, w_down):
    n_loc, n_rows, ffn = h_gate.shape
    tok, model = grad_y.shape
    top_k = topk_idx.shape[0]
    cap = n_rows // n_dev
    vmem = pl.BlockSpec(memory_space=pltpu.VMEM)
    hbm = pl.BlockSpec(memory_space=pl.ANY)
    dma = pltpu.SemaphoreType.DMA
    part = pltpu.VMEM((tok, model), F32)
    return pl.pallas_call(
        functools.partial(exchange_kernel, axis, n_dev),
        name="exchange",
        out_shape=(
            pltpu.VMEM((n_loc, n_rows, model), BF16),
            pltpu.VMEM((n_loc, n_rows, 2 * ffn), BF16),
            pltpu.VMEM((n_loc, n_rows, ffn), BF16),
            pltpu.VMEM((top_k, tok), F32),
            part, part, part,
        ),
        in_specs=[vmem] * 4 + [hbm] * 7,
        out_specs=(vmem,) * 7,
        scratch_shapes=[
            pltpu.VMEM((n_dev, tok, model), BF16),
            pltpu.VMEM((n_dev, 2 * n_loc, tok), F32),
            pltpu.VMEM((n_dev, 2 * n_loc, tok), F32),
            pltpu.VMEM(y_rows.shape, BF16),
            pltpu.VMEM(h_gate.shape, BF16),
            pltpu.VMEM(h_up.shape, BF16),
            pltpu.VMEM((n_loc, model, 2 * ffn), BF16),
            pltpu.VMEM(w_down.shape, BF16),
            pltpu.VMEM(h_gate.shape, F32),
            pltpu.VMEM(h_gate.shape, F32),
            pltpu.VMEM((n_dev, n_loc * cap, tok), BF16),
            pltpu.VMEM((n_dev, n_loc * cap, model), BF16),
            pltpu.VMEM((4, tok, model), F32),
            pltpu.VMEM((4, tok, model), F32),
            pltpu.VMEM((model // COLS, tok, COLS), F32),
            pltpu.VMEM((model // COLS, tok, COLS), F32),
            pltpu.VMEM((model // COLS, tok, COLS), F32),
            pltpu.VMEM((2, model // COLS, tok // 2, COLS), F32),
            dma((5 + 2 * n_loc,)), dma((n_dev - 1,)), dma((n_dev - 1,)), dma((13,)), dma((13,)),
            dma((4 + model // COLS,)), dma((4 + model // COLS,)), dma((2, model // COLS)), dma((2, model // COLS)),
        ],
        compiler_params=pltpu.CompilerParams(collective_id=0, has_side_effects=True, vmem_limit_bytes=EXCHANGE_VMEM),
    )(topk_idx, slot_ids, gate_vals, pair_counts, grad_y, y_rows, h_gate, h_up, w_gate, w_up, w_down)


def weight_kernel(x_hbm, dh_buf, a_buf, d_buf, gg_ref, wg_hbm, wu_hbm, wd_hbm, gg_out, x_buf, wg_buf, wu_buf, wd_buf, in_sem, out_sem):
    n_loc, ffn, model = a_buf.shape[0], a_buf.shape[2], d_buf.shape[2]
    gg_out[...] = gg_ref[...]
    ins = []
    for e in range(n_loc):
        ins.append(pltpu.make_async_copy(x_hbm.at[e], x_buf.at[e], in_sem.at[e]))
        ins[e].start()
    outs = {}

    def store(key, src, dst, sem):
        outs[key] = pltpu.make_async_copy(src, dst, sem)
        outs[key].start()

    for e in range(n_loc):
        slot = e % 2
        for k in range(3):
            if (slot, k) in outs:
                outs.pop((slot, k)).wait()
        for n in range(0, model, COLS):
            wd_buf[slot, :, pl.ds(n, COLS)] = dot_first(a_buf[e], d_buf[e, :, pl.ds(n, COLS)])
        store((slot, 0), wd_buf.at[slot], wd_hbm.at[e], out_sem.at[slot, 0])
        ins[e].wait()
        for n in range(0, ffn, COLS):
            wg_buf[slot, :, pl.ds(n, COLS)] = dot_first(x_buf[e], dh_buf[e, :, pl.ds(n, COLS)])
        store((slot, 1), wg_buf.at[slot], wg_hbm.at[e], out_sem.at[slot, 1])
        for n in range(0, ffn, COLS):
            wu_buf[slot, :, pl.ds(n, COLS)] = dot_first(x_buf[e], dh_buf[e, :, pl.ds(ffn + n, COLS)])
        store((slot, 2), wu_buf.at[slot], wu_hbm.at[e], out_sem.at[slot, 2])
    for copy in outs.values():
        copy.wait()


def weight_grads(x_disp, dh_rows, a_rows, d_rows, gg):
    n_loc, n_rows, model = x_disp.shape
    ffn = a_rows.shape[2]
    flops = 2 * n_loc * n_rows * model * 3 * ffn
    moved = 2 * x_disp.size + 12 * n_loc * model * ffn
    vmem = pl.BlockSpec(memory_space=pltpu.VMEM)
    hbm = pl.BlockSpec(memory_space=pl.ANY)
    return pl.pallas_call(
        weight_kernel,
        name="weight_grads",
        in_specs=[hbm] + [vmem] * 4,
        out_specs=(hbm, hbm, hbm, vmem),
        out_shape=(
            jax.ShapeDtypeStruct((n_loc, model, ffn), F32),
            jax.ShapeDtypeStruct((n_loc, model, ffn), F32),
            jax.ShapeDtypeStruct((n_loc, ffn, model), F32),
            jax.ShapeDtypeStruct(gg.shape, F32),
        ),
        scratch_shapes=[
            pltpu.VMEM(x_disp.shape, BF16),
            pltpu.VMEM((2, model, ffn), F32),
            pltpu.VMEM((2, model, ffn), F32),
            pltpu.VMEM((2, ffn, model), F32),
            pltpu.SemaphoreType.DMA((n_loc,)),
            pltpu.SemaphoreType.DMA((2, 3)),
        ],
        cost_estimate=pl.CostEstimate(flops=flops, bytes_accessed=moved, transcendentals=0),
        compiler_params=pltpu.CompilerParams(vmem_limit_bytes=WEIGHT_VMEM),
    )(pltpu.with_memory_space_constraint(x_disp, pltpu.HBM), *(pltpu.with_memory_space_constraint(rows, pltpu.VMEM) for rows in (dh_rows, a_rows, d_rows, gg)))


def final_kernel(own_ref, left_ref, right_ref, gx_out):
    gx_out[...] = (own_ref[...] + left_ref[...] + right_ref[...]).astype(BF16)


def final_sum(own, from_left, from_right):
    vmem = pl.BlockSpec(memory_space=pltpu.VMEM)
    return pl.pallas_call(
        final_kernel,
        name="final_sum",
        out_shape=jax.ShapeDtypeStruct(own.shape, BF16),
        in_specs=[vmem] * 3,
        out_specs=vmem,
        compiler_params=pltpu.CompilerParams(vmem_limit_bytes=8 * 1024 * 1024),
    )(*(pltpu.with_memory_space_constraint(part, pltpu.VMEM) for part in (own, from_left, from_right)))


def solution(mesh):
    axis = "ep"
    n_dev = mesh.shape[axis]
    rows_spec = P(("dp", "ep"), None)
    cube_spec = P(("dp", "ep"), None, None)
    weight_spec = P("ep", None, None)
    to_right = [(i, (i + 2) % n_dev) for i in range(n_dev)]
    to_left = [(i, (i - 2) % n_dev) for i in range(n_dev)]

    def local_step(grad_y, gate_vals, topk_idx, slot_ids, pair_counts, y_routed, x_disp, h_gate, h_up, w_gate, w_up, w_down):
        y_rows = y_routed.reshape(-1, y_routed.shape[2])
        d_rows, dh_rows, a_rows, gg, for_right, for_left, own = exchange(
            axis, n_dev, topk_idx.T, slot_ids.T, gate_vals.T, pair_counts, grad_y, y_rows, h_gate, h_up, w_gate, w_up, w_down)
        from_left = lax.ppermute(for_right, axis, to_right)
        from_right = lax.ppermute(for_left, axis, to_left)
        grad_wgate, grad_wup, grad_wdown, grad_gate = weight_grads(x_disp, dh_rows, a_rows, d_rows, gg)
        grad_x = final_sum(own, from_left, from_right)
        return grad_x, grad_gate.T, grad_wgate, grad_wup, grad_wdown

    return jax.shard_map(local_step, mesh=mesh, in_specs=(rows_spec, rows_spec, rows_spec, rows_spec, rows_spec, cube_spec, cube_spec, cube_spec, cube_spec, weight_spec, weight_spec, weight_spec), out_specs=(rows_spec, rows_spec, cube_spec, cube_spec, cube_spec), check_vma=False)
```

```python
import functools

import jax
import jax.numpy as jnp
from jax import lax
from jax.experimental import pallas as pl
from jax.experimental.pallas import tpu as pltpu
from jax.sharding import PartitionSpec as P

F32, BF16 = jnp.float32, jnp.bfloat16
COLS = 256
EXCHANGE_VMEM = 50 * 1024 * 1024
WEIGHT_VMEM = 24 * 1024 * 1024
OPP, LEFT, RIGHT, OWN = range(4)


def dot_last(a, b):
    return lax.dot_general(a, b, (((1,), (1,)), ((), ())), preferred_element_type=F32)


def dot_first(a, b):
    return lax.dot_general(a, b, (((0,), (0,)), ((), ())), preferred_element_type=F32)


def exchange_kernel(axis, n_dev, topk_ref, slot_ref, gate_ref, count_ref, gy_hbm, y_hbm, hg_hbm, hu_hbm, wg_hbm, wu_hbm, wd_hbm,
                    d_buf, dh_buf, a_buf, gg_out, right_out, left_out, own_out,
                    gy_all, route_send, route_all, y_buf, hg_buf, hu_buf, wgu_buf, wd_buf, f1_buf, s_buf,
                    oh_buf, r_buf, pair_send, pair_recv, opp_send, opp_keep, opp_recv, hop_recv,
                    load_sem, route_ssem, route_rsem, gy_ssem, gy_rsem, pair_ssem, pair_rsem, hop_ssem, hop_rsem):
    n_loc, n_rows, ffn = hg_hbm.shape
    tok, model = gy_hbm.shape
    top_k = topk_ref.shape[0]
    cap = n_rows // n_dev
    n_exp = n_loc * n_dev
    half = tok // 2
    pair_rows = 2 * cap
    n_chip = n_dev // 2

    me = lax.axis_index(axis)
    chip = lax.div(me, 2)
    core = me - 2 * chip
    chips = [lax.rem(chip + step, n_chip) for step in (2, n_chip - 1, 1, 0)]
    homes = [2 * c + core for c in chips]
    others = [2 * c + 1 - core for c in chips]
    opp, left, right = homes[OPP], homes[LEFT], homes[RIGHT]
    sib = others[OWN]
    top, bottom = pl.ds(0, half), pl.ds(half, half)

    barrier = pltpu.get_barrier_semaphore()
    for step in range(1, n_dev):
        pl.semaphore_signal(barrier, inc=1, device_id={axis: lax.rem(me + step, n_dev)}, device_id_type=pl.DeviceIdType.MESH)

    loads = {}

    def load(name, src, dst):
        loads[name] = pltpu.make_async_copy(src, dst, load_sem.at[len(loads)])
        loads[name].start()

    load("gy", gy_hbm, gy_all.at[me])
    for e in range(n_loc):
        load(("hg", e), hg_hbm.at[e], hg_buf.at[e])
        load(("hu", e), hu_hbm.at[e], hu_buf.at[e])
    load("y", y_hbm, y_buf)
    load("wd", wd_hbm, wd_buf)
    load("wg", wg_hbm, wgu_buf.at[:, :, pl.ds(0, ffn)])
    load("wu", wu_hbm, wgu_buf.at[:, :, pl.ds(ffn, ffn)])

    loads["gy"].wait()
    pl.semaphore_wait(barrier, n_dev - 1)

    def remote(src, dst, ssem, rsem, dev):
        return pltpu.make_async_remote_copy(src_ref=src, dst_ref=dst, send_sem=ssem, recv_sem=rsem, device_id={axis: dev}, device_id_type=pl.DeviceIdType.MESH)

    sends = []

    def gy_copy(block, part, send_slot, recv_slot, dev):
        ref = gy_all.at[block, part]
        return remote(ref, ref, gy_ssem.at[send_slot], gy_rsem.at[recv_slot], dev)

    def gy_send(block, part, recv_slot, dev):
        copy = gy_copy(block, part, recv_slot, recv_slot, dev)
        copy.start()
        sends.append(copy)

    def gy_wait(block, part, recv_slot):
        gy_copy(block, part, recv_slot, recv_slot, sib).wait_recv()

    gy_send(me, top, 0, right)
    gy_send(me, bottom, 2, left)
    gy_send(me, pl.ds(0, tok), 6, sib)

    topk_t = topk_ref[...].astype(F32)
    slot_t = slot_ref[...].astype(F32)
    gate_t = gate_ref[...]
    exp_iota = lax.broadcasted_iota(jnp.int32, (n_exp, tok), 0).astype(F32)
    diag = lax.broadcasted_iota(jnp.int32, (n_exp, n_exp), 0) == lax.broadcasted_iota(jnp.int32, (n_exp, n_exp), 1)
    count = jnp.sum(jnp.where(diag, count_ref[...].astype(F32), 0.0), axis=1, keepdims=True)
    slot_d = jnp.zeros((n_exp, tok), F32)
    gate_d = jnp.zeros((n_exp, tok), F32)
    for j in range(top_k):
        hit = topk_t[j : j + 1] == exp_iota
        slot_d += jnp.where(hit, slot_t[j : j + 1] + 1.0, 0.0)
        gate_d += jnp.where(hit, gate_t[j : j + 1], 0.0)
    slot_d -= 1.0
    slot_d = jnp.where(slot_d < count, slot_d, -1.0)
    for i in range(n_dev):
        route_send[i, 0:n_loc] = slot_d[i * n_loc : (i + 1) * n_loc]
        route_send[i, n_loc : 2 * n_loc] = gate_d[i * n_loc : (i + 1) * n_loc]
    route_all[me] = route_send[me]

    peers = [sib, left, others[LEFT], right, others[RIGHT], opp, others[OPP]]
    arrives = [0, 3, 4, 1, 2, 5, 6]
    for k, dst in enumerate(peers):
        copy = remote(route_send.at[dst], route_all.at[me], route_ssem.at[k], route_rsem.at[arrives[k]], dst)
        copy.start()
        sends.append(copy)
    gy_send(me, bottom, 1, right)
    gy_send(me, top, 3, left)

    chunk = 32
    n_chunk = n_rows // chunk

    def factors(e):
        def body(i, carry):
            rows = pl.ds(pl.multiple_of(i * chunk, chunk), chunk)
            h1 = hg_buf[e, rows].astype(F32)
            h3 = hu_buf[e, rows].astype(F32)
            sig = jax.nn.sigmoid(h1)
            act = h1 * sig
            s_buf[e, rows] = act
            a_buf[e, rows] = (act * h3).astype(BF16)
            f1_buf[e, rows] = h3 * sig * (1.0 + h1 * (1.0 - sig))
            return carry

        loads[("hg", e)].wait()
        loads[("hu", e)].wait()
        lax.fori_loop(0, n_chunk, body, 0)

    for e in range(n_loc):
        factors(e)

    def route_wait(*slots):
        for k in slots:
            remote(route_send.at[peers[k]], route_all.at[peers[k]], route_ssem.at[k], route_rsem.at[k], peers[k]).wait_recv()

    slot_iota = lax.broadcasted_iota(jnp.int32, (cap, tok), 0).astype(F32)

    def build_rows(s):
        route = route_all[s]
        gates = []
        for e in range(n_loc):
            hit = route[e : e + 1] == slot_iota
            oh_buf[s, pl.ds(e * cap, cap)] = jnp.where(hit, 1.0, 0.0).astype(BF16)
            gates.append(jnp.sum(jnp.where(hit, route[n_loc + e : n_loc + e + 1], 0.0), axis=1, keepdims=True))
        gate = jnp.concatenate(gates, axis=0)
        pick = oh_buf[s]
        for n in range(0, model, COLS):
            rows = (jnp.dot(pick, gy_all[s, :, pl.ds(n, COLS)], preferred_element_type=F32) * gate).astype(BF16)
            for e in range(n_loc):
                d_buf[e, pl.ds(pl.multiple_of(s * cap, cap), cap), pl.ds(n, COLS)] = rows[e * cap : (e + 1) * cap]

    def rows_of(c):
        return pl.ds(pl.multiple_of(c * pair_rows, pair_rows), pair_rows)

    def hidden_grads(roles):
        which = [chips[role] for role in roles]

        def body(e, carry):
            d_rows = jnp.concatenate([d_buf[e, rows_of(c)] for c in which], axis=0)
            for n in range(0, ffn, COLS):
                grad = dot_last(d_rows, wd_buf[e, pl.ds(n, COLS)]).astype(BF16).astype(F32)
                for i, c in enumerate(which):
                    part = grad[i * pair_rows : (i + 1) * pair_rows]
                    dh_buf[e, rows_of(c), pl.ds(n, COLS)] = (part * f1_buf[e, rows_of(c), pl.ds(n, COLS)]).astype(BF16)
                    dh_buf[e, rows_of(c), pl.ds(ffn + n, COLS)] = (part * s_buf[e, rows_of(c), pl.ds(n, COLS)]).astype(BF16)
            return carry

        lax.fori_loop(0, n_loc, body, 0, unroll=True)

    def returned(roles, lo, hi, cols):
        which = [chips[role] for role in roles]

        def body(e, carry):
            dh_rows = jnp.concatenate([dh_buf[e, rows_of(c)] for c in which], axis=0)
            out_rows = pl.ds(pl.multiple_of(e * cap, cap), cap)
            for n in cols:
                ret = dot_last(dh_rows, wgu_buf[e, pl.ds(n, COLS)]).astype(BF16)
                for i, c in enumerate(which):
                    for k in range(2):
                        lo_row = i * pair_rows + k * cap
                        r_buf[2 * c + k, out_rows, pl.ds(n, COLS)] = ret[lo_row : lo_row + cap]
            return carry

        lax.fori_loop(lo, hi, body, 0, unroll=True)

    all_cols = range(0, model, COLS)

    def token_sum(s, n):
        return dot_first(oh_buf[s], r_buf[s, :, pl.ds(n, COLS)])

    pairs = {}

    def send_pair(key, slot, ref_send, ref_recv):
        pairs[key] = remote(ref_send, ref_recv, pair_ssem.at[slot], pair_rsem.at[slot], sib)
        pairs[key].start()
        sends.append(pairs[key])

    def finish(*roles):
        for role, _ in roles:
            for n in all_cols:
                pair_send[role, :, pl.ds(n, COLS)] = token_sum(others[role], n)
            send_pair(role, role, pair_send.at[role], pair_recv.at[role])
        for role, out in roles:
            for n in all_cols:
                out[:, pl.ds(n, COLS)] = token_sum(homes[role], n)

    loads["wd"].wait()
    route_wait(0)
    gy_wait(others[OWN], pl.ds(0, tok), 6)
    build_rows(homes[OWN])
    build_rows(others[OWN])
    hidden_grads([OWN])

    gy_wait(left, top, 0)
    gy_send(left, top, 4, right)
    gy_send(left, top, 7, sib)
    gy_wait(right, bottom, 2)
    gy_send(right, bottom, 5, left)
    gy_send(right, bottom, 9, sib)

    loads["wg"].wait()
    loads["wu"].wait()
    returned([OWN], 0, n_loc, all_cols)

    gy_wait(left, bottom, 1)
    gy_send(left, bottom, 8, sib)
    gy_wait(right, top, 3)
    gy_send(right, top, 10, sib)

    finish((OWN, own_out))

    route_wait(1, 2, 3, 4)
    build_rows(homes[LEFT])
    build_rows(homes[RIGHT])
    gy_wait(others[LEFT], top, 7)
    gy_wait(others[LEFT], bottom, 8)
    build_rows(others[LEFT])
    gy_wait(others[RIGHT], bottom, 9)
    gy_wait(others[RIGHT], top, 10)
    build_rows(others[RIGHT])

    gy_wait(opp, top, 4)
    gy_send(opp, top, 11, sib)
    gy_wait(opp, bottom, 5)
    gy_send(opp, bottom, 12, sib)

    hidden_grads([LEFT, RIGHT])
    route_wait(5, 6)

    build_rows(homes[OPP])
    gy_wait(others[OPP], top, 11)
    gy_wait(others[OPP], bottom, 12)
    build_rows(others[OPP])
    hidden_grads([OPP])

    hops = []

    def hop(i):
        pairs[OPP, i].wait_recv()
        opp_keep[i] = opp_keep[i] + opp_recv[i]
        for k, (part, dev) in enumerate(((top, right), (bottom, left))):
            copy = remote(opp_keep.at[i, part], hop_recv.at[k, i], hop_ssem.at[k, i], hop_rsem.at[k, i], dev)
            copy.start()
            sends.append(copy)
            hops.append((k, i, copy))

    for i, n in enumerate(all_cols):
        returned([OPP], 0, n_loc, [n])
        opp_send[i] = token_sum(others[OPP], n)
        send_pair((OPP, i), 4 + i, opp_send.at[i], opp_recv.at[i])
        opp_keep[i] = token_sum(homes[OPP], n)
        if i:
            hop(i - 1)

    half_loc = n_loc // 2
    returned([LEFT, RIGHT], 0, half_loc, all_cols)
    hop(model // COLS - 1)
    returned([LEFT, RIGHT], half_loc, n_loc, all_cols)
    finish((LEFT, left_out), (RIGHT, right_out))

    loads["y"].wait()
    group = 32
    gg = jnp.zeros((top_k, tok), F32)
    tok_major = lax.broadcasted_iota(jnp.int32, (group, top_k, tok), 0)
    tok_lane = lax.broadcasted_iota(jnp.int32, (group, top_k, tok), 2)
    for i in range(tok // group):
        prod = dot_last(y_buf[pl.ds(i * group * top_k, group * top_k)], gy_all[me])
        gg += jnp.sum(jnp.where(tok_major + i * group == tok_lane, prod.reshape(group, top_k, tok), 0.0), axis=0)
    gg_out[...] = gg

    pairs[OWN].wait_recv()
    own_out[...] = own_out[...] + pair_recv[OWN]
    pairs[LEFT].wait_recv()
    left_out[...] = left_out[...] + pair_recv[LEFT]
    pairs[RIGHT].wait_recv()
    right_out[...] = right_out[...] + pair_recv[RIGHT]
    for k, i, copy in hops:
        copy.wait_recv()
        out, part = ((right_out, top), (left_out, bottom))[k]
        cols = pl.ds(i * COLS, COLS)
        out[part, cols] = out[part, cols] + hop_recv[k, i]

    for copy in sends:
        copy.wait_send()


def exchange(axis, n_dev, topk_idx, slot_ids, gate_vals, pair_counts, grad_y, y_rows, h_gate, h_up, w_gate, w_up, w_down):
    n_loc, n_rows, ffn = h_gate.shape
    tok, model = grad_y.shape
    top_k = topk_idx.shape[0]
    cap = n_rows // n_dev
    vmem = pl.BlockSpec(memory_space=pltpu.VMEM)
    hbm = pl.BlockSpec(memory_space=pl.ANY)
    dma = pltpu.SemaphoreType.DMA
    part = pltpu.VMEM((tok, model), F32)
    return pl.pallas_call(
        functools.partial(exchange_kernel, axis, n_dev),
        name="exchange",
        out_shape=(
            pltpu.VMEM((n_loc, n_rows, model), BF16),
            pltpu.VMEM((n_loc, n_rows, 2 * ffn), BF16),
            pltpu.VMEM((n_loc, n_rows, ffn), BF16),
            pltpu.VMEM((top_k, tok), F32),
            part, part, part,
        ),
        in_specs=[vmem] * 4 + [hbm] * 7,
        out_specs=(vmem,) * 7,
        scratch_shapes=[
            pltpu.VMEM((n_dev, tok, model), BF16),
            pltpu.VMEM((n_dev, 2 * n_loc, tok), F32),
            pltpu.VMEM((n_dev, 2 * n_loc, tok), F32),
            pltpu.VMEM(y_rows.shape, BF16),
            pltpu.VMEM(h_gate.shape, BF16),
            pltpu.VMEM(h_up.shape, BF16),
            pltpu.VMEM((n_loc, model, 2 * ffn), BF16),
            pltpu.VMEM(w_down.shape, BF16),
            pltpu.VMEM(h_gate.shape, F32),
            pltpu.VMEM(h_gate.shape, F32),
            pltpu.VMEM((n_dev, n_loc * cap, tok), BF16),
            pltpu.VMEM((n_dev, n_loc * cap, model), BF16),
            pltpu.VMEM((4, tok, model), F32),
            pltpu.VMEM((4, tok, model), F32),
            pltpu.VMEM((model // COLS, tok, COLS), F32),
            pltpu.VMEM((model // COLS, tok, COLS), F32),
            pltpu.VMEM((model // COLS, tok, COLS), F32),
            pltpu.VMEM((2, model // COLS, tok // 2, COLS), F32),
            dma((5 + 2 * n_loc,)), dma((n_dev - 1,)), dma((n_dev - 1,)), dma((13,)), dma((13,)),
            dma((4 + model // COLS,)), dma((4 + model // COLS,)), dma((2, model // COLS)), dma((2, model // COLS)),
        ],
        compiler_params=pltpu.CompilerParams(collective_id=0, has_side_effects=True, vmem_limit_bytes=EXCHANGE_VMEM),
    )(topk_idx, slot_ids, gate_vals, pair_counts, grad_y, y_rows, h_gate, h_up, w_gate, w_up, w_down)


def weight_kernel(x_hbm, dh_buf, a_buf, d_buf, gg_ref, wg_hbm, wu_hbm, wd_hbm, gg_out, x_buf, wg_buf, wu_buf, wd_buf, in_sem, out_sem):
    n_loc, ffn, model = a_buf.shape[0], a_buf.shape[2], d_buf.shape[2]
    gg_out[...] = gg_ref[...]
    ins = []
    for e in range(n_loc):
        ins.append(pltpu.make_async_copy(x_hbm.at[e], x_buf.at[e], in_sem.at[e]))
        ins[e].start()
    outs = {}

    def store(key, src, dst, sem):
        outs[key] = pltpu.make_async_copy(src, dst, sem)
        outs[key].start()

    for e in range(n_loc):
        slot = e % 2
        for k in range(3):
            if (slot, k) in outs:
                outs.pop((slot, k)).wait()
        for n in range(0, model, COLS):
            wd_buf[slot, :, pl.ds(n, COLS)] = dot_first(a_buf[e], d_buf[e, :, pl.ds(n, COLS)])
        store((slot, 0), wd_buf.at[slot], wd_hbm.at[e], out_sem.at[slot, 0])
        ins[e].wait()
        for n in range(0, ffn, COLS):
            wg_buf[slot, :, pl.ds(n, COLS)] = dot_first(x_buf[e], dh_buf[e, :, pl.ds(n, COLS)])
        store((slot, 1), wg_buf.at[slot], wg_hbm.at[e], out_sem.at[slot, 1])
        for n in range(0, ffn, COLS):
            wu_buf[slot, :, pl.ds(n, COLS)] = dot_first(x_buf[e], dh_buf[e, :, pl.ds(ffn + n, COLS)])
        store((slot, 2), wu_buf.at[slot], wu_hbm.at[e], out_sem.at[slot, 2])
    for copy in outs.values():
        copy.wait()


def weight_grads(x_disp, dh_rows, a_rows, d_rows, gg):
    n_loc, n_rows, model = x_disp.shape
    ffn = a_rows.shape[2]
    flops = 2 * n_loc * n_rows * model * 3 * ffn
    moved = 2 * x_disp.size + 12 * n_loc * model * ffn
    vmem = pl.BlockSpec(memory_space=pltpu.VMEM)
    hbm = pl.BlockSpec(memory_space=pl.ANY)
    return pl.pallas_call(
        weight_kernel,
        name="weight_grads",
        in_specs=[hbm] + [vmem] * 4,
        out_specs=(hbm, hbm, hbm, vmem),
        out_shape=(
            jax.ShapeDtypeStruct((n_loc, model, ffn), F32),
            jax.ShapeDtypeStruct((n_loc, model, ffn), F32),
            jax.ShapeDtypeStruct((n_loc, ffn, model), F32),
            jax.ShapeDtypeStruct(gg.shape, F32),
        ),
        scratch_shapes=[
            pltpu.VMEM(x_disp.shape, BF16),
            pltpu.VMEM((2, model, ffn), F32),
            pltpu.VMEM((2, model, ffn), F32),
            pltpu.VMEM((2, ffn, model), F32),
            pltpu.SemaphoreType.DMA((n_loc,)),
            pltpu.SemaphoreType.DMA((2, 3)),
        ],
        cost_estimate=pl.CostEstimate(flops=flops, bytes_accessed=moved, transcendentals=0),
        compiler_params=pltpu.CompilerParams(vmem_limit_bytes=WEIGHT_VMEM),
    )(pltpu.with_memory_space_constraint(x_disp, pltpu.HBM), *(pltpu.with_memory_space_constraint(rows, pltpu.VMEM) for rows in (dh_rows, a_rows, d_rows, gg)))


def final_kernel(own_ref, left_ref, right_ref, gx_out):
    gx_out[...] = (own_ref[...] + left_ref[...] + right_ref[...]).astype(BF16)


def final_sum(own, from_left, from_right):
    vmem = pl.BlockSpec(memory_space=pltpu.VMEM)
    return pl.pallas_call(
        final_kernel,
        name="final_sum",
        out_shape=jax.ShapeDtypeStruct(own.shape, BF16),
        in_specs=[vmem] * 3,
        out_specs=vmem,
        compiler_params=pltpu.CompilerParams(vmem_limit_bytes=8 * 1024 * 1024),
    )(*(pltpu.with_memory_space_constraint(part, pltpu.VMEM) for part in (own, from_left, from_right)))


def solution(mesh):
    axis = "ep"
    n_dev = mesh.shape[axis]
    rows_spec = P(("dp", "ep"), None)
    cube_spec = P(("dp", "ep"), None, None)
    weight_spec = P("ep", None, None)
    to_right = [(i, (i + 2) % n_dev) for i in range(n_dev)]
    to_left = [(i, (i - 2) % n_dev) for i in range(n_dev)]

    def local_step(grad_y, gate_vals, topk_idx, slot_ids, pair_counts, y_routed, x_disp, h_gate, h_up, w_gate, w_up, w_down):
        y_rows = y_routed.reshape(-1, y_routed.shape[2])
        d_rows, dh_rows, a_rows, gg, for_right, for_left, own = exchange(
            axis, n_dev, topk_idx.T, slot_ids.T, gate_vals.T, pair_counts, grad_y, y_rows, h_gate, h_up, w_gate, w_up, w_down)
        from_left = lax.ppermute(for_right, axis, to_right)
        from_right = lax.ppermute(for_left, axis, to_left)
        grad_wgate, grad_wup, grad_wdown, grad_gate = weight_grads(x_disp, dh_rows, a_rows, d_rows, gg)
        grad_x = final_sum(own, from_left, from_right)
        return grad_x, grad_gate.T, grad_wgate, grad_wup, grad_wdown

    return jax.shard_map(local_step, mesh=mesh, in_specs=(rows_spec, rows_spec, rows_spec, rows_spec, rows_spec, cube_spec, cube_spec, cube_spec, cube_spec, weight_spec, weight_spec, weight_spec), out_specs=(rows_spec, rows_spec, cube_spec, cube_spec, cube_spec), check_vma=False)
```

```python
import functools

import jax
import jax.numpy as jnp
from jax import lax
from jax.experimental import pallas as pl
from jax.experimental.pallas import tpu as pltpu
from jax.sharding import PartitionSpec as P

F32, BF16 = jnp.float32, jnp.bfloat16
COLS = 256
EXCHANGE_VMEM = 51 * 1024 * 1024
WEIGHT_VMEM = 24 * 1024 * 1024
OPP, LEFT, RIGHT, OWN = range(4)


def dot_last(a, b):
    return lax.dot_general(a, b, (((1,), (1,)), ((), ())), preferred_element_type=F32)


def dot_first(a, b):
    return lax.dot_general(a, b, (((0,), (0,)), ((), ())), preferred_element_type=F32)


def exchange_kernel(axis, n_dev, topk_ref, slot_ref, gate_ref, count_ref, gy_hbm, y_hbm, hg_hbm, hu_hbm, wg_hbm, wu_hbm, wd_hbm,
                    d_buf, dh_buf, a_buf, gg_out, right_out, left_out, own_out,
                    gy_all, route_send, route_all, y_buf, hg_buf, hu_buf, wgu_buf, wd_buf, wgu_turned, wd_turned, f1_buf, s_buf,
                    oh_buf, r_buf, pair_send, pair_recv, opp_send, opp_keep, opp_recv, hop_recv,
                    load_sem, route_ssem, route_rsem, gy_ssem, gy_rsem, pair_ssem, pair_rsem, hop_ssem, hop_rsem):
    n_loc, n_rows, ffn = hg_hbm.shape
    tok, model = gy_hbm.shape
    top_k = topk_ref.shape[0]
    cap = n_rows // n_dev
    n_exp = n_loc * n_dev
    half = tok // 2
    pair_rows = 2 * cap
    n_chip = n_dev // 2

    me = lax.axis_index(axis)
    chip = lax.div(me, 2)
    core = me - 2 * chip
    chips = [lax.rem(chip + step, n_chip) for step in (2, n_chip - 1, 1, 0)]
    homes = [2 * c + core for c in chips]
    others = [2 * c + 1 - core for c in chips]
    opp, left, right = homes[OPP], homes[LEFT], homes[RIGHT]
    sib = others[OWN]
    top, bottom, whole = pl.ds(0, half), pl.ds(half, half), pl.ds(0, tok)
    quarter = [pl.ds(i * (tok // 4), tok // 4) for i in range(4)]

    barrier = pltpu.get_barrier_semaphore()
    for step in range(1, n_dev):
        pl.semaphore_signal(barrier, inc=1, device_id={axis: lax.rem(me + step, n_dev)}, device_id_type=pl.DeviceIdType.MESH)

    loads = {}

    def load(name, src, dst):
        loads[name] = pltpu.make_async_copy(src, dst, load_sem.at[len(loads)])
        loads[name].start()

    load("gy", gy_hbm, gy_all.at[me])
    for e in range(n_loc):
        load(("hg", e), hg_hbm.at[e], hg_buf.at[e])
        load(("hu", e), hu_hbm.at[e], hu_buf.at[e])
    load("wd", wd_hbm, wd_buf)
    load("wg", wg_hbm, wgu_buf.at[:, :, pl.ds(0, ffn)])
    load("wu", wu_hbm, wgu_buf.at[:, :, pl.ds(ffn, ffn)])
    load("y", y_hbm, y_buf)

    loads["gy"].wait()
    pl.semaphore_wait(barrier, n_dev - 1)

    def remote(src, dst, ssem, rsem, dev):
        return pltpu.make_async_remote_copy(src_ref=src, dst_ref=dst, send_sem=ssem, recv_sem=rsem, device_id={axis: dev}, device_id_type=pl.DeviceIdType.MESH)

    sends = []

    def gy_copy(block, part, send_slot, recv_slot, dev):
        ref = gy_all.at[block, part]
        return remote(ref, ref, gy_ssem.at[send_slot], gy_rsem.at[recv_slot], dev)

    def gy_send(block, part, recv_slot, dev):
        copy = gy_copy(block, part, recv_slot, recv_slot, dev)
        copy.start()
        sends.append(copy)

    def gy_wait(block, part, recv_slot):
        gy_copy(block, part, recv_slot, recv_slot, sib).wait_recv()

    gy_send(me, quarter[0], 0, right)
    gy_send(me, quarter[2], 4, left)
    gy_send(me, quarter[1], 1, right)
    gy_send(me, quarter[3], 5, left)
    gy_send(me, whole, 12, sib)

    topk_t = topk_ref[...].astype(F32)
    slot_t = slot_ref[...].astype(F32)
    gate_t = gate_ref[...]
    exp_iota = lax.broadcasted_iota(jnp.int32, (n_exp, tok), 0).astype(F32)
    diag = lax.broadcasted_iota(jnp.int32, (n_exp, n_exp), 0) == lax.broadcasted_iota(jnp.int32, (n_exp, n_exp), 1)
    count = jnp.sum(jnp.where(diag, count_ref[...].astype(F32), 0.0), axis=1, keepdims=True)
    slot_d = jnp.zeros((n_exp, tok), F32)
    gate_d = jnp.zeros((n_exp, tok), F32)
    for j in range(top_k):
        hit = topk_t[j : j + 1] == exp_iota
        slot_d += jnp.where(hit, slot_t[j : j + 1] + 1.0, 0.0)
        gate_d += jnp.where(hit, gate_t[j : j + 1], 0.0)
    slot_d -= 1.0
    slot_d = jnp.where(slot_d < count, slot_d, -1.0)
    for i in range(n_dev):
        route_send[i, 0:n_loc] = slot_d[i * n_loc : (i + 1) * n_loc]
        route_send[i, n_loc : 2 * n_loc] = gate_d[i * n_loc : (i + 1) * n_loc]
    route_all[me] = route_send[me]

    peers = [sib, left, others[LEFT], right, others[RIGHT], opp, others[OPP]]
    arrives = [0, 3, 4, 1, 2, 5, 6]
    for k, dst in enumerate(peers):
        copy = remote(route_send.at[dst], route_all.at[me], route_ssem.at[k], route_rsem.at[arrives[k]], dst)
        copy.start()
        sends.append(copy)
    gy_send(me, quarter[2], 2, right)
    gy_send(me, quarter[0], 6, left)

    chunk = 32
    n_chunk = n_rows // chunk

    def factors(e):
        def body(i, carry):
            rows = pl.ds(pl.multiple_of(i * chunk, chunk), chunk)
            h1 = hg_buf[e, rows].astype(F32)
            h3 = hu_buf[e, rows].astype(F32)
            sig = jax.nn.sigmoid(h1)
            act = h1 * sig
            s_buf[e, rows] = act
            a_buf[e, rows] = (act * h3).astype(BF16)
            f1_buf[e, rows] = h3 * sig * (1.0 + h1 * (1.0 - sig))
            return carry

        loads[("hg", e)].wait()
        loads[("hu", e)].wait()
        lax.fori_loop(0, n_chunk, body, 0)

    for e in range(n_loc):
        factors(e)

    def route_wait(*slots):
        for k in slots:
            remote(route_send.at[peers[k]], route_all.at[peers[k]], route_ssem.at[k], route_rsem.at[k], peers[k]).wait_recv()

    slot_iota = lax.broadcasted_iota(jnp.int32, (cap, tok), 0).astype(F32)

    def build_rows(s):
        route = route_all[s]
        gates = []
        for e in range(n_loc):
            hit = route[e : e + 1] == slot_iota
            oh_buf[s, pl.ds(e * cap, cap)] = jnp.where(hit, 1.0, 0.0).astype(BF16)
            gates.append(jnp.sum(jnp.where(hit, route[n_loc + e : n_loc + e + 1], 0.0), axis=1, keepdims=True))
        gate = jnp.concatenate(gates, axis=0)
        pick = oh_buf[s]
        for n in range(0, model, COLS):
            rows = (jnp.dot(pick, gy_all[s, :, pl.ds(n, COLS)], preferred_element_type=F32) * gate).astype(BF16)
            for e in range(n_loc):
                d_buf[e, pl.ds(pl.multiple_of(s * cap, cap), cap), pl.ds(n, COLS)] = rows[e * cap : (e + 1) * cap]

    def rows_of(c):
        return pl.ds(pl.multiple_of(c * pair_rows, pair_rows), pair_rows)

    def turn(src, dst, e):
        for i in range(0, src.shape[1], COLS):
            for j in range(0, src.shape[2], COLS):
                dst[e, pl.ds(j, COLS), pl.ds(i, COLS)] = src[e, pl.ds(i, COLS), pl.ds(j, COLS)].T

    def hidden_grads(roles, lo, hi):
        which = [chips[role] for role in roles]

        def body(e, carry):
            d_rows = jnp.concatenate([d_buf[e, rows_of(c)] for c in which], axis=0)
            for n in range(0, ffn, COLS):
                if roles == [OWN]:
                    grad = dot_last(d_rows, wd_buf[e, pl.ds(n, COLS)])
                else:
                    grad = jnp.dot(d_rows, wd_turned[e, :, pl.ds(n, COLS)], preferred_element_type=F32)
                grad = grad.astype(BF16).astype(F32)
                for i, c in enumerate(which):
                    part = grad[i * pair_rows : (i + 1) * pair_rows]
                    dh_buf[e, rows_of(c), pl.ds(n, COLS)] = (part * f1_buf[e, rows_of(c), pl.ds(n, COLS)]).astype(BF16)
                    dh_buf[e, rows_of(c), pl.ds(ffn + n, COLS)] = (part * s_buf[e, rows_of(c), pl.ds(n, COLS)]).astype(BF16)
            if roles == [OWN]:
                turn(wd_buf, wd_turned, e)
            return carry

        lax.fori_loop(lo, hi, body, 0, unroll=True)

    def returned(roles, lo, hi, cols):
        which = [chips[role] for role in roles]

        def body(e, carry):
            dh_rows = jnp.concatenate([dh_buf[e, rows_of(c)] for c in which], axis=0)
            out_rows = pl.ds(pl.multiple_of(e * cap, cap), cap)
            for n in cols:
                if roles == [OWN]:
                    ret = dot_last(dh_rows, wgu_buf[e, pl.ds(n, COLS)])
                else:
                    ret = jnp.dot(dh_rows, wgu_turned[e, :, pl.ds(n, COLS)], preferred_element_type=F32)
                ret = ret.astype(BF16)
                for i in range(len(which)):
                    for k in range(2):
                        lo_row = i * pair_rows + k * cap
                        r_buf[2 * i + k, out_rows, pl.ds(n, COLS)] = ret[lo_row : lo_row + cap]
            if roles == [OWN]:
                turn(wgu_buf, wgu_turned, e)
            return carry

        lax.fori_loop(lo, hi, body, 0, unroll=True)

    all_cols = range(0, model, COLS)

    def token_sum(role, k, n):
        return dot_first(oh_buf[2 * chips[role] + k], r_buf[2 * (role == RIGHT) + k, :, pl.ds(n, COLS)])

    pairs = {}

    def send_pair(key, slot, ref_send, ref_recv):
        pairs[key] = remote(ref_send, ref_recv, pair_ssem.at[slot], pair_rsem.at[slot], sib)
        pairs[key].start()
        sends.append(pairs[key])

    def finish(cols, part, *roles):
        for role, _ in roles:
            for n in cols:
                pair_send[role - 1, :, pl.ds(n, COLS)] = token_sum(role, 1 - core, n)
            block = pl.ds(cols[0], len(cols) * COLS)
            send_pair((role, part), 2 * (role - 1) + part, pair_send.at[role - 1, :, block], pair_recv.at[role - 1, :, block])
        for role, out in roles:
            for n in cols:
                out[:, pl.ds(n, COLS)] = token_sum(role, core, n)

    def add_pair(role, part, cols, out):
        pairs[role, part].wait_recv()
        block = pl.ds(cols[0], len(cols) * COLS)
        out[:, block] = out[:, block] + pair_recv[role - 1, :, block]

    loads["wd"].wait()
    route_wait(0)
    gy_wait(others[OWN], whole, 12)
    build_rows(homes[OWN])
    build_rows(others[OWN])
    hidden_grads([OWN], 0, n_loc - 1)
    gy_wait(left, quarter[0], 0)
    gy_send(left, quarter[0], 8, right)
    gy_wait(right, quarter[2], 4)
    gy_send(right, quarter[2], 10, left)

    hidden_grads([OWN], n_loc - 1, n_loc)
    loads["wg"].wait()
    loads["wu"].wait()
    returned([OWN], 0, 1, all_cols)

    gy_wait(left, quarter[1], 1)
    gy_send(left, quarter[1], 9, right)
    gy_send(me, quarter[3], 3, right)
    gy_wait(right, quarter[3], 5)
    gy_send(right, quarter[3], 11, left)
    gy_send(me, quarter[1], 7, left)
    gy_send(left, top, 13, sib)
    gy_send(right, bottom, 15, sib)
    returned([OWN], 1, n_loc, all_cols)
    finish(all_cols, 0, (OWN, own_out))

    loads["y"].wait()
    group = 32
    gg = jnp.zeros((top_k, tok), F32)
    tok_major = lax.broadcasted_iota(jnp.int32, (group, top_k, tok), 0)
    tok_lane = lax.broadcasted_iota(jnp.int32, (group, top_k, tok), 2)
    for i in range(tok // group):
        prod = dot_last(y_buf[pl.ds(i * group * top_k, group * top_k)], gy_all[me])
        gg += jnp.sum(jnp.where(tok_major + i * group == tok_lane, prod.reshape(group, top_k, tok), 0.0), axis=0)
    gg_out[...] = gg

    gy_wait(opp, quarter[0], 8)
    gy_wait(opp, quarter[1], 9)
    gy_send(opp, top, 17, sib)
    gy_wait(opp, quarter[2], 10)
    gy_wait(opp, quarter[3], 11)
    gy_send(opp, bottom, 18, sib)
    route_wait(5, 6)
    build_rows(homes[OPP])
    gy_wait(others[OPP], top, 17)
    gy_wait(others[OPP], bottom, 18)
    build_rows(others[OPP])
    hidden_grads([OPP], 0, n_loc)

    gy_wait(left, quarter[2], 2)
    gy_wait(left, quarter[3], 3)
    gy_send(left, bottom, 14, sib)
    gy_wait(right, quarter[0], 6)
    gy_wait(right, quarter[1], 7)
    gy_send(right, top, 16, sib)

    hops = []

    def hop(i):
        pairs["hop", i].wait_recv()
        opp_keep[i] = opp_keep[i] + opp_recv[i]
        for k, (part, dev) in enumerate(((top, right), (bottom, left))):
            copy = remote(opp_keep.at[i, part], hop_recv.at[k, i], hop_ssem.at[k, i], hop_rsem.at[k, i], dev)
            copy.start()
            sends.append(copy)
            hops.append((k, i, copy))

    for i, n in enumerate(all_cols):
        returned([OPP], 0, n_loc, [n])
        opp_send[i] = token_sum(OPP, 1 - core, n)
        send_pair(("hop", i), 6 + i, opp_send.at[i], opp_recv.at[i])
        opp_keep[i] = token_sum(OPP, core, n)
        if i > 1:
            hop(i - 2)

    near = ((LEFT, left_out), (RIGHT, right_out))
    route_wait(1, 2, 3, 4)
    build_rows(homes[LEFT])
    hop(model // COLS - 2)
    build_rows(homes[RIGHT])
    hop(model // COLS - 1)
    gy_wait(others[LEFT], top, 13)
    gy_wait(others[LEFT], bottom, 14)
    build_rows(others[LEFT])
    gy_wait(others[RIGHT], bottom, 15)
    gy_wait(others[RIGHT], top, 16)
    build_rows(others[RIGHT])
    hidden_grads([LEFT, RIGHT], 0, n_loc)
    col_parts = (all_cols[:-1], all_cols[-1:])
    add_pair(OWN, 0, all_cols, own_out)
    for part, cols in enumerate(col_parts):
        returned([LEFT, RIGHT], 0, n_loc, cols)
        finish(cols, part, *near)
    for part, cols in enumerate(col_parts):
        for role, out in near:
            add_pair(role, part, cols, out)
    for k, i, copy in hops:
        copy.wait_recv()
        out, part = ((right_out, top), (left_out, bottom))[k]
        cols = pl.ds(i * COLS, COLS)
        out[part, cols] = out[part, cols] + hop_recv[k, i]

    for copy in sends:
        copy.wait_send()


def exchange(axis, n_dev, topk_idx, slot_ids, gate_vals, pair_counts, grad_y, y_rows, h_gate, h_up, w_gate, w_up, w_down):
    n_loc, n_rows, ffn = h_gate.shape
    tok, model = grad_y.shape
    cap = n_rows // n_dev
    vmem = pl.BlockSpec(memory_space=pltpu.VMEM)
    hbm = pl.BlockSpec(memory_space=pl.ANY)
    dma = pltpu.SemaphoreType.DMA
    part = pltpu.VMEM((tok, model), F32)
    return pl.pallas_call(
        functools.partial(exchange_kernel, axis, n_dev),
        name="exchange",
        out_shape=(
            pltpu.VMEM((n_loc, n_rows, model), BF16),
            pltpu.VMEM((n_loc, n_rows, 2 * ffn), BF16),
            pltpu.VMEM((n_loc, n_rows, ffn), BF16),
            pltpu.VMEM((topk_idx.shape[0], tok), F32),
            part, part, part,
        ),
        in_specs=[vmem] * 4 + [hbm] * 7,
        out_specs=(vmem,) * 7,
        scratch_shapes=[
            pltpu.VMEM((n_dev, tok, model), BF16),
            pltpu.VMEM((n_dev, 2 * n_loc, tok), F32),
            pltpu.VMEM((n_dev, 2 * n_loc, tok), F32),
            pltpu.VMEM(y_rows.shape, BF16),
            pltpu.VMEM(h_gate.shape, BF16),
            pltpu.VMEM(h_up.shape, BF16),
            pltpu.VMEM((n_loc, model, 2 * ffn), BF16),
            pltpu.VMEM(w_down.shape, BF16),
            pltpu.VMEM((n_loc, 2 * ffn, model), BF16),
            pltpu.VMEM((n_loc, model, ffn), BF16),
            pltpu.VMEM(h_gate.shape, F32),
            pltpu.VMEM(h_gate.shape, F32),
            pltpu.VMEM((n_dev, n_loc * cap, tok), BF16),
            pltpu.VMEM((4, n_loc * cap, model), BF16),
            pltpu.VMEM((3, tok, model), F32),
            pltpu.VMEM((3, tok, model), F32),
            pltpu.VMEM((model // COLS, tok, COLS), F32),
            pltpu.VMEM((model // COLS, tok, COLS), F32),
            pltpu.VMEM((model // COLS, tok, COLS), F32),
            pltpu.VMEM((2, model // COLS, tok // 2, COLS), F32),
            dma((5 + 2 * n_loc,)), dma((n_dev - 1,)), dma((n_dev - 1,)), dma((19,)), dma((19,)),
            dma((6 + model // COLS,)), dma((6 + model // COLS,)), dma((2, model // COLS)), dma((2, model // COLS)),
        ],
        compiler_params=pltpu.CompilerParams(collective_id=0, has_side_effects=True, vmem_limit_bytes=EXCHANGE_VMEM),
    )(topk_idx, slot_ids, gate_vals, pair_counts, grad_y, y_rows, h_gate, h_up, w_gate, w_up, w_down)


def weight_kernel(x_hbm, dh_buf, a_buf, d_buf, gg_ref, wg_hbm, wu_hbm, wd_hbm, gg_out, x_buf, wg_buf, wu_buf, wd_buf, in_sem, out_sem):
    n_loc, ffn, model = a_buf.shape[0], a_buf.shape[2], d_buf.shape[2]
    gg_out[...] = gg_ref[...]
    ins = []
    for e in range(n_loc):
        ins.append(pltpu.make_async_copy(x_hbm.at[e], x_buf.at[e], in_sem.at[e]))
        ins[e].start()
    outs = {}

    def store(key, src, dst, sem):
        outs[key] = pltpu.make_async_copy(src, dst, sem)
        outs[key].start()

    for e in range(n_loc):
        slot = e % 2
        for k in range(3):
            if (slot, k) in outs:
                outs.pop((slot, k)).wait()
        for n in range(0, model, COLS):
            wd_buf[slot, :, pl.ds(n, COLS)] = dot_first(a_buf[e], d_buf[e, :, pl.ds(n, COLS)])
        store((slot, 0), wd_buf.at[slot], wd_hbm.at[e], out_sem.at[slot, 0])
        ins[e].wait()
        for n in range(0, ffn, COLS):
            wg_buf[slot, :, pl.ds(n, COLS)] = dot_first(x_buf[e], dh_buf[e, :, pl.ds(n, COLS)])
        store((slot, 1), wg_buf.at[slot], wg_hbm.at[e], out_sem.at[slot, 1])
        for n in range(0, ffn, COLS):
            wu_buf[slot, :, pl.ds(n, COLS)] = dot_first(x_buf[e], dh_buf[e, :, pl.ds(ffn + n, COLS)])
        store((slot, 2), wu_buf.at[slot], wu_hbm.at[e], out_sem.at[slot, 2])
    for copy in outs.values():
        copy.wait()


def weight_grads(x_disp, dh_rows, a_rows, d_rows, gg):
    n_loc, n_rows, model = x_disp.shape
    ffn = a_rows.shape[2]
    flops = 2 * n_loc * n_rows * model * 3 * ffn
    moved = 2 * x_disp.size + 12 * n_loc * model * ffn
    vmem = pl.BlockSpec(memory_space=pltpu.VMEM)
    hbm = pl.BlockSpec(memory_space=pl.ANY)
    return pl.pallas_call(
        weight_kernel,
        name="weight_grads",
        in_specs=[hbm] + [vmem] * 4,
        out_specs=(hbm, hbm, hbm, vmem),
        out_shape=(
            jax.ShapeDtypeStruct((n_loc, model, ffn), F32),
            jax.ShapeDtypeStruct((n_loc, model, ffn), F32),
            jax.ShapeDtypeStruct((n_loc, ffn, model), F32),
            jax.ShapeDtypeStruct(gg.shape, F32),
        ),
        scratch_shapes=[
            pltpu.VMEM(x_disp.shape, BF16),
            pltpu.VMEM((2, model, ffn), F32),
            pltpu.VMEM((2, model, ffn), F32),
            pltpu.VMEM((2, ffn, model), F32),
            pltpu.SemaphoreType.DMA((n_loc,)),
            pltpu.SemaphoreType.DMA((2, 3)),
        ],
        cost_estimate=pl.CostEstimate(flops=flops, bytes_accessed=moved, transcendentals=0),
        compiler_params=pltpu.CompilerParams(vmem_limit_bytes=WEIGHT_VMEM),
    )(pltpu.with_memory_space_constraint(x_disp, pltpu.HBM), *(pltpu.with_memory_space_constraint(rows, pltpu.VMEM) for rows in (dh_rows, a_rows, d_rows, gg)))


def final_kernel(own_ref, left_ref, right_ref, gx_out):
    gx_out[...] = (own_ref[...] + left_ref[...] + right_ref[...]).astype(BF16)


def final_sum(own, from_left, from_right):
    vmem = pl.BlockSpec(memory_space=pltpu.VMEM)
    return pl.pallas_call(
        final_kernel,
        name="final_sum",
        out_shape=jax.ShapeDtypeStruct(own.shape, BF16),
        in_specs=[vmem] * 3,
        out_specs=vmem,
        compiler_params=pltpu.CompilerParams(vmem_limit_bytes=8 * 1024 * 1024),
    )(*(pltpu.with_memory_space_constraint(part, pltpu.VMEM) for part in (own, from_left, from_right)))


def solution(mesh):
    axis = "ep"
    n_dev = mesh.shape[axis]
    rows_spec = P(("dp", "ep"), None)
    cube_spec = P(("dp", "ep"), None, None)
    weight_spec = P("ep", None, None)
    to_right = [(i, (i + 2) % n_dev) for i in range(n_dev)]
    to_left = [(i, (i - 2) % n_dev) for i in range(n_dev)]

    def local_step(grad_y, gate_vals, topk_idx, slot_ids, pair_counts, y_routed, x_disp, h_gate, h_up, w_gate, w_up, w_down):
        y_rows = y_routed.reshape(-1, y_routed.shape[2])
        d_rows, dh_rows, a_rows, gg, for_right, for_left, own = exchange(
            axis, n_dev, topk_idx.T, slot_ids.T, gate_vals.T, pair_counts, grad_y, y_rows, h_gate, h_up, w_gate, w_up, w_down)
        from_left = lax.ppermute(for_right, axis, to_right)
        from_right = lax.ppermute(for_left, axis, to_left)
        grad_wgate, grad_wup, grad_wdown, grad_gate = weight_grads(x_disp, dh_rows, a_rows, d_rows, gg)
        grad_x = final_sum(own, from_left, from_right)
        return grad_x, grad_gate.T, grad_wgate, grad_wup, grad_wdown

    return jax.shard_map(local_step, mesh=mesh, in_specs=(rows_spec, rows_spec, rows_spec, rows_spec, rows_spec, cube_spec, cube_spec, cube_spec, cube_spec, weight_spec, weight_spec, weight_spec), out_specs=(rows_spec, rows_spec, cube_spec, cube_spec, cube_spec), check_vma=False)
```

```python
import functools

import jax
import jax.numpy as jnp
from jax import lax
from jax.experimental import pallas as pl
from jax.experimental.pallas import tpu as pltpu
from jax.sharding import PartitionSpec as P

F32, BF16 = jnp.float32, jnp.bfloat16
COLS = 256
EXCHANGE_VMEM = 51 * 1024 * 1024
WEIGHT_VMEM = 24 * 1024 * 1024
OPP, LEFT, RIGHT, OWN = range(4)


def dot_last(a, b):
    return lax.dot_general(a, b, (((1,), (1,)), ((), ())), preferred_element_type=F32)


def dot_first(a, b):
    return lax.dot_general(a, b, (((0,), (0,)), ((), ())), preferred_element_type=F32)


def exchange_kernel(axis, n_dev, topk_ref, slot_ref, gate_ref, count_ref, gy_hbm, y_hbm, hg_hbm, hu_hbm, wg_hbm, wu_hbm, wd_hbm,
                    d_buf, dh_buf, a_buf, gg_out, right_out, left_out, own_out,
                    gy_all, route_send, route_all, y_buf, hg_buf, hu_buf, wgu_buf, wd_buf, wgu_turned, wd_turned, f1_buf, s_buf,
                    oh_buf, r_buf, pair_send, pair_recv, opp_send, opp_keep, opp_recv, hop_recv,
                    load_sem, route_ssem, route_rsem, gy_ssem, gy_rsem, pair_ssem, pair_rsem, hop_ssem, hop_rsem):
    n_loc, n_rows, ffn = hg_hbm.shape
    tok, model = gy_hbm.shape
    top_k = topk_ref.shape[0]
    cap = n_rows // n_dev
    n_exp = n_loc * n_dev
    half = tok // 2
    pair_rows = 2 * cap
    n_chip = n_dev // 2

    me = lax.axis_index(axis)
    chip = lax.div(me, 2)
    core = me - 2 * chip
    chips = [lax.rem(chip + step, n_chip) for step in (2, n_chip - 1, 1, 0)]
    homes = [2 * c + core for c in chips]
    others = [2 * c + 1 - core for c in chips]
    opp, left, right = homes[OPP], homes[LEFT], homes[RIGHT]
    sib = others[OWN]
    top, bottom, whole = pl.ds(0, half), pl.ds(half, half), pl.ds(0, tok)
    quarter = [pl.ds(i * (tok // 4), tok // 4) for i in range(4)]

    barrier = pltpu.get_barrier_semaphore()
    for step in range(1, n_dev):
        pl.semaphore_signal(barrier, inc=1, device_id={axis: lax.rem(me + step, n_dev)}, device_id_type=pl.DeviceIdType.MESH)

    loads = {}

    def load(name, src, dst):
        loads[name] = pltpu.make_async_copy(src, dst, load_sem.at[len(loads)])
        loads[name].start()

    load("gy", gy_hbm, gy_all.at[me])
    for e in range(n_loc):
        load(("hg", e), hg_hbm.at[e], hg_buf.at[e])
        load(("hu", e), hu_hbm.at[e], hu_buf.at[e])
    load("wd", wd_hbm, wd_buf)
    load("wg", wg_hbm, wgu_buf.at[:, :, pl.ds(0, ffn)])
    load("wu", wu_hbm, wgu_buf.at[:, :, pl.ds(ffn, ffn)])
    load("y", y_hbm, y_buf)

    loads["gy"].wait()
    pl.semaphore_wait(barrier, n_dev - 1)

    def remote(src, dst, ssem, rsem, dev):
        return pltpu.make_async_remote_copy(src_ref=src, dst_ref=dst, send_sem=ssem, recv_sem=rsem, device_id={axis: dev}, device_id_type=pl.DeviceIdType.MESH)

    def gy_copy(block, part, recv_slot, dev):
        ref = gy_all.at[block, part]
        return remote(ref, ref, gy_ssem, gy_rsem.at[recv_slot], dev)

    def gy_send(block, part, recv_slot, dev):
        gy_copy(block, part, recv_slot, dev).start()

    def gy_wait(block, part, recv_slot):
        gy_copy(block, part, recv_slot, sib).wait_recv()

    gy_send(me, quarter[0], 0, right)
    gy_send(me, quarter[2], 3, left)
    gy_send(me, whole, 8, sib)

    topk_t = topk_ref[...].astype(F32)
    slot_t = slot_ref[...].astype(F32)
    gate_t = gate_ref[...]
    exp_iota = lax.broadcasted_iota(jnp.int32, (n_exp, tok), 0).astype(F32)
    diag = lax.broadcasted_iota(jnp.int32, (n_exp, n_exp), 0) == lax.broadcasted_iota(jnp.int32, (n_exp, n_exp), 1)
    count = jnp.sum(jnp.where(diag, count_ref[...].astype(F32), 0.0), axis=1, keepdims=True)
    slot_d = jnp.zeros((n_exp, tok), F32)
    gate_d = jnp.zeros((n_exp, tok), F32)
    for j in range(top_k):
        hit = topk_t[j : j + 1] == exp_iota
        slot_d += jnp.where(hit, slot_t[j : j + 1] + 1.0, 0.0)
        gate_d += jnp.where(hit, gate_t[j : j + 1], 0.0)
    slot_d -= 1.0
    slot_d = jnp.where(slot_d < count, slot_d, -1.0)
    for i in range(n_dev):
        route_send[i, 0:n_loc] = slot_d[i * n_loc : (i + 1) * n_loc]
        route_send[i, n_loc : 2 * n_loc] = gate_d[i * n_loc : (i + 1) * n_loc]
    route_all[me] = route_send[me]

    peers = [sib, left, others[LEFT], right, others[RIGHT], opp, others[OPP]]
    for k, dst in enumerate(peers):
        remote(route_send.at[dst], route_all.at[me], route_ssem, route_rsem.at[(k + 3) // 4], dst).start()
    for to_right, to_left, slot in ((1, 3, 1), (2, 0, 2), (3, 1, 2)):
        gy_send(me, quarter[to_right], slot, right)
        gy_send(me, quarter[to_left], 3 + slot, left)

    chunk = 32
    n_chunk = n_rows // chunk

    def factors(e):
        def body(i, carry):
            rows = pl.ds(pl.multiple_of(i * chunk, chunk), chunk)
            h1 = hg_buf[e, rows].astype(F32)
            h3 = hu_buf[e, rows].astype(F32)
            sig = jax.nn.sigmoid(h1)
            act = h1 * sig
            s_buf[e, rows] = act
            a_buf[e, rows] = (act * h3).astype(BF16)
            f1_buf[e, rows] = h3 * sig * (1.0 + h1 * (1.0 - sig))
            return carry

        loads[("hg", e)].wait()
        loads[("hu", e)].wait()
        lax.fori_loop(0, n_chunk, body, 0)

    for e in range(n_loc):
        factors(e)

    def route_wait(slot, n):
        blocks = route_all.at[pl.ds(0, n)]
        remote(blocks, blocks, route_ssem, route_rsem.at[slot], sib).wait_recv()

    slot_iota = lax.broadcasted_iota(jnp.int32, (cap, tok), 0).astype(F32)

    def build_rows(s):
        route = route_all[s]
        picks, gates = [], []
        for e in range(n_loc):
            hit = route[e : e + 1] == slot_iota
            picks.append(jnp.where(hit, 1.0, 0.0).astype(BF16))
            gates.append(jnp.sum(jnp.where(hit, route[n_loc + e : n_loc + e + 1], 0.0), axis=1, keepdims=True))
        gate = jnp.concatenate(gates, axis=0)
        pick = jnp.concatenate(picks, axis=0)
        oh_buf[s] = pick.T
        for n in range(0, model, COLS):
            rows = (jnp.dot(pick, gy_all[s, :, pl.ds(n, COLS)], preferred_element_type=F32) * gate).astype(BF16)
            for e in range(n_loc):
                d_buf[e, pl.ds(pl.multiple_of(s * cap, cap), cap), pl.ds(n, COLS)] = rows[e * cap : (e + 1) * cap]

    def rows_of(c):
        return pl.ds(pl.multiple_of(c * pair_rows, pair_rows), pair_rows)

    def turn(src, dst, e):
        for i in range(0, src.shape[1], COLS):
            for j in range(0, src.shape[2], COLS):
                dst[e, pl.ds(j, COLS), pl.ds(i, COLS)] = src[e, pl.ds(i, COLS), pl.ds(j, COLS)].T

    def hidden_grads(roles, lo, hi):
        which = [chips[role] for role in roles]

        def body(e, carry):
            d_rows = jnp.concatenate([d_buf[e, rows_of(c)] for c in which], axis=0)
            for n in range(0, ffn, COLS):
                if roles == [OWN]:
                    grad = dot_last(d_rows, wd_buf[e, pl.ds(n, COLS)])
                else:
                    grad = jnp.dot(d_rows, wd_turned[e, :, pl.ds(n, COLS)], preferred_element_type=F32)
                grad = grad.astype(BF16).astype(F32)
                for i, c in enumerate(which):
                    part = grad[i * pair_rows : (i + 1) * pair_rows]
                    dh_buf[e, rows_of(c), pl.ds(n, COLS)] = (part * f1_buf[e, rows_of(c), pl.ds(n, COLS)]).astype(BF16)
                    dh_buf[e, rows_of(c), pl.ds(ffn + n, COLS)] = (part * s_buf[e, rows_of(c), pl.ds(n, COLS)]).astype(BF16)
            if roles == [OWN]:
                turn(wd_buf, wd_turned, e)
            return carry

        lax.fori_loop(lo, hi, body, 0, unroll=True)

    def returned(roles, lo, hi, cols):
        which = [chips[role] for role in roles]

        def body(e, carry):
            dh_rows = jnp.concatenate([dh_buf[e, rows_of(c)] for c in which], axis=0)
            out_rows = pl.ds(pl.multiple_of(e * cap, cap), cap)
            for n in cols:
                if roles == [OWN]:
                    ret = dot_last(dh_rows, wgu_buf[e, pl.ds(n, COLS)])
                else:
                    ret = jnp.dot(dh_rows, wgu_turned[e, :, pl.ds(n, COLS)], preferred_element_type=F32)
                ret = ret.astype(BF16)
                for i in range(len(which)):
                    for k in range(2):
                        lo_row = i * pair_rows + k * cap
                        r_buf[2 * i + k, out_rows, pl.ds(n, COLS)] = ret[lo_row : lo_row + cap]
            if roles == [OWN]:
                turn(wgu_buf, wgu_turned, e)
            return carry

        lax.fori_loop(lo, hi, body, 0, unroll=True)

    all_cols = range(0, model, COLS)

    def token_sum(role, k, n):
        return jnp.dot(oh_buf[2 * chips[role] + k], r_buf[2 * (role == RIGHT) + k, :, pl.ds(n, COLS)], preferred_element_type=F32)

    def finish(cols, slot, *roles):
        block = pl.ds(cols[0], len(cols) * COLS)
        for role, _ in roles:
            for n in cols:
                pair_send[role - 1, :, pl.ds(n, COLS)] = token_sum(role, 1 - core, n)
            remote(pair_send.at[role - 1, :, block], pair_recv.at[role - 1, :, block], pair_ssem.at[0], pair_rsem.at[slot], sib).start()
        for role, out in roles:
            for n in cols:
                out[:, pl.ds(n, COLS)] = token_sum(role, core, n)

    def add_pair(cols, slot, *roles):
        block = pl.ds(cols[0], len(cols) * COLS)
        first = roles[0][0] - 1
        ref = pair_recv.at[pl.ds(first, len(roles)), :, block]
        remote(ref, ref, pair_ssem.at[0], pair_rsem.at[slot], sib).wait_recv()
        for role, out in roles:
            out[:, block] = out[:, block] + pair_recv[role - 1, :, block]

    loads["wd"].wait()
    route_wait(0, 1)
    gy_wait(others[OWN], whole, 8)
    build_rows(homes[OWN])
    build_rows(others[OWN])
    hidden_grads([OWN], 0, n_loc)
    gy_wait(left, quarter[0], 0)
    gy_send(left, quarter[0], 6, right)
    gy_wait(right, quarter[2], 3)
    gy_send(right, quarter[2], 7, left)

    loads["wg"].wait()
    loads["wu"].wait()
    returned([OWN], 0, 1, all_cols)

    gy_wait(left, quarter[1], 1)
    gy_send(left, quarter[1], 6, right)
    gy_send(left, top, 9, sib)
    gy_wait(right, quarter[3], 4)
    gy_send(right, quarter[3], 7, left)
    gy_send(right, bottom, 10, sib)

    returned([OWN], 1, n_loc, all_cols)

    gy_wait(left, bottom, 2)
    gy_send(left, bottom, 9, sib)
    gy_wait(right, top, 5)
    gy_send(right, top, 10, sib)

    finish(all_cols, 0, (OWN, own_out))

    loads["y"].wait()
    group = 32
    gg = jnp.zeros((top_k, tok), F32)
    tok_major = lax.broadcasted_iota(jnp.int32, (group, top_k, tok), 0)
    tok_lane = lax.broadcasted_iota(jnp.int32, (group, top_k, tok), 2)
    for i in range(tok // group):
        prod = dot_last(y_buf[pl.ds(i * group * top_k, group * top_k)], gy_all[me])
        gg += jnp.sum(jnp.where(tok_major + i * group == tok_lane, prod.reshape(group, top_k, tok), 0.0), axis=0)
    gg_out[...] = gg

    route_wait(1, 4)
    build_rows(homes[LEFT])
    build_rows(homes[RIGHT])
    gy_wait(others[LEFT], whole, 9)
    build_rows(others[LEFT])
    gy_wait(others[RIGHT], whole, 10)
    build_rows(others[RIGHT])

    gy_wait(opp, top, 6)
    gy_send(opp, top, 11, sib)
    gy_wait(opp, bottom, 7)
    gy_send(opp, bottom, 11, sib)
    route_wait(2, 2)
    build_rows(homes[OPP])
    hidden_grads([LEFT, RIGHT], 0, n_loc)

    gy_wait(others[OPP], whole, 11)
    build_rows(others[OPP])
    hidden_grads([OPP], 0, n_loc)

    def opp_pair(i):
        return remote(opp_send.at[i], opp_recv.at[i], pair_ssem.at[1], pair_rsem.at[3 + i], sib)

    def hop(i):
        opp_pair(i).wait_recv()
        opp_keep[i] = opp_keep[i] + opp_recv[i]
        for k, (part, dev) in enumerate(((top, right), (bottom, left))):
            remote(opp_keep.at[i, part], hop_recv.at[i, k], hop_ssem, hop_rsem.at[i], dev).start()

    for i, n in enumerate(all_cols):
        returned([OPP], 0, n_loc, [n])
        opp_send[i] = token_sum(OPP, 1 - core, n)
        opp_pair(i).start()
        opp_keep[i] = token_sum(OPP, core, n)
        if i:
            hop(i - 1)

    near = ((LEFT, left_out), (RIGHT, right_out))
    col_parts = (all_cols[:-1], all_cols[-1:])
    add_pair(all_cols, 0, (OWN, own_out))
    for part, cols in enumerate(col_parts):
        returned([LEFT, RIGHT], 0, n_loc, cols)
        if part == 0:
            hop(model // COLS - 1)
        finish(cols, 1 + part, *near)
    for part, cols in enumerate(col_parts):
        add_pair(cols, 1 + part, *near)
    for i, n in enumerate(all_cols):
        remote(hop_recv.at[i], hop_recv.at[i], hop_ssem, hop_rsem.at[i], right).wait_recv()
        cols = pl.ds(n, COLS)
        right_out[top, cols] = right_out[top, cols] + hop_recv[i, 0]
        left_out[bottom, cols] = left_out[bottom, cols] + hop_recv[i, 1]

    sent = gy_all.at[pl.ds(0, n_dev - 1)]
    for ref, ssem, rsem in ((sent, gy_ssem, gy_rsem), (route_all.at[pl.ds(0, n_dev - 1)], route_ssem, route_rsem), (pair_send, pair_ssem.at[0], pair_rsem),
                            (opp_send, pair_ssem.at[1], pair_rsem), (hop_recv, hop_ssem, hop_rsem)):
        remote(ref, ref, ssem, rsem.at[0], sib).wait_send()


def exchange(axis, n_dev, topk_idx, slot_ids, gate_vals, pair_counts, grad_y, y_rows, h_gate, h_up, w_gate, w_up, w_down):
    n_loc, n_rows, ffn = h_gate.shape
    tok, model = grad_y.shape
    cap = n_rows // n_dev
    vmem = pl.BlockSpec(memory_space=pltpu.VMEM)
    hbm = pl.BlockSpec(memory_space=pl.ANY)
    dma = pltpu.SemaphoreType.DMA
    part = pltpu.VMEM((tok, model), F32)
    return pl.pallas_call(
        functools.partial(exchange_kernel, axis, n_dev),
        name="exchange",
        out_shape=(
            pltpu.VMEM((n_loc, n_rows, model), BF16),
            pltpu.VMEM((n_loc, n_rows, 2 * ffn), BF16),
            pltpu.VMEM((n_loc, n_rows, ffn), BF16),
            pltpu.VMEM((topk_idx.shape[0], tok), F32),
            part, part, part,
        ),
        in_specs=[vmem] * 4 + [hbm] * 7,
        out_specs=(vmem,) * 7,
        scratch_shapes=[
            pltpu.VMEM((n_dev, tok, model), BF16),
            pltpu.VMEM((n_dev, 2 * n_loc, tok), F32),
            pltpu.VMEM((n_dev, 2 * n_loc, tok), F32),
            pltpu.VMEM(y_rows.shape, BF16),
            pltpu.VMEM(h_gate.shape, BF16),
            pltpu.VMEM(h_up.shape, BF16),
            pltpu.VMEM((n_loc, model, 2 * ffn), BF16),
            pltpu.VMEM(w_down.shape, BF16),
            pltpu.VMEM((n_loc, 2 * ffn, model), BF16),
            pltpu.VMEM((n_loc, model, ffn), BF16),
            pltpu.VMEM(h_gate.shape, F32),
            pltpu.VMEM(h_gate.shape, F32),
            pltpu.VMEM((n_dev, tok, n_loc * cap), BF16),
            pltpu.VMEM((4, n_loc * cap, model), BF16),
            pltpu.VMEM((3, tok, model), F32),
            pltpu.VMEM((3, tok, model), F32),
            pltpu.VMEM((model // COLS, tok, COLS), F32),
            pltpu.VMEM((model // COLS, tok, COLS), F32),
            pltpu.VMEM((model // COLS, tok, COLS), F32),
            pltpu.VMEM((model // COLS, 2, tok // 2, COLS), F32),
            dma((5 + 2 * n_loc,)), dma, dma((3,)), dma, dma((12,)), dma((2,)), dma((3 + model // COLS,)), dma, dma((model // COLS,)),
        ],
        compiler_params=pltpu.CompilerParams(collective_id=0, has_side_effects=True, vmem_limit_bytes=EXCHANGE_VMEM),
    )(topk_idx, slot_ids, gate_vals, pair_counts, grad_y, y_rows, h_gate, h_up, w_gate, w_up, w_down)


def weight_kernel(x_hbm, dh_buf, a_buf, d_buf, gg_ref, wg_hbm, wu_hbm, wd_hbm, gg_out, x_buf, wg_buf, wu_buf, wd_buf, in_sem, out_sem):
    n_loc, ffn, model = a_buf.shape[0], a_buf.shape[2], d_buf.shape[2]
    gg_out[...] = gg_ref[...]
    ins = []
    for e in range(n_loc):
        ins.append(pltpu.make_async_copy(x_hbm.at[e], x_buf.at[e], in_sem.at[e]))
        ins[e].start()
    outs = {}

    def store(key, src, dst, sem):
        outs[key] = pltpu.make_async_copy(src, dst, sem)
        outs[key].start()

    for e in range(n_loc):
        slot = e % 2
        for k in range(3):
            if (slot, k) in outs:
                outs.pop((slot, k)).wait()
        for n in range(0, model, COLS):
            wd_buf[slot, :, pl.ds(n, COLS)] = dot_first(a_buf[e], d_buf[e, :, pl.ds(n, COLS)])
        store((slot, 0), wd_buf.at[slot], wd_hbm.at[e], out_sem.at[slot, 0])
        ins[e].wait()
        for n in range(0, ffn, COLS):
            wg_buf[slot, :, pl.ds(n, COLS)] = dot_first(x_buf[e], dh_buf[e, :, pl.ds(n, COLS)])
        store((slot, 1), wg_buf.at[slot], wg_hbm.at[e], out_sem.at[slot, 1])
        for n in range(0, ffn, COLS):
            wu_buf[slot, :, pl.ds(n, COLS)] = dot_first(x_buf[e], dh_buf[e, :, pl.ds(ffn + n, COLS)])
        store((slot, 2), wu_buf.at[slot], wu_hbm.at[e], out_sem.at[slot, 2])
    for copy in outs.values():
        copy.wait()


def weight_grads(x_disp, dh_rows, a_rows, d_rows, gg):
    n_loc, n_rows, model = x_disp.shape
    ffn = a_rows.shape[2]
    flops = 2 * n_loc * n_rows * model * 3 * ffn
    moved = 2 * x_disp.size + 12 * n_loc * model * ffn
    vmem = pl.BlockSpec(memory_space=pltpu.VMEM)
    hbm = pl.BlockSpec(memory_space=pl.ANY)
    return pl.pallas_call(
        weight_kernel,
        name="weight_grads",
        in_specs=[hbm] + [vmem] * 4,
        out_specs=(hbm, hbm, hbm, vmem),
        out_shape=(
            jax.ShapeDtypeStruct((n_loc, model, ffn), F32),
            jax.ShapeDtypeStruct((n_loc, model, ffn), F32),
            jax.ShapeDtypeStruct((n_loc, ffn, model), F32),
            jax.ShapeDtypeStruct(gg.shape, F32),
        ),
        scratch_shapes=[
            pltpu.VMEM(x_disp.shape, BF16),
            pltpu.VMEM((2, model, ffn), F32),
            pltpu.VMEM((2, model, ffn), F32),
            pltpu.VMEM((2, ffn, model), F32),
            pltpu.SemaphoreType.DMA((n_loc,)),
            pltpu.SemaphoreType.DMA((2, 3)),
        ],
        cost_estimate=pl.CostEstimate(flops=flops, bytes_accessed=moved, transcendentals=0),
        compiler_params=pltpu.CompilerParams(vmem_limit_bytes=WEIGHT_VMEM),
    )(pltpu.with_memory_space_constraint(x_disp, pltpu.HBM), *(pltpu.with_memory_space_constraint(rows, pltpu.VMEM) for rows in (dh_rows, a_rows, d_rows, gg)))


def final_kernel(own_ref, left_ref, right_ref, gx_out):
    gx_out[...] = (own_ref[...] + left_ref[...] + right_ref[...]).astype(BF16)


def final_sum(own, from_left, from_right):
    vmem = pl.BlockSpec(memory_space=pltpu.VMEM)
    return pl.pallas_call(
        final_kernel,
        name="final_sum",
        out_shape=jax.ShapeDtypeStruct(own.shape, BF16),
        in_specs=[vmem] * 3,
        out_specs=vmem,
        compiler_params=pltpu.CompilerParams(vmem_limit_bytes=8 * 1024 * 1024),
    )(*(pltpu.with_memory_space_constraint(part, pltpu.VMEM) for part in (own, from_left, from_right)))


def solution(mesh):
    axis = "ep"
    n_dev = mesh.shape[axis]
    rows_spec = P(("dp", "ep"), None)
    cube_spec = P(("dp", "ep"), None, None)
    weight_spec = P("ep", None, None)
    to_right = [(i, (i + 2) % n_dev) for i in range(n_dev)]
    to_left = [(i, (i - 2) % n_dev) for i in range(n_dev)]

    def local_step(grad_y, gate_vals, topk_idx, slot_ids, pair_counts, y_routed, x_disp, h_gate, h_up, w_gate, w_up, w_down):
        y_rows = y_routed.reshape(-1, y_routed.shape[2])
        d_rows, dh_rows, a_rows, gg, for_right, for_left, own = exchange(
            axis, n_dev, topk_idx.T, slot_ids.T, gate_vals.T, pair_counts, grad_y, y_rows, h_gate, h_up, w_gate, w_up, w_down)
        from_left = lax.ppermute(for_right, axis, to_right)
        from_right = lax.ppermute(for_left, axis, to_left)
        grad_wgate, grad_wup, grad_wdown, grad_gate = weight_grads(x_disp, dh_rows, a_rows, d_rows, gg)
        grad_x = final_sum(own, from_left, from_right)
        return grad_x, grad_gate.T, grad_wgate, grad_wup, grad_wdown

    return jax.shard_map(local_step, mesh=mesh, in_specs=(rows_spec, rows_spec, rows_spec, rows_spec, rows_spec, cube_spec, cube_spec, cube_spec, cube_spec, weight_spec, weight_spec, weight_spec), out_specs=(rows_spec, rows_spec, cube_spec, cube_spec, cube_spec), check_vma=False)
```

```python
import functools

import jax
import jax.numpy as jnp
from jax import lax
from jax.experimental import pallas as pl
from jax.experimental.pallas import tpu as pltpu
from jax.sharding import PartitionSpec as P

F32, BF16 = jnp.float32, jnp.bfloat16
COLS = 256
EXCHANGE_VMEM = 51 * 1024 * 1024
WEIGHT_VMEM = 24 * 1024 * 1024
OPP, LEFT, RIGHT, OWN = range(4)


def dot_last(a, b):
    return lax.dot_general(a, b, (((1,), (1,)), ((), ())), preferred_element_type=F32)


def dot_first(a, b):
    return lax.dot_general(a, b, (((0,), (0,)), ((), ())), preferred_element_type=F32)


def exchange_kernel(axis, n_dev, topk_ref, slot_ref, gate_ref, count_ref, gy_hbm, y_hbm, hg_hbm, hu_hbm, wg_hbm, wu_hbm, wd_hbm,
                    d_buf, dh_buf, a_buf, gg_out, right_out, left_out, own_out,
                    gy_all, route_send, route_all, y_buf, hg_buf, hu_buf, wgu_buf, wd_buf, wgu_turned, wd_turned, f1_buf, s_buf,
                    oh_buf, r_buf, pair_send, pair_recv, opp_send, opp_keep, opp_recv, hop_recv,
                    load_sem, route_ssem, route_rsem, gy_ssem, gy_rsem, pair_ssem, pair_rsem, hop_ssem, hop_rsem):
    n_loc, n_rows, ffn = hg_hbm.shape
    tok, model = gy_hbm.shape
    top_k = topk_ref.shape[0]
    cap = n_rows // n_dev
    n_exp = n_loc * n_dev
    half = tok // 2
    pair_rows = 2 * cap
    n_chip = n_dev // 2

    me = lax.axis_index(axis)
    chip = lax.div(me, 2)
    core = me - 2 * chip
    chips = [lax.rem(chip + step, n_chip) for step in (2, n_chip - 1, 1, 0)]
    homes = [2 * c + core for c in chips]
    others = [2 * c + 1 - core for c in chips]
    opp, left, right = homes[OPP], homes[LEFT], homes[RIGHT]
    sib = others[OWN]
    top, bottom, whole = pl.ds(0, half), pl.ds(half, half), pl.ds(0, tok)
    quarter = [pl.ds(i * (tok // 4), tok // 4) for i in range(4)]

    barrier = pltpu.get_barrier_semaphore()
    for step in range(1, n_dev):
        pl.semaphore_signal(barrier, inc=1, device_id={axis: lax.rem(me + step, n_dev)}, device_id_type=pl.DeviceIdType.MESH)

    loads = {}

    def load(name, src, dst):
        loads[name] = pltpu.make_async_copy(src, dst, load_sem.at[len(loads)])
        loads[name].start()

    load("gy", gy_hbm, gy_all.at[me])
    for e in range(n_loc):
        load(("hg", e), hg_hbm.at[e], hg_buf.at[e])
        load(("hu", e), hu_hbm.at[e], hu_buf.at[e])
    load("wd", wd_hbm, wd_buf)
    load("wg", wg_hbm, wgu_buf.at[:, :, pl.ds(0, ffn)])
    load("wu", wu_hbm, wgu_buf.at[:, :, pl.ds(ffn, ffn)])
    load("y", y_hbm, y_buf)

    loads["gy"].wait()
    pl.semaphore_wait(barrier, n_dev - 1)

    def remote(src, dst, ssem, rsem, dev):
        return pltpu.make_async_remote_copy(src_ref=src, dst_ref=dst, send_sem=ssem, recv_sem=rsem, device_id={axis: dev}, device_id_type=pl.DeviceIdType.MESH)

    def gy_copy(block, part, recv_slot, dev):
        ref = gy_all.at[block, part]
        return remote(ref, ref, gy_ssem, gy_rsem.at[recv_slot], dev)

    def gy_send(block, part, recv_slot, dev):
        gy_copy(block, part, recv_slot, dev).start()

    def gy_wait(block, part, recv_slot):
        gy_copy(block, part, recv_slot, sib).wait_recv()

    gy_send(me, quarter[0], 0, right)
    gy_send(me, quarter[2], 3, left)
    gy_send(me, whole, 8, sib)

    topk_t = topk_ref[...].astype(F32)
    slot_t = slot_ref[...].astype(F32)
    gate_t = gate_ref[...]
    exp_iota = lax.broadcasted_iota(jnp.int32, (n_exp, tok), 0).astype(F32)
    diag = lax.broadcasted_iota(jnp.int32, (n_exp, n_exp), 0) == lax.broadcasted_iota(jnp.int32, (n_exp, n_exp), 1)
    count = jnp.sum(jnp.where(diag, count_ref[...].astype(F32), 0.0), axis=1, keepdims=True)
    slot_d = jnp.zeros((n_exp, tok), F32)
    gate_d = jnp.zeros((n_exp, tok), F32)
    for j in range(top_k):
        hit = topk_t[j : j + 1] == exp_iota
        slot_d += jnp.where(hit, slot_t[j : j + 1] + 1.0, 0.0)
        gate_d += jnp.where(hit, gate_t[j : j + 1], 0.0)
    slot_d -= 1.0
    slot_d = jnp.where(slot_d < count, slot_d, -1.0)
    for i in range(n_dev):
        route_send[i, 0:n_loc] = slot_d[i * n_loc : (i + 1) * n_loc]
        route_send[i, n_loc : 2 * n_loc] = gate_d[i * n_loc : (i + 1) * n_loc]
    route_all[me] = route_send[me]

    peers = [sib, left, others[LEFT], right, others[RIGHT], opp, others[OPP]]
    for k, dst in enumerate(peers):
        remote(route_send.at[dst], route_all.at[me], route_ssem, route_rsem.at[(k + 3) // 4], dst).start()
    for to_right, to_left, slot in ((1, 3, 1), (2, 0, 2), (3, 1, 2)):
        gy_send(me, quarter[to_right], slot, right)
        gy_send(me, quarter[to_left], 3 + slot, left)

    chunk = 32
    n_chunk = n_rows // chunk

    def factors(e):
        def body(i, carry):
            rows = pl.ds(pl.multiple_of(i * chunk, chunk), chunk)
            h1 = hg_buf[e, rows].astype(F32)
            h3 = hu_buf[e, rows].astype(F32)
            sig = jax.nn.sigmoid(h1)
            act = h1 * sig
            s_buf[e, rows] = act
            a_buf[e, rows] = (act * h3).astype(BF16)
            f1_buf[e, rows] = h3 * sig * (1.0 + h1 * (1.0 - sig))
            return carry

        loads[("hg", e)].wait()
        loads[("hu", e)].wait()
        lax.fori_loop(0, n_chunk, body, 0)

    for e in range(n_loc):
        factors(e)

    def route_wait(slot, n):
        blocks = route_all.at[pl.ds(0, n)]
        remote(blocks, blocks, route_ssem, route_rsem.at[slot], sib).wait_recv()

    slot_iota = lax.broadcasted_iota(jnp.int32, (cap, tok), 0).astype(F32)

    def build_rows(s):
        route = route_all[s]
        picks, gates = [], []
        for e in range(n_loc):
            hit = route[e : e + 1] == slot_iota
            picks.append(jnp.where(hit, 1.0, 0.0).astype(BF16))
            gates.append(jnp.sum(jnp.where(hit, route[n_loc + e : n_loc + e + 1], 0.0), axis=1, keepdims=True))
        gate = jnp.concatenate(gates, axis=0)
        pick = jnp.concatenate(picks, axis=0)
        oh_buf[s] = pick.T
        for n in range(0, model, COLS):
            rows = (jnp.dot(pick, gy_all[s, :, pl.ds(n, COLS)], preferred_element_type=F32) * gate).astype(BF16)
            for e in range(n_loc):
                d_buf[e, pl.ds(pl.multiple_of(s * cap, cap), cap), pl.ds(n, COLS)] = rows[e * cap : (e + 1) * cap]

    def rows_of(c):
        return pl.ds(pl.multiple_of(c * pair_rows, pair_rows), pair_rows)

    def turn(src, dst, e):
        for i in range(0, src.shape[1], COLS):
            for j in range(0, src.shape[2], COLS):
                dst[e, pl.ds(j, COLS), pl.ds(i, COLS)] = src[e, pl.ds(i, COLS), pl.ds(j, COLS)].T

    def hidden_grads(roles, lo, hi):
        which = [chips[role] for role in roles]

        def body(e, carry):
            d_rows = jnp.concatenate([d_buf[e, rows_of(c)] for c in which], axis=0)
            for n in range(0, ffn, COLS):
                if roles == [OWN]:
                    grad = dot_last(d_rows, wd_buf[e, pl.ds(n, COLS)])
                else:
                    grad = jnp.dot(d_rows, wd_turned[e, :, pl.ds(n, COLS)], preferred_element_type=F32)
                grad = grad.astype(BF16).astype(F32)
                for i, c in enumerate(which):
                    part = grad[i * pair_rows : (i + 1) * pair_rows]
                    dh_buf[e, rows_of(c), pl.ds(n, COLS)] = (part * f1_buf[e, rows_of(c), pl.ds(n, COLS)]).astype(BF16)
                    dh_buf[e, rows_of(c), pl.ds(ffn + n, COLS)] = (part * s_buf[e, rows_of(c), pl.ds(n, COLS)]).astype(BF16)
            if roles == [OWN]:
                turn(wd_buf, wd_turned, e)
            return carry

        lax.fori_loop(lo, hi, body, 0, unroll=True)

    def returned(roles, lo, hi, cols):
        which = [chips[role] for role in roles]

        def body(e, carry):
            dh_rows = jnp.concatenate([dh_buf[e, rows_of(c)] for c in which], axis=0)
            out_rows = pl.ds(pl.multiple_of(e * cap, cap), cap)
            for n in cols:
                if roles == [OWN]:
                    ret = dot_last(dh_rows, wgu_buf[e, pl.ds(n, COLS)])
                else:
                    ret = jnp.dot(dh_rows, wgu_turned[e, :, pl.ds(n, COLS)], preferred_element_type=F32)
                ret = ret.astype(BF16)
                for i in range(len(which)):
                    for k in range(2):
                        lo_row = i * pair_rows + k * cap
                        r_buf[2 * i + k, out_rows, pl.ds(n, COLS)] = ret[lo_row : lo_row + cap]
            if roles == [OWN]:
                turn(wgu_buf, wgu_turned, e)
            return carry

        lax.fori_loop(lo, hi, body, 0, unroll=True)

    all_cols = range(0, model, COLS)

    def token_sum(role, k, n):
        return jnp.dot(oh_buf[2 * chips[role] + k], r_buf[2 * (role == RIGHT) + k, :, pl.ds(n, COLS)], preferred_element_type=F32)

    def finish(cols, slot, *roles):
        block = pl.ds(cols[0], len(cols) * COLS)
        for role, _ in roles:
            for n in cols:
                pair_send[role - 1, :, pl.ds(n, COLS)] = token_sum(role, 1 - core, n)
            remote(pair_send.at[role - 1, :, block], pair_recv.at[role - 1, :, block], pair_ssem.at[0], pair_rsem.at[slot], sib).start()
        for role, out in roles:
            for n in cols:
                out[:, pl.ds(n, COLS)] = token_sum(role, core, n)

    def add_pair(cols, slot, *roles):
        block = pl.ds(cols[0], len(cols) * COLS)
        first = roles[0][0] - 1
        ref = pair_recv.at[pl.ds(first, len(roles)), :, block]
        remote(ref, ref, pair_ssem.at[0], pair_rsem.at[slot], sib).wait_recv()
        for role, out in roles:
            out[:, block] = out[:, block] + pair_recv[role - 1, :, block]

    loads["wd"].wait()
    route_wait(0, 1)
    gy_wait(others[OWN], whole, 8)
    build_rows(homes[OWN])
    build_rows(others[OWN])
    hidden_grads([OWN], 0, n_loc)
    gy_wait(left, quarter[0], 0)
    gy_send(left, quarter[0], 6, right)

    loads["wg"].wait()
    loads["wu"].wait()
    returned([OWN], 0, 1, all_cols)
    gy_wait(right, quarter[2], 3)
    gy_send(right, quarter[2], 7, left)
    gy_wait(left, quarter[1], 1)
    gy_send(left, quarter[1], 6, right)
    gy_send(left, top, 9, sib)

    returned([OWN], 1, 2, all_cols)
    gy_wait(right, quarter[3], 4)
    gy_send(right, quarter[3], 7, left)
    gy_send(right, bottom, 10, sib)

    returned([OWN], 2, n_loc, all_cols)
    gy_wait(left, bottom, 2)
    gy_send(left, bottom, 9, sib)
    finish(all_cols, 0, (OWN, own_out))
    gy_wait(right, top, 5)
    gy_send(right, top, 10, sib)

    route_wait(1, 4)
    build_rows(homes[LEFT])
    build_rows(homes[RIGHT])
    gy_wait(others[LEFT], whole, 9)
    build_rows(others[LEFT])
    gy_wait(others[RIGHT], whole, 10)
    build_rows(others[RIGHT])

    gy_wait(opp, top, 6)
    gy_send(opp, top, 11, sib)
    gy_wait(opp, bottom, 7)
    gy_send(opp, bottom, 11, sib)
    route_wait(2, 2)
    build_rows(homes[OPP])
    hidden_grads([LEFT, RIGHT], 0, n_loc)

    gy_wait(others[OPP], whole, 11)
    build_rows(others[OPP])
    hidden_grads([OPP], 0, n_loc)

    def opp_pair(i):
        return remote(opp_send.at[i], opp_recv.at[i], pair_ssem.at[1], pair_rsem.at[3 + i], sib)

    def hop(i):
        opp_pair(i).wait_recv()
        opp_keep[i] = opp_keep[i] + opp_recv[i]
        for k, (part, dev) in enumerate(((top, right), (bottom, left))):
            remote(opp_keep.at[i, part], hop_recv.at[i, k], hop_ssem, hop_rsem.at[i], dev).start()

    for i, n in enumerate(all_cols):
        returned([OPP], 0, n_loc, [n])
        opp_send[i] = token_sum(OPP, 1 - core, n)
        opp_pair(i).start()
        opp_keep[i] = token_sum(OPP, core, n)
        if i:
            hop(i - 1)

    near = ((LEFT, left_out), (RIGHT, right_out))
    col_parts = (all_cols[:-1], all_cols[-1:])
    add_pair(all_cols, 0, (OWN, own_out))
    for part, cols in enumerate(col_parts):
        returned([LEFT, RIGHT], 0, n_loc, cols)
        if part == 0:
            hop(model // COLS - 1)
        finish(cols, 1 + part, *near)
    loads["y"].wait()
    group = 32
    gg = jnp.zeros((top_k, tok), F32)
    tok_major = lax.broadcasted_iota(jnp.int32, (group, top_k, tok), 0)
    tok_lane = lax.broadcasted_iota(jnp.int32, (group, top_k, tok), 2)
    for i in range(tok // group):
        prod = dot_last(y_buf[pl.ds(i * group * top_k, group * top_k)], gy_all[me])
        gg += jnp.sum(jnp.where(tok_major + i * group == tok_lane, prod.reshape(group, top_k, tok), 0.0), axis=0)
    gg_out[...] = gg

    for part, cols in enumerate(col_parts):
        add_pair(cols, 1 + part, *near)
    for i, n in enumerate(all_cols):
        remote(hop_recv.at[i], hop_recv.at[i], hop_ssem, hop_rsem.at[i], right).wait_recv()
        cols = pl.ds(n, COLS)
        right_out[top, cols] = right_out[top, cols] + hop_recv[i, 0]
        left_out[bottom, cols] = left_out[bottom, cols] + hop_recv[i, 1]

    sent = gy_all.at[pl.ds(0, n_dev - 1)]
    for ref, ssem, rsem in ((sent, gy_ssem, gy_rsem), (route_all.at[pl.ds(0, n_dev - 1)], route_ssem, route_rsem), (pair_send, pair_ssem.at[0], pair_rsem),
                            (opp_send, pair_ssem.at[1], pair_rsem), (hop_recv, hop_ssem, hop_rsem)):
        remote(ref, ref, ssem, rsem.at[0], sib).wait_send()


def exchange(axis, n_dev, topk_idx, slot_ids, gate_vals, pair_counts, grad_y, y_rows, h_gate, h_up, w_gate, w_up, w_down):
    n_loc, n_rows, ffn = h_gate.shape
    tok, model = grad_y.shape
    cap = n_rows // n_dev
    vmem = pl.BlockSpec(memory_space=pltpu.VMEM)
    hbm = pl.BlockSpec(memory_space=pl.ANY)
    dma = pltpu.SemaphoreType.DMA
    part = pltpu.VMEM((tok, model), F32)
    return pl.pallas_call(
        functools.partial(exchange_kernel, axis, n_dev),
        name="exchange",
        out_shape=(
            pltpu.VMEM((n_loc, n_rows, model), BF16),
            pltpu.VMEM((n_loc, n_rows, 2 * ffn), BF16),
            pltpu.VMEM((n_loc, n_rows, ffn), BF16),
            pltpu.VMEM((topk_idx.shape[0], tok), F32),
            part, part, part,
        ),
        in_specs=[vmem] * 4 + [hbm] * 7,
        out_specs=(vmem,) * 7,
        scratch_shapes=[
            pltpu.VMEM((n_dev, tok, model), BF16),
            pltpu.VMEM((n_dev, 2 * n_loc, tok), F32),
            pltpu.VMEM((n_dev, 2 * n_loc, tok), F32),
            pltpu.VMEM(y_rows.shape, BF16),
            pltpu.VMEM(h_gate.shape, BF16),
            pltpu.VMEM(h_up.shape, BF16),
            pltpu.VMEM((n_loc, model, 2 * ffn), BF16),
            pltpu.VMEM(w_down.shape, BF16),
            pltpu.VMEM((n_loc, 2 * ffn, model), BF16),
            pltpu.VMEM((n_loc, model, ffn), BF16),
            pltpu.VMEM(h_gate.shape, F32),
            pltpu.VMEM(h_gate.shape, F32),
            pltpu.VMEM((n_dev, tok, n_loc * cap), BF16),
            pltpu.VMEM((4, n_loc * cap, model), BF16),
            pltpu.VMEM((3, tok, model), F32),
            pltpu.VMEM((3, tok, model), F32),
            pltpu.VMEM((model // COLS, tok, COLS), F32),
            pltpu.VMEM((model // COLS, tok, COLS), F32),
            pltpu.VMEM((model // COLS, tok, COLS), F32),
            pltpu.VMEM((model // COLS, 2, tok // 2, COLS), F32),
            dma((5 + 2 * n_loc,)), dma, dma((3,)), dma, dma((12,)), dma((2,)), dma((3 + model // COLS,)), dma, dma((model // COLS,)),
        ],
        compiler_params=pltpu.CompilerParams(collective_id=0, has_side_effects=True, vmem_limit_bytes=EXCHANGE_VMEM),
    )(topk_idx, slot_ids, gate_vals, pair_counts, grad_y, y_rows, h_gate, h_up, w_gate, w_up, w_down)


def weight_kernel(x_hbm, dh_buf, a_buf, d_buf, gg_ref, wg_hbm, wu_hbm, wd_hbm, gg_out, x_buf, wg_buf, wu_buf, wd_buf, in_sem, out_sem):
    n_loc, ffn, model = a_buf.shape[0], a_buf.shape[2], d_buf.shape[2]
    gg_out[...] = gg_ref[...]
    ins = []
    for e in range(n_loc):
        ins.append(pltpu.make_async_copy(x_hbm.at[e], x_buf.at[e], in_sem.at[e]))
        ins[e].start()
    outs = {}

    def store(key, src, dst, sem):
        outs[key] = pltpu.make_async_copy(src, dst, sem)
        outs[key].start()

    for e in range(n_loc):
        slot = e % 2
        for k in range(3):
            if (slot, k) in outs:
                outs.pop((slot, k)).wait()
        for n in range(0, model, COLS):
            wd_buf[slot, :, pl.ds(n, COLS)] = dot_first(a_buf[e], d_buf[e, :, pl.ds(n, COLS)])
        store((slot, 0), wd_buf.at[slot], wd_hbm.at[e], out_sem.at[slot, 0])
        ins[e].wait()
        for n in range(0, ffn, COLS):
            wg_buf[slot, :, pl.ds(n, COLS)] = dot_first(x_buf[e], dh_buf[e, :, pl.ds(n, COLS)])
        store((slot, 1), wg_buf.at[slot], wg_hbm.at[e], out_sem.at[slot, 1])
        for n in range(0, ffn, COLS):
            wu_buf[slot, :, pl.ds(n, COLS)] = dot_first(x_buf[e], dh_buf[e, :, pl.ds(ffn + n, COLS)])
        store((slot, 2), wu_buf.at[slot], wu_hbm.at[e], out_sem.at[slot, 2])
    for copy in outs.values():
        copy.wait()


def weight_grads(x_disp, dh_rows, a_rows, d_rows, gg):
    n_loc, n_rows, model = x_disp.shape
    ffn = a_rows.shape[2]
    flops = 2 * n_loc * n_rows * model * 3 * ffn
    moved = 2 * x_disp.size + 12 * n_loc * model * ffn
    vmem = pl.BlockSpec(memory_space=pltpu.VMEM)
    hbm = pl.BlockSpec(memory_space=pl.ANY)
    return pl.pallas_call(
        weight_kernel,
        name="weight_grads",
        in_specs=[hbm] + [vmem] * 4,
        out_specs=(hbm, hbm, hbm, vmem),
        out_shape=(
            jax.ShapeDtypeStruct((n_loc, model, ffn), F32),
            jax.ShapeDtypeStruct((n_loc, model, ffn), F32),
            jax.ShapeDtypeStruct((n_loc, ffn, model), F32),
            jax.ShapeDtypeStruct(gg.shape, F32),
        ),
        scratch_shapes=[
            pltpu.VMEM(x_disp.shape, BF16),
            pltpu.VMEM((2, model, ffn), F32),
            pltpu.VMEM((2, model, ffn), F32),
            pltpu.VMEM((2, ffn, model), F32),
            pltpu.SemaphoreType.DMA((n_loc,)),
            pltpu.SemaphoreType.DMA((2, 3)),
        ],
        cost_estimate=pl.CostEstimate(flops=flops, bytes_accessed=moved, transcendentals=0),
        compiler_params=pltpu.CompilerParams(vmem_limit_bytes=WEIGHT_VMEM),
    )(pltpu.with_memory_space_constraint(x_disp, pltpu.HBM), *(pltpu.with_memory_space_constraint(rows, pltpu.VMEM) for rows in (dh_rows, a_rows, d_rows, gg)))


def final_kernel(own_ref, left_ref, right_ref, gx_out):
    gx_out[...] = (own_ref[...] + left_ref[...] + right_ref[...]).astype(BF16)


def final_sum(own, from_left, from_right):
    vmem = pl.BlockSpec(memory_space=pltpu.VMEM)
    return pl.pallas_call(
        final_kernel,
        name="final_sum",
        out_shape=jax.ShapeDtypeStruct(own.shape, BF16),
        in_specs=[vmem] * 3,
        out_specs=vmem,
        compiler_params=pltpu.CompilerParams(vmem_limit_bytes=8 * 1024 * 1024),
    )(*(pltpu.with_memory_space_constraint(part, pltpu.VMEM) for part in (own, from_left, from_right)))


def solution(mesh):
    axis = "ep"
    n_dev = mesh.shape[axis]
    rows_spec = P(("dp", "ep"), None)
    cube_spec = P(("dp", "ep"), None, None)
    weight_spec = P("ep", None, None)
    to_right = [(i, (i + 2) % n_dev) for i in range(n_dev)]
    to_left = [(i, (i - 2) % n_dev) for i in range(n_dev)]

    def local_step(grad_y, gate_vals, topk_idx, slot_ids, pair_counts, y_routed, x_disp, h_gate, h_up, w_gate, w_up, w_down):
        y_rows = y_routed.reshape(-1, y_routed.shape[2])
        d_rows, dh_rows, a_rows, gg, for_right, for_left, own = exchange(
            axis, n_dev, topk_idx.T, slot_ids.T, gate_vals.T, pair_counts, grad_y, y_rows, h_gate, h_up, w_gate, w_up, w_down)
        from_left = lax.ppermute(for_right, axis, to_right)
        from_right = lax.ppermute(for_left, axis, to_left)
        grad_wgate, grad_wup, grad_wdown, grad_gate = weight_grads(x_disp, dh_rows, a_rows, d_rows, gg)
        grad_x = final_sum(own, from_left, from_right)
        return grad_x, grad_gate.T, grad_wgate, grad_wup, grad_wdown

    return jax.shard_map(local_step, mesh=mesh, in_specs=(rows_spec, rows_spec, rows_spec, rows_spec, rows_spec, cube_spec, cube_spec, cube_spec, cube_spec, weight_spec, weight_spec, weight_spec), out_specs=(rows_spec, rows_spec, cube_spec, cube_spec, cube_spec), check_vma=False)
```

```python
import functools

import jax
import jax.numpy as jnp
from jax import lax
from jax.experimental import pallas as pl
from jax.experimental.pallas import tpu as pltpu
from jax.sharding import PartitionSpec as P

F32, BF16 = jnp.float32, jnp.bfloat16
COLS = 256
EXCHANGE_VMEM = 51 * 1024 * 1024
WEIGHT_VMEM = 24 * 1024 * 1024
OPP, LEFT, RIGHT, OWN = range(4)


def dot_last(a, b):
    return lax.dot_general(a, b, (((1,), (1,)), ((), ())), preferred_element_type=F32)


def dot_first(a, b):
    return lax.dot_general(a, b, (((0,), (0,)), ((), ())), preferred_element_type=F32)


def exchange_kernel(axis, n_dev, topk_ref, slot_ref, gate_ref, count_ref, gy_hbm, y_hbm, hg_hbm, hu_hbm, wg_hbm, wu_hbm, wd_hbm,
                    d_buf, dh_buf, a_buf, gg_out, right_out, left_out, own_out,
                    gy_all, route_send, route_all, y_buf, hg_buf, hu_buf, wgu_buf, wd_buf, wgu_turned, wd_turned, f1_buf, s_buf,
                    oh_buf, r_buf, pair_send, pair_recv, opp_send, opp_keep, opp_recv, hop_recv,
                    load_sem, route_ssem, route_rsem, gy_ssem, gy_rsem, pair_ssem, pair_rsem, hop_ssem, hop_rsem):
    n_loc, n_rows, ffn = hg_hbm.shape
    tok, model = gy_hbm.shape
    top_k = topk_ref.shape[0]
    cap = n_rows // n_dev
    n_exp = n_loc * n_dev
    half = tok // 2
    pair_rows = 2 * cap
    n_chip = n_dev // 2

    me = lax.axis_index(axis)
    chip = lax.div(me, 2)
    core = me - 2 * chip
    chips = [lax.rem(chip + step, n_chip) for step in (2, n_chip - 1, 1, 0)]
    homes = [2 * c + core for c in chips]
    others = [2 * c + 1 - core for c in chips]
    opp, left, right = homes[OPP], homes[LEFT], homes[RIGHT]
    sib = others[OWN]
    top, bottom, whole = pl.ds(0, half), pl.ds(half, half), pl.ds(0, tok)
    quarter = [pl.ds(i * (tok // 4), tok // 4) for i in range(4)]

    barrier = pltpu.get_barrier_semaphore()
    for step in range(1, n_dev):
        pl.semaphore_signal(barrier, inc=1, device_id={axis: lax.rem(me + step, n_dev)}, device_id_type=pl.DeviceIdType.MESH)

    loads = {}

    def load(name, src, dst):
        loads[name] = pltpu.make_async_copy(src, dst, load_sem.at[len(loads)])
        loads[name].start()

    load("gy", gy_hbm, gy_all.at[me])
    for e in range(n_loc):
        load(("hg", e), hg_hbm.at[e], hg_buf.at[e])
        load(("hu", e), hu_hbm.at[e], hu_buf.at[e])
    load("wd", wd_hbm, wd_buf)
    load("wg", wg_hbm, wgu_buf.at[:, :, pl.ds(0, ffn)])
    load("wu", wu_hbm, wgu_buf.at[:, :, pl.ds(ffn, ffn)])
    load("y", y_hbm, y_buf)

    loads["gy"].wait()
    pl.semaphore_wait(barrier, n_dev - 1)

    def remote(src, dst, ssem, rsem, dev):
        return pltpu.make_async_remote_copy(src_ref=src, dst_ref=dst, send_sem=ssem, recv_sem=rsem, device_id={axis: dev}, device_id_type=pl.DeviceIdType.MESH)

    def gy_copy(block, part, recv_slot, dev):
        ref = gy_all.at[block, part]
        return remote(ref, ref, gy_ssem, gy_rsem.at[recv_slot], dev)

    def gy_send(block, part, recv_slot, dev):
        gy_copy(block, part, recv_slot, dev).start()

    def gy_wait(block, part, recv_slot):
        gy_copy(block, part, recv_slot, sib).wait_recv()

    gy_send(me, quarter[0], 0, right)
    gy_send(me, quarter[2], 3, left)
    gy_send(me, whole, 8, sib)

    topk_t = topk_ref[...].astype(F32)
    slot_t = slot_ref[...].astype(F32)
    gate_t = gate_ref[...]
    exp_iota = lax.broadcasted_iota(jnp.int32, (n_exp, tok), 0).astype(F32)
    diag = lax.broadcasted_iota(jnp.int32, (n_exp, n_exp), 0) == lax.broadcasted_iota(jnp.int32, (n_exp, n_exp), 1)
    count = jnp.sum(jnp.where(diag, count_ref[...].astype(F32), 0.0), axis=1, keepdims=True)
    slot_d = jnp.zeros((n_exp, tok), F32)
    gate_d = jnp.zeros((n_exp, tok), F32)
    for j in range(top_k):
        hit = topk_t[j : j + 1] == exp_iota
        slot_d += jnp.where(hit, slot_t[j : j + 1] + 1.0, 0.0)
        gate_d += jnp.where(hit, gate_t[j : j + 1], 0.0)
    slot_d -= 1.0
    slot_d = jnp.where(slot_d < count, slot_d, -1.0)
    for i in range(n_dev):
        route_send[i, 0:n_loc] = slot_d[i * n_loc : (i + 1) * n_loc]
        route_send[i, n_loc : 2 * n_loc] = gate_d[i * n_loc : (i + 1) * n_loc]
    route_all[me] = route_send[me]

    peers = [sib, left, others[LEFT], right, others[RIGHT], opp, others[OPP]]
    for k, dst in enumerate(peers):
        remote(route_send.at[dst], route_all.at[me], route_ssem, route_rsem.at[(k + 3) // 4], dst).start()
    for to_right, to_left, slot in ((1, 3, 1), (2, 0, 2), (3, 1, 2)):
        gy_send(me, quarter[to_right], slot, right)
        gy_send(me, quarter[to_left], 3 + slot, left)

    chunk = 32
    n_chunk = n_rows // chunk

    def factors(e):
        def body(i, carry):
            rows = pl.ds(pl.multiple_of(i * chunk, chunk), chunk)
            h1 = hg_buf[e, rows].astype(F32)
            h3 = hu_buf[e, rows].astype(F32)
            sig = jax.nn.sigmoid(h1)
            act = h1 * sig
            s_buf[e, rows] = act
            a_buf[e, rows] = (act * h3).astype(BF16)
            f1_buf[e, rows] = h3 * sig * (1.0 + h1 * (1.0 - sig))
            return carry

        loads[("hg", e)].wait()
        loads[("hu", e)].wait()
        lax.fori_loop(0, n_chunk, body, 0)

    for e in range(n_loc):
        factors(e)

    def route_wait(slot, n):
        blocks = route_all.at[pl.ds(0, n)]
        remote(blocks, blocks, route_ssem, route_rsem.at[slot], sib).wait_recv()

    slot_iota = lax.broadcasted_iota(jnp.int32, (cap, tok), 0).astype(F32)

    def build_rows(s):
        route = route_all[s]
        picks, gates = [], []
        for e in range(n_loc):
            hit = route[e : e + 1] == slot_iota
            picks.append(jnp.where(hit, 1.0, 0.0).astype(BF16))
            gates.append(jnp.sum(jnp.where(hit, route[n_loc + e : n_loc + e + 1], 0.0), axis=1, keepdims=True))
        gate = jnp.concatenate(gates, axis=0)
        pick = jnp.concatenate(picks, axis=0)
        oh_buf[s] = pick.T
        for n in range(0, model, COLS):
            rows = (jnp.dot(pick, gy_all[s, :, pl.ds(n, COLS)], preferred_element_type=F32) * gate).astype(BF16)
            for e in range(n_loc):
                d_buf[e, pl.ds(pl.multiple_of(s * cap, cap), cap), pl.ds(n, COLS)] = rows[e * cap : (e + 1) * cap]

    def rows_of(c):
        return pl.ds(pl.multiple_of(c * pair_rows, pair_rows), pair_rows)

    def turn(src, dst, e):
        for i in range(0, src.shape[1], COLS):
            for j in range(0, src.shape[2], COLS):
                dst[e, pl.ds(j, COLS), pl.ds(i, COLS)] = src[e, pl.ds(i, COLS), pl.ds(j, COLS)].T

    def hidden_grads(roles, lo, hi):
        which = [chips[role] for role in roles]

        def body(e, carry):
            d_rows = jnp.concatenate([d_buf[e, rows_of(c)] for c in which], axis=0)
            for n in range(0, ffn, COLS):
                if roles == [OWN]:
                    grad = dot_last(d_rows, wd_buf[e, pl.ds(n, COLS)])
                else:
                    grad = jnp.dot(d_rows, wd_turned[e, :, pl.ds(n, COLS)], preferred_element_type=F32)
                grad = grad.astype(BF16).astype(F32)
                for i, c in enumerate(which):
                    part = grad[i * pair_rows : (i + 1) * pair_rows]
                    dh_buf[e, rows_of(c), pl.ds(n, COLS)] = (part * f1_buf[e, rows_of(c), pl.ds(n, COLS)]).astype(BF16)
                    dh_buf[e, rows_of(c), pl.ds(ffn + n, COLS)] = (part * s_buf[e, rows_of(c), pl.ds(n, COLS)]).astype(BF16)
            if roles == [OWN]:
                turn(wd_buf, wd_turned, e)
            return carry

        lax.fori_loop(lo, hi, body, 0, unroll=True)

    def returned(roles, lo, hi, cols):
        which = [chips[role] for role in roles]

        def body(e, carry):
            dh_rows = jnp.concatenate([dh_buf[e, rows_of(c)] for c in which], axis=0)
            out_rows = pl.ds(pl.multiple_of(e * cap, cap), cap)
            for n in cols:
                if roles == [OWN]:
                    ret = dot_last(dh_rows, wgu_buf[e, pl.ds(n, COLS)])
                else:
                    ret = jnp.dot(dh_rows, wgu_turned[e, :, pl.ds(n, COLS)], preferred_element_type=F32)
                ret = ret.astype(BF16)
                for i in range(len(which)):
                    for k in range(2):
                        lo_row = i * pair_rows + k * cap
                        r_buf[2 * i + k, out_rows, pl.ds(n, COLS)] = ret[lo_row : lo_row + cap]
            if roles == [OWN]:
                turn(wgu_buf, wgu_turned, e)
            return carry

        lax.fori_loop(lo, hi, body, 0, unroll=True)

    all_cols = range(0, model, COLS)

    def token_sum(role, k, n):
        return jnp.dot(oh_buf[2 * chips[role] + k], r_buf[2 * (role == RIGHT) + k, :, pl.ds(n, COLS)], preferred_element_type=F32)

    def finish(cols, slot, *roles):
        block = pl.ds(cols[0], len(cols) * COLS)
        for role, _ in roles:
            for n in cols:
                pair_send[role - 1, :, pl.ds(n, COLS)] = token_sum(role, 1 - core, n)
            remote(pair_send.at[role - 1, :, block], pair_recv.at[role - 1, :, block], pair_ssem.at[0], pair_rsem.at[slot], sib).start()
        for role, out in roles:
            for n in cols:
                out[:, pl.ds(n, COLS)] = token_sum(role, core, n)

    def add_pair(cols, slot, *roles):
        block = pl.ds(cols[0], len(cols) * COLS)
        first = roles[0][0] - 1
        ref = pair_recv.at[pl.ds(first, len(roles)), :, block]
        remote(ref, ref, pair_ssem.at[0], pair_rsem.at[slot], sib).wait_recv()
        for role, out in roles:
            out[:, block] = out[:, block] + pair_recv[role - 1, :, block]

    loads["wd"].wait()
    route_wait(0, 1)
    gy_wait(others[OWN], whole, 8)
    build_rows(homes[OWN])
    build_rows(others[OWN])
    hidden_grads([OWN], 0, n_loc)
    gy_wait(left, quarter[0], 0)
    gy_send(left, quarter[0], 6, right)

    loads["wg"].wait()
    loads["wu"].wait()
    returned([OWN], 0, 1, all_cols)
    gy_wait(right, quarter[2], 3)
    gy_send(right, quarter[2], 7, left)
    gy_wait(left, quarter[1], 1)
    gy_send(left, quarter[1], 6, right)
    gy_send(left, top, 9, sib)

    returned([OWN], 1, 2, all_cols)
    gy_wait(right, quarter[3], 4)
    gy_send(right, quarter[3], 7, left)
    gy_send(right, bottom, 10, sib)

    returned([OWN], 2, n_loc, all_cols)
    gy_wait(left, bottom, 2)
    gy_send(left, bottom, 9, sib)
    finish(all_cols, 0, (OWN, own_out))
    gy_wait(right, top, 5)
    gy_send(right, top, 10, sib)

    route_wait(1, 4)
    build_rows(homes[LEFT])
    build_rows(homes[RIGHT])
    gy_wait(others[LEFT], whole, 9)
    build_rows(others[LEFT])
    gy_wait(others[RIGHT], whole, 10)
    build_rows(others[RIGHT])

    gy_wait(opp, top, 6)
    gy_send(opp, top, 11, sib)
    gy_wait(opp, bottom, 7)
    gy_send(opp, bottom, 11, sib)
    route_wait(2, 2)
    build_rows(homes[OPP])
    hidden_grads([LEFT, RIGHT], 0, n_loc // 2)

    gy_wait(others[OPP], whole, 11)
    build_rows(others[OPP])
    hidden_grads([OPP], 0, n_loc)

    def opp_pair(i):
        return remote(opp_send.at[i], opp_recv.at[i], pair_ssem.at[1], pair_rsem.at[3 + i], sib)

    def hop(i):
        opp_pair(i).wait_recv()
        opp_keep[i] = opp_keep[i] + opp_recv[i]
        for k, (part, dev) in enumerate(((top, right), (bottom, left))):
            remote(opp_keep.at[i, part], hop_recv.at[i, k], hop_ssem, hop_rsem.at[i], dev).start()

    for i, n in enumerate(all_cols):
        returned([OPP], 0, n_loc, [n])
        opp_send[i] = token_sum(OPP, 1 - core, n)
        opp_pair(i).start()
        opp_keep[i] = token_sum(OPP, core, n)
        if i:
            hop(i - 1)

    near = ((LEFT, left_out), (RIGHT, right_out))
    col_parts = (all_cols[:-1], all_cols[-1:])
    add_pair(all_cols, 0, (OWN, own_out))
    hidden_grads([LEFT, RIGHT], n_loc // 2, n_loc)
    hop(model // COLS - 1)
    for part, cols in enumerate(col_parts):
        returned([LEFT, RIGHT], 0, n_loc, cols)
        finish(cols, 1 + part, *near)
    loads["y"].wait()
    group = 32
    gg = jnp.zeros((top_k, tok), F32)
    tok_major = lax.broadcasted_iota(jnp.int32, (group, top_k, tok), 0)
    tok_lane = lax.broadcasted_iota(jnp.int32, (group, top_k, tok), 2)
    for i in range(tok // group):
        prod = dot_last(y_buf[pl.ds(i * group * top_k, group * top_k)], gy_all[me])
        gg += jnp.sum(jnp.where(tok_major + i * group == tok_lane, prod.reshape(group, top_k, tok), 0.0), axis=0)
    gg_out[...] = gg

    for part, cols in enumerate(col_parts):
        add_pair(cols, 1 + part, *near)
    for i, n in enumerate(all_cols):
        remote(hop_recv.at[i], hop_recv.at[i], hop_ssem, hop_rsem.at[i], right).wait_recv()
        cols = pl.ds(n, COLS)
        right_out[top, cols] = right_out[top, cols] + hop_recv[i, 0]
        left_out[bottom, cols] = left_out[bottom, cols] + hop_recv[i, 1]

    sent = gy_all.at[pl.ds(0, n_dev - 1)]
    for ref, ssem, rsem in ((sent, gy_ssem, gy_rsem), (route_all.at[pl.ds(0, n_dev - 1)], route_ssem, route_rsem), (pair_send, pair_ssem.at[0], pair_rsem),
                            (opp_send, pair_ssem.at[1], pair_rsem), (hop_recv, hop_ssem, hop_rsem)):
        remote(ref, ref, ssem, rsem.at[0], sib).wait_send()


def exchange(axis, n_dev, topk_idx, slot_ids, gate_vals, pair_counts, grad_y, y_rows, h_gate, h_up, w_gate, w_up, w_down):
    n_loc, n_rows, ffn = h_gate.shape
    tok, model = grad_y.shape
    cap = n_rows // n_dev
    vmem = pl.BlockSpec(memory_space=pltpu.VMEM)
    hbm = pl.BlockSpec(memory_space=pl.ANY)
    dma = pltpu.SemaphoreType.DMA
    part = pltpu.VMEM((tok, model), F32)
    return pl.pallas_call(
        functools.partial(exchange_kernel, axis, n_dev),
        name="exchange",
        out_shape=(
            pltpu.VMEM((n_loc, n_rows, model), BF16),
            pltpu.VMEM((n_loc, n_rows, 2 * ffn), BF16),
            pltpu.VMEM((n_loc, n_rows, ffn), BF16),
            pltpu.VMEM((topk_idx.shape[0], tok), F32),
            part, part, part,
        ),
        in_specs=[vmem] * 4 + [hbm] * 7,
        out_specs=(vmem,) * 7,
        scratch_shapes=[
            pltpu.VMEM((n_dev, tok, model), BF16),
            pltpu.VMEM((n_dev, 2 * n_loc, tok), F32),
            pltpu.VMEM((n_dev, 2 * n_loc, tok), F32),
            pltpu.VMEM(y_rows.shape, BF16),
            pltpu.VMEM(h_gate.shape, BF16),
            pltpu.VMEM(h_up.shape, BF16),
            pltpu.VMEM((n_loc, model, 2 * ffn), BF16),
            pltpu.VMEM(w_down.shape, BF16),
            pltpu.VMEM((n_loc, 2 * ffn, model), BF16),
            pltpu.VMEM((n_loc, model, ffn), BF16),
            pltpu.VMEM(h_gate.shape, F32),
            pltpu.VMEM(h_gate.shape, F32),
            pltpu.VMEM((n_dev, tok, n_loc * cap), BF16),
            pltpu.VMEM((4, n_loc * cap, model), BF16),
            pltpu.VMEM((3, tok, model), F32),
            pltpu.VMEM((3, tok, model), F32),
            pltpu.VMEM((model // COLS, tok, COLS), F32),
            pltpu.VMEM((model // COLS, tok, COLS), F32),
            pltpu.VMEM((model // COLS, tok, COLS), F32),
            pltpu.VMEM((model // COLS, 2, tok // 2, COLS), F32),
            dma((5 + 2 * n_loc,)), dma, dma((3,)), dma, dma((12,)), dma((2,)), dma((3 + model // COLS,)), dma, dma((model // COLS,)),
        ],
        compiler_params=pltpu.CompilerParams(collective_id=0, has_side_effects=True, vmem_limit_bytes=EXCHANGE_VMEM),
    )(topk_idx, slot_ids, gate_vals, pair_counts, grad_y, y_rows, h_gate, h_up, w_gate, w_up, w_down)


def weight_kernel(x_hbm, dh_buf, a_buf, d_buf, gg_ref, wg_hbm, wu_hbm, wd_hbm, gg_out, x_buf, wg_buf, wu_buf, wd_buf, in_sem, out_sem):
    n_loc, ffn, model = a_buf.shape[0], a_buf.shape[2], d_buf.shape[2]
    gg_out[...] = gg_ref[...]
    ins = []
    for e in range(n_loc):
        ins.append(pltpu.make_async_copy(x_hbm.at[e], x_buf.at[e], in_sem.at[e]))
        ins[e].start()
    outs = {}

    def store(key, src, dst, sem):
        outs[key] = pltpu.make_async_copy(src, dst, sem)
        outs[key].start()

    for e in range(n_loc):
        slot = e % 2
        for k in range(3):
            if (slot, k) in outs:
                outs.pop((slot, k)).wait()
        for n in range(0, model, COLS):
            wd_buf[slot, :, pl.ds(n, COLS)] = dot_first(a_buf[e], d_buf[e, :, pl.ds(n, COLS)])
        store((slot, 0), wd_buf.at[slot], wd_hbm.at[e], out_sem.at[slot, 0])
        ins[e].wait()
        for n in range(0, ffn, COLS):
            wg_buf[slot, :, pl.ds(n, COLS)] = dot_first(x_buf[e], dh_buf[e, :, pl.ds(n, COLS)])
        store((slot, 1), wg_buf.at[slot], wg_hbm.at[e], out_sem.at[slot, 1])
        for n in range(0, ffn, COLS):
            wu_buf[slot, :, pl.ds(n, COLS)] = dot_first(x_buf[e], dh_buf[e, :, pl.ds(ffn + n, COLS)])
        store((slot, 2), wu_buf.at[slot], wu_hbm.at[e], out_sem.at[slot, 2])
    for copy in outs.values():
        copy.wait()


def weight_grads(x_disp, dh_rows, a_rows, d_rows, gg):
    n_loc, n_rows, model = x_disp.shape
    ffn = a_rows.shape[2]
    flops = 2 * n_loc * n_rows * model * 3 * ffn
    moved = 2 * x_disp.size + 12 * n_loc * model * ffn
    vmem = pl.BlockSpec(memory_space=pltpu.VMEM)
    hbm = pl.BlockSpec(memory_space=pl.ANY)
    return pl.pallas_call(
        weight_kernel,
        name="weight_grads",
        in_specs=[hbm] + [vmem] * 4,
        out_specs=(hbm, hbm, hbm, vmem),
        out_shape=(
            jax.ShapeDtypeStruct((n_loc, model, ffn), F32),
            jax.ShapeDtypeStruct((n_loc, model, ffn), F32),
            jax.ShapeDtypeStruct((n_loc, ffn, model), F32),
            jax.ShapeDtypeStruct(gg.shape, F32),
        ),
        scratch_shapes=[
            pltpu.VMEM(x_disp.shape, BF16),
            pltpu.VMEM((2, model, ffn), F32),
            pltpu.VMEM((2, model, ffn), F32),
            pltpu.VMEM((2, ffn, model), F32),
            pltpu.SemaphoreType.DMA((n_loc,)),
            pltpu.SemaphoreType.DMA((2, 3)),
        ],
        cost_estimate=pl.CostEstimate(flops=flops, bytes_accessed=moved, transcendentals=0),
        compiler_params=pltpu.CompilerParams(vmem_limit_bytes=WEIGHT_VMEM),
    )(pltpu.with_memory_space_constraint(x_disp, pltpu.HBM), *(pltpu.with_memory_space_constraint(rows, pltpu.VMEM) for rows in (dh_rows, a_rows, d_rows, gg)))


def final_kernel(own_ref, left_ref, right_ref, gx_out):
    gx_out[...] = (own_ref[...] + left_ref[...] + right_ref[...]).astype(BF16)


def final_sum(own, from_left, from_right):
    vmem = pl.BlockSpec(memory_space=pltpu.VMEM)
    return pl.pallas_call(
        final_kernel,
        name="final_sum",
        out_shape=jax.ShapeDtypeStruct(own.shape, BF16),
        in_specs=[vmem] * 3,
        out_specs=vmem,
        compiler_params=pltpu.CompilerParams(vmem_limit_bytes=8 * 1024 * 1024),
    )(*(pltpu.with_memory_space_constraint(part, pltpu.VMEM) for part in (own, from_left, from_right)))


def solution(mesh):
    axis = "ep"
    n_dev = mesh.shape[axis]
    rows_spec = P(("dp", "ep"), None)
    cube_spec = P(("dp", "ep"), None, None)
    weight_spec = P("ep", None, None)
    to_right = [(i, (i + 2) % n_dev) for i in range(n_dev)]
    to_left = [(i, (i - 2) % n_dev) for i in range(n_dev)]

    def local_step(grad_y, gate_vals, topk_idx, slot_ids, pair_counts, y_routed, x_disp, h_gate, h_up, w_gate, w_up, w_down):
        y_rows = y_routed.reshape(-1, y_routed.shape[2])
        d_rows, dh_rows, a_rows, gg, for_right, for_left, own = exchange(
            axis, n_dev, topk_idx.T, slot_ids.T, gate_vals.T, pair_counts, grad_y, y_rows, h_gate, h_up, w_gate, w_up, w_down)
        from_left = lax.ppermute(for_right, axis, to_right)
        from_right = lax.ppermute(for_left, axis, to_left)
        grad_wgate, grad_wup, grad_wdown, grad_gate = weight_grads(x_disp, dh_rows, a_rows, d_rows, gg)
        grad_x = final_sum(own, from_left, from_right)
        return grad_x, grad_gate.T, grad_wgate, grad_wup, grad_wdown

    return jax.shard_map(local_step, mesh=mesh, in_specs=(rows_spec, rows_spec, rows_spec, rows_spec, rows_spec, cube_spec, cube_spec, cube_spec, cube_spec, weight_spec, weight_spec, weight_spec), out_specs=(rows_spec, rows_spec, cube_spec, cube_spec, cube_spec), check_vma=False)
```
